256 devices in a mesh: tm: 4 (over y), users: 64 (over z, x, core).
Axes of the slice: x: 4, y: 4, z: 8, core: 2. Of those that a mesh axis runs over, the one named last changes fastest.
Arguments:
- features: float32 [1048576, 128], P(('tm', 'users')), may hold values from -6 to 6
- home: int32 [1048576, 1], P(('tm', 'users')), may hold values from 0 to 63; in each aligned block of 4096 rows (0 to 4095, 4096 to 8191, ...) at most 128 rows name the same one
- account: int32 [1048576], P(('tm', 'users')), may hold values from 0 to 127
- flags: int32 [1048576], P(('tm', 'users')), may hold values 0 or 1
Outputs:
- session_mean: float32 [1048576, 128], P(('tm', 'users'))
The draws below stay inside these ranges and needn't reach their ends.
Inputs may be any that keep to these rules, and one draw needn't show every extreme that they name: `home`: the 4096 events of one device name one owner at most 128 times, a bound that some block reaches.
All inputs are finite; a program needn't handle non-finite values. No bound on the sum of `flags` on one device may be relied on, other than what follows from the above.
Results may differ from the reference program's by a relative error of at most 0.00007.
Values sent between devices are 32-bit elements; how exact they have to be, the bound alone decides.
No kernel may reach another device: no remote copies, remote signals or barrier semaphores. Data moves between devices by JAX's collectives and lax.ppermute only.
A program may use at most 64 MiB of HBM per device.

```python
import math
import jax
import jax.numpy as jnp
import numpy as np
from jax import lax

F = 128
EV_DEV = 4096
ACCOUNTS = 128
CAP = 128
EVENTS = 1048576
N_USERS = 64


def set_ends(array, key, least, largest):
    spot = [jax.random.randint(jax.random.fold_in(key, axis), (), 0, length) for axis, length in enumerate(array.shape)]
    longest = array.shape.index(max(array.shape))
    beside = spot[:longest] + [(spot[longest] + 1) % array.shape[longest]] + spot[longest + 1:]
    return array.at[tuple(spot)].set(least).at[tuple(beside)].set(largest)


def levels(key, dims, shards, low, high):
    def one(position, shards_of):
        heights = jax.random.uniform(jax.random.fold_in(jax.random.fold_in(key, 6), position), (shards_of,), jnp.float32, low / len(shards), high / len(shards))
        return jnp.repeat(jnp.exp(heights), dims[position] // shards_of).reshape((-1,) + (1,) * (len(dims) - position - 1))

    gain = one(*shards[0])
    for cut in shards[1:]:
        gain = gain * one(*cut)
    return gain


def routed_block(key, own, number, rows, number_of, top, most, lean):
    sequence = jax.random.permutation(key, number_of)
    heavy_load, usual = load_shares(number_of, rows * top, most, lean, True), load_shares(number_of, rows * top, most, lean, False)
    places = jnp.arange(number_of)

    def named(lengths, turn):
        used = int((lengths > 0).sum())
        fixed = max(1, used // 4)
        shifted = fixed + (places - fixed + turn * (used - fixed)) % max(1, number_of - fixed)
        return jnp.zeros((number_of,), jnp.int32).at[sequence[jnp.where(places < fixed, places, shifted)]].set(jnp.asarray(lengths, jnp.int32))

    lengths = jnp.where(number % 4 == 0, named(heavy_load, number // 4), named(usual, number - number // 4 - 1))
    mixed = jax.random.permutation(jax.random.fold_in(own, 3), number_of)
    source_of, receiver = mixed[0:number_of // 2 * 2:2], mixed[1:number_of // 2 * 2:2]
    margin = jnp.minimum(lengths[source_of] - 1, most - lengths[receiver]) // 2
    margin = jnp.where((source_of == sequence[0]) | (receiver == sequence[0]) | (lengths[receiver] == 0), 0, jnp.maximum(margin, 0))
    shifted = jax.random.randint(jax.random.fold_in(own, 4), (number_of // 2,), 0, 1 << 20) % (margin + 1)
    lengths = lengths.at[source_of].add(-shifted).at[receiver].add(shifted)
    labels = jnp.searchsorted(jnp.cumsum(lengths), jnp.arange(rows * top), side="right").astype(jnp.int32)
    table = labels.reshape(top, rows).T
    table = table[jax.random.permutation(jax.random.fold_in(own, 1), rows)]
    turn = jax.random.randint(jax.random.fold_in(own, 2), (rows, 1), 0, top)
    return jnp.take_along_axis(table, (jnp.arange(top)[None, :] + turn) % top, axis=1)


def load_shares(count, total, limit, slope, full):
    weights = [(1 << 20) // math.isqrt(grade ** slope) + 1 for grade in range(1, count + 1)]
    largest = limit if full else min(limit, max(-(-total // count), total * weights[0] // sum(weights)))
    least = 1 if total - largest >= count - 1 else 0
    given, spare = [largest] + [least] * (count - 1), total - largest - least * (count - 1)
    while spare > 0:
        candidates = [i for i in range(1, count) if given[i] < largest] or [i for i in range(1, count) if given[i] < limit]
        mass, remaining = sum([weights[i] for i in candidates]), spare
        for i in candidates:
            extra = min(limit - given[i], max(1, remaining * weights[i] // mass), spare)
            given[i] = given[i] + extra
            spare = spare - extra
    return np.array(given)


def gaussian(stream_key, extent, deviation, bound, shards=(), dtype=jnp.bfloat16):
    gain = levels(stream_key, extent, shards, -0.22, 0.18) if shards else 1.0
    drawn = jax.random.normal(stream_key, extent, jnp.float32) * deviation * gain
    return jnp.minimum(jnp.maximum(drawn, -bound), bound).astype(dtype)


def setup_inputs(seed: int = 0) -> dict:
    key_list = jax.random.split(jax.random.key(seed), 5)
    features = gaussian(key_list[0], (EVENTS, F), 1.0, 6.0, ((0, 256),), jnp.float32)
    home_keys = jax.random.split(jax.random.fold_in(key_list[1], 1), EVENTS // EV_DEV)
    home_turns = jax.random.permutation(jax.random.fold_in(key_list[1], 3), EVENTS // EV_DEV)
    home = jax.vmap(lambda own, number: routed_block(jax.random.fold_in(key_list[1], 2), own, number, EV_DEV, N_USERS, 1, CAP, 2))(home_keys, home_turns).reshape((EVENTS, 1))
    account = set_ends(jax.random.randint(key_list[2], (EVENTS,), 0, ACCOUNTS), jax.random.fold_in(key_list[2], 1), 0, ACCOUNTS - 1).astype(jnp.int32)
    flags = set_ends((jax.random.randint(key_list[3], (EVENTS,), 0, 64) < 1).astype(jnp.int32), jax.random.fold_in(key_list[3], 1), 0, 1)
    return dict(features=features, home=home, account=account, flags=flags)


def combine_runs(earlier, later):
    carry_on = 1.0 - later[2]
    return (later[0] + carry_on[..., None] * earlier[0], later[1] + carry_on * earlier[1], jnp.maximum(earlier[2], later[2]))


def reference(features, home, account, flags):
    user = home[:, 0].astype(jnp.int32) * ACCOUNTS + account.astype(jnp.int32)
    order = jnp.argsort(user, stable=True)
    user_sorted = user[order]
    flag_sorted = flags[order].astype(jnp.int32)
    values = features[order]
    changed = jnp.concatenate([jnp.ones((1,), jnp.int32), (user_sorted[1:] != user_sorted[:-1]).astype(jnp.int32)])
    starts = jnp.maximum(changed, flag_sorted).astype(jnp.float32)
    singles = jnp.ones(starts.shape, jnp.float32)
    sums, counts, marks = lax.associative_scan(combine_runs, (values, singles, starts))
    means = sums / counts[:, None]
    return jnp.zeros_like(features).at[order].set(means)
```

```python
import functools

import jax
import jax.numpy as jnp
from jax import lax
from jax.experimental import pallas as pl
from jax.experimental.pallas import tpu as pltpu
from jax.sharding import Mesh, PartitionSpec as P

LANES = 128
ROWS = 136
NZ, NX, NC = 8, 4, 2
OWNERS = NZ * NX * NC
HALF = OWNERS // NC
CHUNK = HALF // NX
BF16, F32, I32 = jnp.bfloat16, jnp.float32, jnp.int32
VMEM = pl.BlockSpec(memory_space=pltpu.VMEM)
SMEM = pl.BlockSpec(memory_space=pltpu.SMEM)


def dot(a, b):
    return lax.dot_general(a, b, (((1,), (0,)), ((), ())), preferred_element_type=F32)


def dot_nt(a, b):
    return lax.dot_general(a, b, (((1,), (1,)), ((), ())), preferred_element_type=F32)


def iota(shape, dim):
    return lax.broadcasted_iota(I32, shape, dim)


def as_bf16(mask):
    return jnp.where(mask, 1.0, 0.0).astype(BF16)


def two_parts(v):
    high = v.astype(BF16)
    low = (v - high.astype(F32)).astype(BF16)
    return jnp.concatenate([high, low], axis=1)


def masked_sum(mask, parts):
    both = dot(mask, parts)
    return both[:, :LANES] + both[:, LANES:]


def column(row):
    return jnp.broadcast_to(row, (LANES, LANES)).T


def call(kernel, out, args, specs, out_specs=None, scratch=(), cost=1_000_000, limit=24):
    return pl.pallas_call(
        kernel,
        out_shape=out,
        in_specs=specs,
        out_specs=out_specs or jax.tree.map(lambda _: VMEM, out),
        scratch_shapes=list(scratch),
        cost_estimate=pl.CostEstimate(flops=cost, bytes_accessed=1_000_000, transcendentals=0),
        compiler_params=pltpu.CompilerParams(vmem_limit_bytes=limit << 20),
    )(*args)


def block(n=None):
    shape = (ROWS, LANES) if n is None else (n, ROWS, LANES)
    return jax.ShapeDtypeStruct(shape, F32)


def regroup_kernel(
    place, home, account, flags, features, slot_out, acc_out, flag_out, grouped, other, mine,
    slots, sem,
):
    lines = home.shape[0]
    below = as_bf16(iota((LANES, LANES), 0) < iota((LANES, LANES), 1))
    with_total = jnp.concatenate([below, jnp.ones((LANES, LANES), BF16)], axis=1)
    owner_ids = iota((OWNERS, LANES), 0)
    before = jnp.zeros((OWNERS, LANES), F32)
    codes = jnp.zeros((OWNERS, LANES), F32)
    for b in range(lines):
        home_row = home[b : b + 1, :]
        chosen = owner_ids == home_row
        counted = dot(as_bf16(chosen), with_total)
        rank = jnp.sum(
            jnp.where(chosen, counted[:, :LANES] + before, 0.0), axis=0, keepdims=True
        )
        before = before + counted[:, LANES:]
        slot_out[b : b + 1, :] = home_row * LANES + rank.astype(I32)
        code = (account[b : b + 1, :] * 2 + flags[b : b + 1, :] + 1).astype(F32)
        rank_of = as_bf16(iota((LANES, LANES), 0) == rank.astype(I32))
        codes = codes + dot_nt(jnp.where(chosen, code, 0.0).astype(BF16), rank_of)
    copy = pltpu.make_async_copy(slot_out, slots, sem)
    copy.start()
    code_ids = codes.astype(I32) - 1
    acc_out[...] = jnp.right_shift(code_ids, 1)
    flag_out[...] = jnp.where(code_ids >= 0, jnp.bitwise_and(code_ids, 1), 0).astype(F32)
    zero = jnp.zeros((LANES, LANES), F32)

    def clear(o, _):
        grouped[pl.ds(o * LANES, LANES), :] = zero
        return 0

    lax.fori_loop(0, OWNERS, clear, 0)
    copy.wait()

    def spread(b, _):
        for j in range(LANES):
            grouped[pl.ds(slots[b, j], 1), :] = features[pl.ds(b * LANES + j, 1), :]
        return 0

    lax.fori_loop(0, lines, spread, 0)

    after = as_bf16(iota((LANES, LANES), 0) > iota((LANES, LANES), 1))
    ones = jnp.ones((8, LANES), BF16)
    sub = iota((8, LANES), 0)
    half_of = place[0]

    def closing(o, out, at):
        acc_row = acc_out[pl.ds(o, 1), :]
        flag_row = flag_out[pl.ds(o, 1), :]
        member = iota((LANES, LANES), 0) == acc_row
        member_flags = jnp.where(member, flag_row, 0.0).astype(BF16)
        later_flags = dot(member_flags, after)
        counted = as_bf16(member & (later_flags < 0.5))
        values = two_parts(grouped[pl.ds(pl.multiple_of(o * LANES, LANES), LANES), :])
        out[at, :LANES, :] = masked_sum(counted, values)
        count = dot_nt(ones, counted)
        mark = jnp.minimum(dot_nt(ones, member_flags), 1.0)
        out[at, LANES:, :] = jnp.where(sub == 0, count, jnp.where(sub == 1, mark, 0.0))

    for out, base in ((other, (1 - half_of) * HALF), (mine, half_of * HALF)):

        def some(g, _, out=out, base=base):
            for i in range(4):
                closing(base + g * 4 + i, out, g * 4 + i)
            return 0

        lax.fori_loop(0, HALF // 4, some, 0)


def running_kernel(
    slots, slot_rows, home, account, acc_rows, flag_rows, grouped,
    run_out, count_out, open_out, user_out, run, counts, opens,
):
    lines = home.shape[0]
    after = as_bf16(iota((LANES, LANES), 0) > iota((LANES, LANES), 1))
    up_to = iota((LANES, LANES), 1) <= iota((LANES, LANES), 0)
    ones = jnp.ones((8, LANES), BF16)

    def some(g, _):
        rows = pl.ds(pl.multiple_of(g * 8, 8), 8)
        acc8 = acc_rows[rows, :]
        flag8 = flag_rows[rows, :]
        acc_cols = acc8.astype(F32).T
        count8, open8 = [], []
        for i in range(8):
            acc_row = acc8[i : i + 1, :].astype(F32)
            acc_col = jnp.broadcast_to(acc_cols[:, i : i + 1], (LANES, LANES))
            same = (acc_col == acc_row) & (acc_row >= 0.0) & up_to
            same_flags = jnp.where(same, flag8[i : i + 1, :], 0.0).astype(BF16)
            between = dot(same_flags, after)
            session = as_bf16(same & (between < 0.5))
            at = pl.ds(pl.multiple_of((g * 8 + i) * LANES, LANES), LANES)
            run[at, :] = masked_sum(session, two_parts(grouped[at, :]))
            count8.append(dot_nt(ones, session)[:1, :])
            open8.append(dot_nt(ones, same_flags)[:1, :])
        counts[rows, :] = jnp.concatenate(count8, axis=0)
        opens[rows, :] = jnp.where(jnp.concatenate(open8, axis=0) < 0.5, 1.0, 0.0)
        return 0

    lax.fori_loop(0, OWNERS // 8, some, 0)

    def scalars(t, _):
        rows = pl.ds(pl.multiple_of(t * 8, 8), 8)
        home8 = home[rows, :]
        rank = slot_rows[rows, :] - home8 * LANES
        count = jnp.zeros((8, LANES), F32)
        is_open = jnp.zeros((8, LANES), F32)
        for o in range(OWNERS):
            here = home8 == o
            for_count = jnp.broadcast_to(counts[o : o + 1, :], (8, LANES))
            for_open = jnp.broadcast_to(opens[o : o + 1, :], (8, LANES))
            count = jnp.where(here, jnp.take_along_axis(for_count, rank, axis=1), count)
            is_open = jnp.where(here, jnp.take_along_axis(for_open, rank, axis=1), is_open)
        count_out[rows, :] = count
        open_out[rows, :] = is_open
        user_out[rows, :] = home8 * ROWS + jnp.where(is_open > 0.5, account[rows, :], ROWS - 1)
        return 0

    lax.fori_loop(0, lines // 8, scalars, 0)

    def collect(b, _):
        for j in range(LANES):
            run_out[pl.ds(b * LANES + j, 1), :] = run[pl.ds(slots[b, j], 1), :]
        return 0

    lax.fori_loop(0, lines, collect, 0)


def joined(earlier, later):
    mark = later[LANES + 1 : LANES + 2, :]
    sums = later[:LANES, :] + column(1.0 - mark) * earlier[:LANES, :]
    sub = iota((8, LANES), 0)
    tail, first = later[LANES:, :], earlier[LANES:, :]
    tail = jnp.where(
        sub == 0, tail + (1.0 - mark) * first, jnp.where(sub == 1, jnp.maximum(tail, first), 0.0)
    )
    return jnp.concatenate([sums, tail], axis=0)


def core_kernel(place, mine, got, *outs):
    first, x = place[0] == 0, place[1]
    for k in range(NX):
        base = lax.rem(x + k, NX) * CHUNK

        def one(i, _, k=k, base=base):
            a, b = mine[base + i], got[base + i]
            outs[k][i] = joined(jnp.where(first, a, b), jnp.where(first, b, a))
            return 0

        lax.fori_loop(0, CHUNK, one, 0)


def row_kernel(place, t0, t1, t2, t3, out):
    tables = (t0, t1, t2, t3)
    for x in range(NX):

        @pl.when(place[1] == x)
        def _(x=x):
            def one(i, _):
                total = tables[x % NX][i]
                for j in range(1, NX):
                    total = joined(total, tables[(x - j) % NX][i])
                out[i] = total
                return 0

            lax.fori_loop(0, CHUNK, one, 0)


def plane_kernel(rows, out):
    total = rows[0]
    for z in range(1, NZ):
        total = joined(total, rows[z])
    out[...] = total


def rows_back_kernel(place, rows, planes, out):
    state = jnp.zeros((ROWS, LANES), F32)
    for y in range(planes.shape[0] - 1):
        state = jnp.where(y < place[2], joined(state, planes[y]), state)
    for z in range(NZ):
        out[z] = state
        if z < NZ - 1:
            state = joined(state, rows[z])


def chips_back_kernel(place, came, t0, t1, t2, t3, *outs):
    tables = (t0, t1, t2, t3)
    for x in range(NX):

        @pl.when(place[1] == x)
        def _(x=x):
            def one(i, _):
                state = came[i]
                for j in range(NX):
                    k = (x - j) % NX
                    outs[k][i] = state
                    if j < NX - 1:
                        state = joined(state, tables[k][i])
                return 0

            lax.fori_loop(0, CHUNK, one, 0)


def cores_back_kernel(place, p0, p1, p2, p3, mine, got, keep, send):
    parts = (p0, p1, p2, p3)
    first, x = place[0] == 0, place[1]
    for k in range(NX):
        base = lax.rem(x + k, NX) * CHUNK

        def one(i, _, k=k, base=base):
            state = parts[k][i]
            second = joined(state, jnp.where(first, mine[base + i], got[base + i]))
            keep[base + i] = jnp.where(first, state, second)
            send[base + i] = jnp.where(first, second, state)
            return 0

        lax.fori_loop(0, CHUNK, one, 0)


def finish_kernel(
    place, users, run, count, is_open, home, account, mine, got, out, table, picked, sems
):
    half_of = place[0]
    copies = [
        pltpu.make_async_copy(mine, table.at[pl.ds(half_of * HALF, HALF)], sems.at[0]),
        pltpu.make_async_copy(got, table.at[pl.ds((1 - half_of) * HALF, HALF)], sems.at[1]),
    ]
    for copy in copies:
        copy.start()
    for copy in copies:
        copy.wait()
    lines = home.shape[0]
    flat = table.reshape(OWNERS * ROWS, LANES)
    scale = []
    for t in range(lines // 8):
        rows = slice(8 * t, 8 * t + 8)
        home8, account8 = home[rows, :], account[rows, :]

        def owner(o, came):
            row = jnp.broadcast_to(table[o, LANES : LANES + 1, :], (8, LANES))
            return jnp.where(home8 == o, jnp.take_along_axis(row, account8, axis=1), came)

        came = jnp.zeros((8, LANES), F32)
        for o in range(OWNERS):
            came = owner(o, came)
        scale.append(1.0 / (count[rows, :] + is_open[rows, :] * came))
    scale = jnp.concatenate(scale, axis=0)
    if lines < LANES:
        scale = jnp.concatenate([scale, jnp.zeros((LANES - lines, LANES), F32)], axis=0)
    scale = scale.T

    def pick(b, _):
        for j in range(LANES):
            picked[pl.ds(b * LANES + j, 1), :] = flat[pl.ds(users[b, j], 1), :]
        return 0

    lax.fori_loop(0, lines, pick, 0)
    for b in range(lines):
        at = pl.ds(b * LANES, LANES)
        factor = jnp.broadcast_to(scale[:, b : b + 1], (LANES, LANES))
        out[at, :] = (run[at, :] + picked[at, :]) * factor


def ring(n, k):
    return [(i, (i + k) % n) for i in range(n)]


def body(features, home, account, flags):
    rows = features.shape[0]
    lines = rows // LANES
    home = home.reshape(lines, LANES)
    account = account.reshape(lines, LANES)
    flags = flags.reshape(lines, LANES)
    place = jnp.stack([lax.axis_index(a).astype(I32) for a in ("c", "x", "y", "z")])
    small = jax.ShapeDtypeStruct((lines, LANES), I32)
    small_f = jax.ShapeDtypeStruct((lines, LANES), F32)
    by_owner = functools.partial(jax.ShapeDtypeStruct, (OWNERS, LANES))
    slot, acc_rows, flag_rows, grouped, other, mine = call(
        regroup_kernel,
        [small, by_owner(I32), by_owner(F32),
         jax.ShapeDtypeStruct((OWNERS * LANES, LANES), F32), block(HALF), block(HALF)],
        (place, home, account, flags, features),
        [SMEM, VMEM, VMEM, VMEM, VMEM],
        scratch=[pltpu.SMEM((lines, LANES), I32), pltpu.SemaphoreType.DMA],
        cost=10_000_000_000,
    )
    swap = ring(NC, 1)
    got = lax.ppermute(other, "c", swap)
    run, count, is_open, users = call(
        running_kernel,
        [jax.ShapeDtypeStruct((rows, LANES), F32), small_f, small_f, small],
        (slot, slot, home, account, acc_rows, flag_rows, grouped),
        [SMEM] + [VMEM] * 6,
        scratch=[pltpu.VMEM((OWNERS * LANES, LANES), F32), pltpu.VMEM((OWNERS, LANES), F32),
                 pltpu.VMEM((OWNERS, LANES), F32)],
        cost=20_000_000_000,
    )
    chunks = call(core_kernel, [block(CHUNK)] * NX, (place, mine, got), [SMEM, VMEM, VMEM])
    tables = [chunks[0]] + [lax.ppermute(chunks[k], "x", ring(NX, k)) for k in range(1, NX)]
    row_total = call(row_kernel, block(CHUNK), (place, *tables), [SMEM] + [VMEM] * NX)
    row_totals = lax.all_to_all(row_total, "z", 0, 0, tiled=True)
    plane_total = call(plane_kernel, block(), (row_totals,), [VMEM])
    planes = lax.all_gather(plane_total, "y", axis=0)
    came = call(
        rows_back_kernel, block(NZ), (place, row_totals, planes), [SMEM, VMEM, VMEM]
    )
    came = lax.all_to_all(came, "z", 0, 0, tiled=True)
    parts = call(
        chips_back_kernel, [block(CHUNK)] * NX, (place, came, *tables), [SMEM] + [VMEM] * (NX + 1)
    )
    parts = [parts[0]] + [lax.ppermute(parts[k], "x", ring(NX, -k)) for k in range(1, NX)]
    keep, send = call(
        cores_back_kernel, [block(HALF)] * 2, (place, *parts, mine, got), [SMEM] + [VMEM] * (NX + 2)
    )
    last = lax.ppermute(send, "c", swap)
    anywhere = pl.BlockSpec(memory_space=pl.ANY)
    return call(
        finish_kernel,
        jax.ShapeDtypeStruct((rows, LANES), F32),
        (place, users, run, count, is_open, home, account, keep, last),
        [SMEM, SMEM] + [VMEM] * 5 + [anywhere] * 2,
        scratch=[pltpu.VMEM((OWNERS, ROWS, LANES), F32), pltpu.VMEM((rows, LANES), F32),
                 pltpu.SemaphoreType.DMA((2,))],
    )


def solution(mesh):
    split = Mesh(mesh.devices.reshape(-1, NZ, NX, NC), ("y", "z", "x", "c"))
    axes = ("y", "z", "x", "c")
    return jax.shard_map(
        body,
        mesh=split,
        in_specs=(P(axes, None), P(axes, None), P(axes), P(axes)),
        out_specs=P(axes, None),
        check_vma=False,
    )
```

```python
import functools

import jax
import jax.numpy as jnp
from jax import lax
from jax.experimental import pallas as pl
from jax.experimental.pallas import tpu as pltpu
from jax.sharding import Mesh, PartitionSpec as P

LANES = 128
GROUPS = 1
PART = LANES // GROUPS
ROWS = PART + 8
NZ, NX, NC = 8, 4, 2
OWNERS = NZ * NX * NC
HALF = OWNERS // NC
CHUNK = HALF // NX
BF16, F32, I32 = jnp.bfloat16, jnp.float32, jnp.int32
VMEM = pl.BlockSpec(memory_space=pltpu.VMEM)
SMEM = pl.BlockSpec(memory_space=pltpu.SMEM)
HBM = pl.BlockSpec(memory_space=pltpu.HBM)
ANY = pl.BlockSpec(memory_space=pl.ANY)


def dot(a, b):
    return lax.dot_general(a, b, (((1,), (0,)), ((), ())), preferred_element_type=F32)


def dot_nt(a, b):
    return lax.dot_general(a, b, (((1,), (1,)), ((), ())), preferred_element_type=F32)


def iota(shape, dim):
    return lax.broadcasted_iota(I32, shape, dim)


def as_bf16(mask):
    return jnp.where(mask, 1.0, 0.0).astype(BF16)


def two_parts(v):
    high = v.astype(BF16)
    low = (v - high.astype(F32)).astype(BF16)
    return jnp.concatenate([high, low], axis=1)


def masked_sum(mask, parts):
    both = dot(mask, parts)
    return both[:, :LANES] + both[:, LANES:]


def call(kernel, out, args, specs, out_specs=None, scratch=(), cost=1_000_000, limit=24):
    return pl.pallas_call(
        kernel,
        out_shape=out,
        in_specs=specs,
        out_specs=out_specs or jax.tree.map(lambda _: VMEM, out),
        scratch_shapes=list(scratch),
        cost_estimate=pl.CostEstimate(flops=cost, bytes_accessed=1_000_000, transcendentals=0),
        compiler_params=pltpu.CompilerParams(vmem_limit_bytes=limit << 20),
    )(*args)


def block(*lead):
    return jax.ShapeDtypeStruct((*lead, ROWS, LANES), F32)


def regroup_kernel(
    events, features_in, slot_out, acc_out, flag_out, grouped, features, slots, sems,
):
    arrival = pltpu.make_async_copy(features_in, features, sems.at[0])
    arrival.start()
    lines = slot_out.shape[0]
    zero = jnp.zeros((LANES, LANES), F32)
    below = as_bf16(iota((LANES, LANES), 0) < iota((LANES, LANES), 1))
    with_total = jnp.concatenate([below, jnp.ones((LANES, LANES), BF16)], axis=1)
    owner_ids = iota((OWNERS, LANES), 0)
    before = jnp.zeros((OWNERS, LANES), F32)
    codes = jnp.zeros((OWNERS, LANES), F32)
    each = grouped.shape[0] // LANES // lines
    for b in range(lines):
        home_row = events[b : b + 1, :]
        account_row = events[lines + b : lines + b + 1, :]
        flag_row = events[2 * lines + b : 2 * lines + b + 1, :]
        chosen = owner_ids == home_row
        counted = dot(as_bf16(chosen), with_total)
        rank = jnp.sum(
            jnp.where(chosen, counted[:, :LANES] + before, 0.0), axis=0, keepdims=True
        )
        before = before + counted[:, LANES:]
        slot_out[b : b + 1, :] = home_row * LANES + rank.astype(I32)
        code = (account_row * 2 + flag_row + 1).astype(F32)
        rank_of = as_bf16(iota((LANES, LANES), 0) == rank.astype(I32))
        codes = codes + dot_nt(jnp.where(chosen, code, 0.0).astype(BF16), rank_of)
        for i in range(each):
            grouped[(b * each + i) * LANES : (b * each + i + 1) * LANES, :] = zero
    copy = pltpu.make_async_copy(slot_out, slots, sems.at[1])
    copy.start()
    code_ids = codes.astype(I32) - 1
    acc_out[...] = jnp.right_shift(code_ids, 1)
    flag_out[...] = jnp.where(code_ids >= 0, jnp.bitwise_and(code_ids, 1), 0).astype(F32)
    arrival.wait()
    copy.wait()

    def spread(b, _):
        for j in range(LANES):
            grouped[pl.ds(slots[b, j], 1), :] = features[pl.ds(b * LANES + j, 1), :]
        return 0

    lax.fori_loop(0, lines, spread, 0)


def closing_kernel(k, place, acc_rows, flag_rows, grouped, ready, other, mine):
    after = as_bf16(iota((LANES, LANES), 0) > iota((LANES, LANES), 1))
    ones = jnp.ones((8, LANES), BF16)
    sub = iota((8, LANES), 0)
    chunk = lax.rem(place[1] + k, NX) * CHUNK
    for out, half_of in ((other, 1 - place[0]), (mine, place[0])):
        base = pl.multiple_of(half_of * HALF + chunk, CHUNK)
        acc8 = acc_rows[pl.ds(base, CHUNK), :]
        flag8 = flag_rows[pl.ds(base, CHUNK), :]
        for i in range(CHUNK):
            member = iota((LANES, LANES), 0) == acc8[i : i + 1, :]
            member_flags = jnp.where(member, flag8[i : i + 1, :], 0.0).astype(BF16)
            later_flags = dot(member_flags, after)
            counted = as_bf16(member & (later_flags < 0.5))
            at = pl.multiple_of((base + i) * LANES, LANES)
            sums = masked_sum(counted, two_parts(grouped[pl.ds(at, LANES), :]))
            count = dot_nt(ones, counted)
            mark = jnp.minimum(dot_nt(ones, member_flags), 1.0)
            tail = jnp.where(sub == 0, count, jnp.where(sub == 1, mark, 0.0))
            for g in range(GROUPS):
                out[g, i, :PART, :] = sums[g * PART : (g + 1) * PART, :]
                out[g, i, PART:, :] = tail


def running_kernel(
    slots, slot_rows, home, account, acc_rows, flag_rows, grouped,
    ready, run_out, count_out, open_out, user_out, run, counts, opens,
):
    lines = home.shape[0]
    after = as_bf16(iota((LANES, LANES), 0) > iota((LANES, LANES), 1))
    up_to = iota((LANES, LANES), 1) <= iota((LANES, LANES), 0)
    ones = jnp.ones((8, LANES), BF16)

    def some(g, _):
        rows = pl.ds(pl.multiple_of(g * 8, 8), 8)
        acc8 = acc_rows[rows, :]
        flag8 = flag_rows[rows, :]
        acc_cols = acc8.astype(F32).T
        count8, open8 = [], []
        for i in range(8):
            acc_row = acc8[i : i + 1, :].astype(F32)
            acc_col = jnp.broadcast_to(acc_cols[:, i : i + 1], (LANES, LANES))
            same = (acc_col == acc_row) & (acc_row >= 0.0) & up_to
            same_flags = jnp.where(same, flag8[i : i + 1, :], 0.0).astype(BF16)
            between = dot(same_flags, after)
            session = as_bf16(same & (between < 0.5))
            at = pl.ds(pl.multiple_of((g * 8 + i) * LANES, LANES), LANES)
            run[at, :] = masked_sum(session, two_parts(grouped[at, :]))
            count8.append(dot_nt(ones, session)[:1, :])
            open8.append(dot_nt(ones, same_flags)[:1, :])
        counts[rows, :] = jnp.concatenate(count8, axis=0)
        opens[rows, :] = jnp.where(jnp.concatenate(open8, axis=0) < 0.5, 1.0, 0.0)
        return 0

    lax.fori_loop(0, OWNERS // 8, some, 0)

    def scalars(t, _):
        rows = pl.ds(pl.multiple_of(t * 8, 8), 8)
        home8 = home[rows, :]
        rank = slot_rows[rows, :] - home8 * LANES
        count = jnp.zeros((8, LANES), F32)
        is_open = jnp.zeros((8, LANES), F32)
        for o in range(OWNERS):
            here = home8 == o
            for_count = jnp.broadcast_to(counts[o : o + 1, :], (8, LANES))
            for_open = jnp.broadcast_to(opens[o : o + 1, :], (8, LANES))
            count = jnp.where(here, jnp.take_along_axis(for_count, rank, axis=1), count)
            is_open = jnp.where(here, jnp.take_along_axis(for_open, rank, axis=1), is_open)
        count_out[rows, :] = count
        open_out[rows, :] = is_open
        account8 = account[rows, :]
        group = account8 // PART
        row = jnp.where(is_open > 0.5, account8 - group * PART, ROWS - 1)
        user_out[rows, :] = (group * OWNERS + home8) * ROWS + row
        return 0

    lax.fori_loop(0, lines // 8, scalars, 0)

    def collect(b, _):
        for j in range(LANES):
            run_out[pl.ds(b * LANES + j, 1), :] = run[pl.ds(slots[b, j], 1), :]
        return 0

    lax.fori_loop(0, lines, collect, 0)


def keeps(blocks):
    marks = jnp.concatenate([b[PART + 1 : PART + 2, :] for b in blocks], axis=0)
    return (1.0 - marks).T


def joined(group, earlier, later, keep):
    keep = keep[group * PART : (group + 1) * PART, :]
    sums = later[:PART, :] + jnp.broadcast_to(keep, (PART, LANES)) * earlier[:PART, :]
    tail, first = later[PART:, :], earlier[PART:, :]
    mark = tail[1:2, :]
    sub = iota((8, LANES), 0)
    tail = jnp.where(
        sub == 0, tail + (1.0 - mark) * first, jnp.where(sub == 1, jnp.maximum(tail, first), 0.0)
    )
    return jnp.concatenate([sums, tail], axis=0)


def core_kernel(place, mine, got, *outs):
    first = place[0] == 0
    for g in range(GROUPS):
        pairs = [(mine[g, i], got[g, i]) for i in range(CHUNK)]
        early = [jnp.where(first, a, b) for a, b in pairs]
        late = [jnp.where(first, b, a) for a, b in pairs]
        keep = keeps(late)
        for i in range(CHUNK):
            outs[g][i] = joined(g, early[i], late[i], keep[:, i : i + 1])


def row_kernel(group, place, t0, t1, t2, t3, out):
    tables = (t0, t1, t2, t3)
    for x in range(NX):

        @pl.when(place[1] == x)
        def _(x=x):
            order = [tables[(x - j) % NX] for j in range(NX)]
            keep = [None] + [keeps([t[i] for i in range(CHUNK)]) for t in order[1:]]
            for i in range(CHUNK):
                total = order[0][i]
                for j in range(1, NX):
                    total = joined(group, total, order[j][i], keep[j][:, i : i + 1])
                out[i] = total


def plane_kernel(*refs):
    out = refs[-1]
    for g in range(GROUPS):
        rows = refs[g]
        keep = keeps([rows[z] for z in range(NZ)])
        total = rows[0]
        for z in range(1, NZ):
            total = joined(g, total, rows[z], keep[:, z : z + 1])
        out[g] = total


def rows_back_kernel(place, *refs):
    planes = refs[:3]
    for g in range(GROUPS):
        rows, out = refs[3 + g], refs[3 + GROUPS + g]
        keep = keeps([planes[r][g] for r in range(3)] + [rows[z] for z in range(5)])
        keep_rest = keeps([rows[z] for z in range(8)])
        state = jnp.zeros((ROWS, LANES), F32)
        for r in range(2, -1, -1):
            more = joined(g, state, planes[r][g], keep[:, r : r + 1])
            state = jnp.where(place[2] > r, more, state)
        for z in range(NZ):
            out[z] = state
            if z < NZ - 1:
                state = joined(g, state, rows[z], keep_rest[:, z : z + 1])


def chips_back_kernel(group, place, came, t0, t1, t2, t3, *outs):
    tables = (t0, t1, t2, t3)
    for x in range(NX):

        @pl.when(place[1] == x)
        def _(x=x):
            order = [(x - j) % NX for j in range(NX)]
            keep = [keeps([tables[k][i] for i in range(CHUNK)]) for k in order[:-1]]
            for i in range(CHUNK):
                state = came[i]
                for j, k in enumerate(order):
                    outs[k][i] = state
                    if j < NX - 1:
                        state = joined(group, state, tables[k][i], keep[j][:, i : i + 1])


def cores_back_kernel(group, place, ready, *refs):
    parts, mine, got = refs[:NX], refs[NX : 2 * NX], refs[2 * NX : 3 * NX]
    keep_out, send = refs[3 * NX :]
    first = place[0] == 0
    for k in range(NX):
        base = lax.rem(place[1] + k, NX) * CHUNK
        early = [jnp.where(first, mine[k][group, i], got[k][group, i]) for i in range(CHUNK)]
        keep = keeps(early)
        for i in range(CHUNK):
            state = parts[k][i]
            second = joined(group, state, early[i], keep[:, i : i + 1])
            keep_out[base + i] = jnp.where(first, state, second)
            send[base + i] = jnp.where(first, second, state)


def finish_kernel(place, users, run, count, is_open, home, account, *refs):
    keep, got = refs[:GROUPS], refs[GROUPS : 2 * GROUPS]
    out, table, picked, sems = refs[2 * GROUPS :]
    bases = (place[0] * HALF, (1 - place[0]) * HALF)
    copies = [
        pltpu.make_async_copy(
            side[g], table.at[pl.ds(g * OWNERS + bases[s], HALF)], sems.at[2 * g + s]
        )
        for g in range(GROUPS)
        for s, side in enumerate((keep, got))
    ]
    for copy in copies:
        copy.start()
    lines = home.shape[0]
    flat = table.reshape(GROUPS * OWNERS * ROWS, LANES)
    scale = []
    for t in range(lines // 8):
        rows = slice(8 * t, 8 * t + 8)
        home8, account8 = home[rows, :], account[rows, :]
        came = jnp.zeros((8, LANES), F32)
        for s, side in enumerate((keep[0], got[0])):
            for i in range(HALF):
                row = jnp.broadcast_to(side[i, PART : PART + 1, :], (8, LANES))
                found = jnp.take_along_axis(row, account8, axis=1)
                came = jnp.where(home8 == bases[s] + i, found, came)
        scale.append(1.0 / (count[rows, :] + is_open[rows, :] * came))
    scale = jnp.concatenate(scale, axis=0)
    if lines < LANES:
        scale = jnp.concatenate([scale, jnp.zeros((LANES - lines, LANES), F32)], axis=0)
    scale = scale.T
    for copy in copies:
        copy.wait()

    def pick(b, _):
        for j in range(LANES):
            picked[pl.ds(b * LANES + j, 1), :] = flat[pl.ds(users[b, j], 1), :]
        return 0

    lax.fori_loop(0, lines, pick, 0)
    for b in range(lines):
        at = pl.ds(b * LANES, LANES)
        factor = jnp.broadcast_to(scale[:, b : b + 1], (LANES, LANES))
        out[at, :] = (run[at, :] + picked[at, :]) * factor


def ring(n, k):
    return [(i, (i + k) % n) for i in range(n)]


def body(features, home, account, flags):
    rows = features.shape[0]
    lines = rows // LANES
    home = home.reshape(lines, LANES)
    account = account.reshape(lines, LANES)
    flags = flags.reshape(lines, LANES)
    place = jnp.stack([lax.axis_index(a).astype(I32) for a in ("c", "x", "y")])
    small = jax.ShapeDtypeStruct((lines, LANES), I32)
    small_f = jax.ShapeDtypeStruct((lines, LANES), F32)
    by_owner = functools.partial(jax.ShapeDtypeStruct, (OWNERS, LANES))
    slot, acc_rows, flag_rows, grouped = call(
        regroup_kernel,
        [small, by_owner(I32), by_owner(F32),
         jax.ShapeDtypeStruct((OWNERS * LANES, LANES), F32)],
        (jnp.concatenate([home, account, flags]), features),
        [VMEM, HBM],
        scratch=[pltpu.VMEM((rows, LANES), F32), pltpu.SMEM((lines, LANES), I32),
                 pltpu.SemaphoreType.DMA((2,))],
        cost=5_000_000_000,
    )
    swap = ring(NC, 1)
    mine, got, tables = [None] * NX, [None] * NX, [[None] * NX for _ in range(GROUPS)]
    order = (2, 1, 3, 0)
    chunks = [None] * NX

    def meet(k):
        chunks[k] = call(core_kernel, [block(CHUNK)] * GROUPS, (place, mine[k], got[k]),
                         [SMEM] + [VMEM] * 2, cost=300_000_000)
        for g in range(GROUPS):
            part = chunks[k][g]
            tables[g][k] = lax.ppermute(part, "x", ring(NX, k)) if k else part

    for at, k in enumerate(order):
        ready = chunks[order[at - 2]][0] if at >= 2 else acc_rows
        other, mine[k] = call(
            functools.partial(closing_kernel, k),
            [block(GROUPS, CHUNK)] * 2,
            (place, acc_rows, flag_rows, grouped, ready),
            [SMEM] + [VMEM] * 3 + [ANY],
            cost=1_500_000_000,
        )
        got[k] = lax.ppermute(other, "c", swap)
        if at:
            meet(order[at - 1])
    meet(order[-1])
    row_totals = []
    for g in range(GROUPS):
        total = call(functools.partial(row_kernel, g), block(CHUNK), (place, *tables[g]),
                     [SMEM] + [VMEM] * NX)
        row_totals.append(lax.all_to_all(total, "z", 0, 0, tiled=True))
    plane = call(plane_kernel, block(GROUPS), tuple(row_totals), [VMEM] * GROUPS)
    ny = lax.axis_size("y")
    planes = [
        lax.ppermute(plane, "y", [(i, i + r) for i in range(ny - r)]) for r in range(1, ny)
    ]
    came = call(rows_back_kernel, [block(NZ)] * GROUPS, (place, *planes, *row_totals),
                [SMEM] + [VMEM] * (3 + GROUPS))
    parts = []
    for g in range(GROUPS):
        mid = lax.all_to_all(came[g], "z", 0, 0, tiled=True)
        part = call(functools.partial(chips_back_kernel, g), [block(CHUNK)] * NX,
                    (place, mid, *tables[g]), [SMEM] + [VMEM] * (NX + 1))
        parts.append(
            [lax.ppermute(part[k], "x", ring(NX, -k)) if k else part[k] for k in range(NX)]
        )
    run, count, is_open, users = call(
        running_kernel,
        [jax.ShapeDtypeStruct((rows, LANES), F32), small_f, small_f, small],
        (slot, slot, home, account, acc_rows, flag_rows, grouped, parts[-1][0]),
        [SMEM] + [VMEM] * 6 + [ANY],
        scratch=[pltpu.VMEM((OWNERS * LANES, LANES), F32), pltpu.VMEM((OWNERS, LANES), F32),
                 pltpu.VMEM((OWNERS, LANES), F32)],
        cost=20_000_000_000,
    )
    keep, last = [], []
    for g in range(GROUPS):
        stay, send = call(
            functools.partial(cores_back_kernel, g), [block(HALF)] * 2,
            (place, count, *parts[g], *mine, *got), [SMEM, ANY] + [VMEM] * (3 * NX)
        )
        keep.append(stay)
        last.append(lax.ppermute(send, "c", swap))
    return call(
        finish_kernel,
        jax.ShapeDtypeStruct((rows, LANES), F32),
        (place, users, run, count, is_open, home, account, *keep, *last),
        [SMEM, SMEM] + [VMEM] * (5 + 2 * GROUPS),
        scratch=[pltpu.VMEM((GROUPS * OWNERS, ROWS, LANES), F32), pltpu.VMEM((rows, LANES), F32),
                 pltpu.SemaphoreType.DMA((2 * GROUPS,))],
    )


def solution(mesh):
    split = Mesh(mesh.devices.reshape(-1, NZ, NX, NC), ("y", "z", "x", "c"))
    axes = ("y", "z", "x", "c")
    return jax.shard_map(
        body,
        mesh=split,
        in_specs=(P(axes, None), P(axes, None), P(axes), P(axes)),
        out_specs=P(axes, None),
        check_vma=False,
    )
```

```python
import functools

import jax
import jax.numpy as jnp
from jax import lax
from jax.experimental import pallas as pl
from jax.experimental.pallas import tpu as pltpu
from jax.sharding import Mesh, PartitionSpec as P


LANES = 128
GROUPS = 2
PART = LANES // GROUPS
ROWS = PART + 8
NZ, NX, NC = 8, 4, 2
OWNERS = NZ * NX * NC
HALF = OWNERS // NC
CHUNK = HALF // NX
BF16, F32, I32 = jnp.bfloat16, jnp.float32, jnp.int32
VMEM = pl.BlockSpec(memory_space=pltpu.VMEM)
SMEM = pl.BlockSpec(memory_space=pltpu.SMEM)
HBM = pl.BlockSpec(memory_space=pltpu.HBM)
ANY = pl.BlockSpec(memory_space=pl.ANY)


def dot(a, b):
    return lax.dot_general(a, b, (((1,), (0,)), ((), ())), preferred_element_type=F32)


def dot_nt(a, b):
    return lax.dot_general(a, b, (((1,), (1,)), ((), ())), preferred_element_type=F32)


def iota(shape, dim):
    return lax.broadcasted_iota(I32, shape, dim)


def as_bf16(mask):
    return jnp.where(mask, 1.0, 0.0).astype(BF16)


def two_parts(v):
    high = v.astype(BF16)
    low = (v - high.astype(F32)).astype(BF16)
    return jnp.concatenate([high, low], axis=1)


def masked_sum(mask, parts):
    both = dot(mask, parts)
    return both[:, :LANES] + both[:, LANES:]


def call(kernel, out, args, specs, out_specs=None, scratch=(), cost=1_000_000, limit=24, aliases=None):
    return pl.pallas_call(
        kernel,
        out_shape=out,
        in_specs=specs,
        out_specs=out_specs or jax.tree.map(lambda _: VMEM, out),
        scratch_shapes=list(scratch),
        input_output_aliases=aliases or {},
        cost_estimate=pl.CostEstimate(flops=cost, bytes_accessed=1_000_000, transcendentals=0),
        compiler_params=pltpu.CompilerParams(vmem_limit_bytes=limit << 20),
    )(*args)


def block(*lead):
    return jax.ShapeDtypeStruct((*lead, ROWS, LANES), F32)


def rank_kernel(events, slot_out, acc_out, flag_out, cleared):
    lines = slot_out.shape[0]
    zero = jnp.zeros((LANES, LANES), F32)
    below = as_bf16(iota((LANES, LANES), 0) < iota((LANES, LANES), 1))
    with_total = jnp.concatenate([below, jnp.ones((LANES, LANES), BF16)], axis=1)
    owner_ids = iota((OWNERS, LANES), 0)
    before = jnp.zeros((OWNERS, LANES), F32)
    codes = jnp.zeros((OWNERS, LANES), F32)
    each = cleared.shape[0] // LANES // lines
    for b in range(lines):
        home_row = events[b : b + 1, :]
        account_row = events[lines + b : lines + b + 1, :]
        flag_row = events[2 * lines + b : 2 * lines + b + 1, :]
        chosen = owner_ids == home_row
        counted = dot(as_bf16(chosen), with_total)
        rank = jnp.sum(
            jnp.where(chosen, counted[:, :LANES] + before, 0.0), axis=0, keepdims=True
        )
        before = before + counted[:, LANES:]
        slot_out[b : b + 1, :] = home_row * LANES + rank.astype(I32)
        code = (account_row * 2 + flag_row + 1).astype(F32)
        rank_of = as_bf16(iota((LANES, LANES), 0) == rank.astype(I32))
        codes = codes + dot_nt(jnp.where(chosen, code, 0.0).astype(BF16), rank_of)
        for i in range(each):
            cleared[(b * each + i) * LANES : (b * each + i + 1) * LANES, :] = zero
    code_ids = codes.astype(I32) - 1
    acc_out[...] = jnp.right_shift(code_ids, 1)
    flag_out[...] = jnp.where(code_ids >= 0, jnp.bitwise_and(code_ids, 1), 0).astype(F32)


def spread_kernel(slot_rows, features, cleared, grouped, slots, sem):
    copy = pltpu.make_async_copy(slot_rows, slots, sem)
    copy.start()
    copy.wait()

    def spread(b, _):
        for j in range(LANES):
            grouped[pl.ds(slots[b, j], 1), :] = features[pl.ds(b * LANES + j, 1), :]
        return 0

    lax.fori_loop(0, slot_rows.shape[0], spread, 0)


def after_and_ones():
    after = as_bf16(iota((LANES, LANES), 0) > iota((LANES, LANES), 1))
    return jnp.concatenate([after, jnp.ones((LANES, LANES), BF16)], axis=1)


def cut(v, i):
    return v[i * LANES : (i + 1) * LANES, :]


def counted_rows(counted, flagged):
    count = dot(jnp.concatenate(counted, axis=0), jnp.ones((LANES, LANES), BF16))
    lane = iota((LANES, LANES), 1)
    both = jnp.zeros((LANES, LANES), F32)
    for i in range(8):
        both = jnp.where(lane == i, cut(count, i), both)
        both = jnp.where(lane == 8 + i, cut(flagged, i), both)
    return both.T


def closing_kernel(k, place, acc_rows, flag_rows, grouped, ready, other, mine):
    sub = iota((8, LANES), 0)
    sides = after_and_ones()
    chunk = lax.rem(place[1] + k, NX) * CHUNK
    for out, half_of in ((other, 1 - place[0]), (mine, place[0])):
        base = pl.multiple_of(half_of * HALF + chunk, CHUNK)
        acc8 = acc_rows[pl.ds(base, CHUNK), :]
        flag8 = flag_rows[pl.ds(base, CHUNK), :]
        member = [iota((LANES, LANES), 0) == acc8[i : i + 1, :] for i in range(CHUNK)]
        member_flags = [
            jnp.where(member[i], flag8[i : i + 1, :], 0.0).astype(BF16) for i in range(CHUNK)
        ]
        flagged = dot(jnp.concatenate(member_flags, axis=0), sides)
        counted = [
            as_bf16(member[i] & (cut(flagged, i)[:, :LANES] < 0.5)) for i in range(CHUNK)
        ]
        rows = counted_rows(counted, flagged[:, LANES:])
        for i in range(CHUNK):
            at = pl.multiple_of((base + i) * LANES, LANES)
            sums = masked_sum(counted[i], two_parts(grouped[pl.ds(at, LANES), :]))
            mark = jnp.minimum(rows[8 + i : 9 + i, :], 1.0)
            tail = jnp.where(sub == 0, rows[i : i + 1, :], jnp.where(sub == 1, mark, 0.0))
            for g in range(GROUPS):
                out[g, i, :PART, :] = sums[g * PART : (g + 1) * PART, :]
                out[g, i, PART:, :] = tail


def running_kernel(acc_rows, flag_rows, grouped, ready, run, counts, opens):
    sides = after_and_ones()
    up_to = iota((LANES, LANES), 1) <= iota((LANES, LANES), 0)

    def some(g, _):
        rows = pl.ds(pl.multiple_of(g * 8, 8), 8)
        acc8 = acc_rows[rows, :].astype(F32)
        flag8 = flag_rows[rows, :]
        acc_cols = acc8.T
        same = []
        for i in range(8):
            acc_col = jnp.broadcast_to(acc_cols[:, i : i + 1], (LANES, LANES))
            same.append((acc_col == acc8[i : i + 1, :]) & (acc_col >= 0.0) & up_to)
        same_flags = [
            jnp.where(same[i], flag8[i : i + 1, :], 0.0).astype(BF16) for i in range(8)
        ]
        flagged = dot(jnp.concatenate(same_flags, axis=0), sides)
        session = [as_bf16(same[i] & (cut(flagged, i)[:, :LANES] < 0.5)) for i in range(8)]
        for i in range(8):
            at = pl.ds(pl.multiple_of((g * 8 + i) * LANES, LANES), LANES)
            run[at, :] = masked_sum(session[i], two_parts(grouped[at, :]))
        found = counted_rows(session, flagged[:, LANES:])
        counts[rows, :] = found[:8, :]
        opens[rows, :] = jnp.where(found[8:16, :] < 0.5, 1.0, 0.0)
        return 0

    lax.fori_loop(0, OWNERS // 8, some, 0)


def in_time_kernel(
    slots, slot_rows, home, account, run, counts, opens, ready,
    run_out, count_out, open_out, user_out,
):
    lines = home.shape[0]

    def scalars(t, _):
        rows = pl.ds(pl.multiple_of(t * 8, 8), 8)
        home8 = home[rows, :]
        rank = slot_rows[rows, :] - home8 * LANES
        count = jnp.zeros((8, LANES), F32)
        is_open = jnp.zeros((8, LANES), F32)
        for o in range(OWNERS):
            here = home8 == o
            for_count = jnp.broadcast_to(counts[o : o + 1, :], (8, LANES))
            for_open = jnp.broadcast_to(opens[o : o + 1, :], (8, LANES))
            count = jnp.where(here, jnp.take_along_axis(for_count, rank, axis=1), count)
            is_open = jnp.where(here, jnp.take_along_axis(for_open, rank, axis=1), is_open)
        count_out[rows, :] = count
        open_out[rows, :] = is_open
        account8 = account[rows, :]
        group = account8 // PART
        row = jnp.where(is_open > 0.5, account8 - group * PART, ROWS - 1)
        user_out[rows, :] = (group * OWNERS + home8) * ROWS + row
        return 0

    lax.fori_loop(0, lines // 8, scalars, 0)

    def collect(b, _):
        for j in range(LANES):
            run_out[pl.ds(b * LANES + j, 1), :] = run[pl.ds(slots[b, j], 1), :]
        return 0

    lax.fori_loop(0, lines, collect, 0)


def keeps(blocks):
    marks = jnp.concatenate([b[PART + 1 : PART + 2, :] for b in blocks], axis=0)
    return (1.0 - marks).T


def joined(group, earlier, later, keep):
    keep = keep[group * PART : (group + 1) * PART, :]
    sums = later[:PART, :] + jnp.broadcast_to(keep, (PART, LANES)) * earlier[:PART, :]
    tail, first = later[PART:, :], earlier[PART:, :]
    mark = tail[1:2, :]
    sub = iota((8, LANES), 0)
    tail = jnp.where(
        sub == 0, tail + (1.0 - mark) * first, jnp.where(sub == 1, jnp.maximum(tail, first), 0.0)
    )
    return jnp.concatenate([sums, tail], axis=0)


def core_kernel(group, place, mine, got, ready, out):
    first = place[0] == 0
    pairs = [(mine[group, i], got[group, i]) for i in range(CHUNK)]
    early = [jnp.where(first, a, b) for a, b in pairs]
    late = [jnp.where(first, b, a) for a, b in pairs]
    keep = keeps(late)
    for i in range(CHUNK):
        out[i] = joined(group, early[i], late[i], keep[:, i : i + 1])


def row_kernel(group, place, t0, t1, t2, t3, ready, out):
    tables = (t0, t1, t2, t3)
    for x in range(NX):

        @pl.when(place[1] == x)
        def _(x=x):
            order = [tables[(x - j) % NX] for j in range(NX)]
            keep = [None] + [keeps([t[i] for i in range(CHUNK)]) for t in order[1:]]
            for i in range(CHUNK):
                total = order[0][i]
                for j in range(1, NX):
                    total = joined(group, total, order[j][i], keep[j][:, i : i + 1])
                out[i] = total


def touch_kernel(rows, out):
    out[...] = rows[0, :8, :]


def plane_kernel(*refs):
    out = refs[-1]
    for g in range(GROUPS):
        rows = refs[g]
        keep = keeps([rows[z] for z in range(NZ)])
        total = rows[0]
        for z in range(1, NZ):
            total = joined(g, total, rows[z], keep[:, z : z + 1])
        out[g] = total


def rows_back_kernel(group, place, p1, p2, p3, rows, ready, out):
    planes = (p1, p2, p3)
    keep_planes = keeps([p[group] for p in planes] + [rows[z] for z in range(5)])
    keep = keeps([rows[z] for z in range(NZ)])
    state = jnp.zeros((ROWS, LANES), F32)
    for r in range(2, -1, -1):
        more = joined(group, state, planes[r][group], keep_planes[:, r : r + 1])
        state = jnp.where(place[2] > r, more, state)
    for z in range(NZ):
        out[z] = state
        if z < NZ - 1:
            state = joined(group, state, rows[z], keep[:, z : z + 1])


def chips_back_kernel(group, place, came, t0, t1, t2, t3, *outs):
    tables = (t0, t1, t2, t3)
    for x in range(NX):

        @pl.when(place[1] == x)
        def _(x=x):
            order = [(x - j) % NX for j in range(NX)]
            keep = [keeps([tables[k][i] for i in range(CHUNK)]) for k in order[:-1]]
            for i in range(CHUNK):
                state = came[i]
                for j, k in enumerate(order):
                    outs[k][i] = state
                    if j < NX - 1:
                        state = joined(group, state, tables[k][i], keep[j][:, i : i + 1])


def cores_back_kernel(group, place, ready, *refs):
    parts, mine, got = refs[:NX], refs[NX : 2 * NX], refs[2 * NX : 3 * NX]
    keep_out, send = refs[3 * NX :]
    first = place[0] == 0
    for k in range(NX):
        base = lax.rem(place[1] + k, NX) * CHUNK
        early = [jnp.where(first, mine[k][group, i], got[k][group, i]) for i in range(CHUNK)]
        keep = keeps(early)
        for i in range(CHUNK):
            state = parts[k][i]
            second = joined(group, state, early[i], keep[:, i : i + 1])
            keep_out[base + i] = jnp.where(first, state, second)
            send[base + i] = jnp.where(first, second, state)


def finish_kernel(place, users, run, count, is_open, home, account, *refs):
    keep, got = refs[:GROUPS], refs[GROUPS : 2 * GROUPS]
    out, table, picked, sems = refs[2 * GROUPS :]
    bases = (place[0] * HALF, (1 - place[0]) * HALF)
    copies = [
        pltpu.make_async_copy(
            side[g], table.at[pl.ds(g * OWNERS + bases[s], HALF)], sems.at[2 * g + s]
        )
        for g in range(GROUPS)
        for s, side in enumerate((keep, got))
    ]
    for copy in copies:
        copy.start()
    lines = home.shape[0]
    flat = table.reshape(GROUPS * OWNERS * ROWS, LANES)
    scale = []
    for t in range(lines // 8):
        rows = slice(8 * t, 8 * t + 8)
        home8, account8 = home[rows, :], account[rows, :]
        came = jnp.zeros((8, LANES), F32)
        for s, side in enumerate((keep[0], got[0])):
            for i in range(HALF):
                row = jnp.broadcast_to(side[i, PART : PART + 1, :], (8, LANES))
                found = jnp.take_along_axis(row, account8, axis=1)
                came = jnp.where(home8 == bases[s] + i, found, came)
        scale.append(1.0 / (count[rows, :] + is_open[rows, :] * came))
    scale = jnp.concatenate(scale, axis=0)
    if lines < LANES:
        scale = jnp.concatenate([scale, jnp.zeros((LANES - lines, LANES), F32)], axis=0)
    scale = scale.T
    for copy in copies:
        copy.wait()

    def pick(b, _):
        for j in range(LANES):
            picked[pl.ds(b * LANES + j, 1), :] = flat[pl.ds(users[b, j], 1), :]
        return 0

    lax.fori_loop(0, lines, pick, 0)
    for b in range(lines):
        at = pl.ds(b * LANES, LANES)
        factor = jnp.broadcast_to(scale[:, b : b + 1], (LANES, LANES))
        out[at, :] = (run[at, :] + picked[at, :]) * factor


def ring(n, k):
    return [(i, (i + k) % n) for i in range(n)]


def body(features, home, account, flags):
    rows = features.shape[0]
    lines = rows // LANES
    home = home.reshape(lines, LANES)
    account = account.reshape(lines, LANES)
    flags = flags.reshape(lines, LANES)
    place = jnp.stack([lax.axis_index(a).astype(I32) for a in ("c", "x", "y")])
    small = jax.ShapeDtypeStruct((lines, LANES), I32)
    small_f = jax.ShapeDtypeStruct((lines, LANES), F32)
    by_owner = functools.partial(jax.ShapeDtypeStruct, (OWNERS, LANES))
    by_slot = jax.ShapeDtypeStruct((OWNERS * LANES, LANES), F32)
    slot, acc_rows, flag_rows, cleared = call(
        rank_kernel,
        [small, by_owner(I32), by_owner(F32), by_slot],
        (jnp.concatenate([home, account, flags]),),
        [VMEM],
        cost=2_000_000_000,
    )
    grouped = call(
        spread_kernel,
        by_slot,
        (slot, features, cleared),
        [VMEM] * 3,
        scratch=[pltpu.SMEM((lines, LANES), I32), pltpu.SemaphoreType.DMA],
        cost=4_000_000_000,
        aliases={2: 0},
    )
    swap = ring(NC, 1)
    order = (2, 1, 3, 0)
    mine, got = [None] * NX, [None] * NX
    tables = [[None] * NX for _ in range(GROUPS)]

    def meet(g, k, ready):
        chunk = call(functools.partial(core_kernel, g), block(CHUNK),
                     (place, mine[k], got[k], ready), [SMEM, VMEM, VMEM, ANY], cost=300_000_000)
        tables[g][k] = lax.ppermute(chunk, "x", ring(NX, k)) if k else chunk
        return chunk

    met = []
    for at, k in enumerate(order):
        other, mine[k] = call(
            functools.partial(closing_kernel, k),
            [block(GROUPS, CHUNK)] * 2,
            (place, acc_rows, flag_rows, grouped, met[at - 2] if at >= 2 else acc_rows),
            [SMEM] + [VMEM] * 3 + [ANY],
            cost=1_500_000_000,
        )
        got[k] = lax.ppermute(other, "c", swap)
        if at:
            met.append(meet(0, order[at - 1], acc_rows))
    for g in range(1, GROUPS):
        for k in order[:-1]:
            met.append(meet(g, k, met[-1]))
    for g in range(GROUPS):
        met.append(meet(g, 0, met[-1]))
    run_slots, counts, opens = call(
        running_kernel,
        [by_slot, by_owner(F32), by_owner(F32)],
        (acc_rows, flag_rows, grouped, met[-1]),
        [VMEM] * 3 + [ANY],
        cost=8_000_000_000,
    )
    row_totals = []
    for g in range(GROUPS):
        ready = counts
        if g:
            ready = call(touch_kernel, jax.ShapeDtypeStruct((8, LANES), F32),
                         (row_totals[-1],), [VMEM])
        total = call(functools.partial(row_kernel, g), block(CHUNK),
                     (place, *tables[g], ready), [SMEM] + [VMEM] * NX + [ANY])
        row_totals.append(lax.all_to_all(total, "z", 0, 0, tiled=True))
    plane = call(plane_kernel, block(GROUPS), tuple(row_totals), [VMEM] * GROUPS)
    ny = lax.axis_size("y")
    planes = [
        lax.ppermute(plane, "y", [(i, i + r) for i in range(ny - r)]) for r in range(1, ny)
    ]
    parts = []
    for g in range(GROUPS):
        ready = parts[-1][0] if g else counts
        came = call(functools.partial(rows_back_kernel, g), block(NZ),
                    (place, *planes, row_totals[g], ready), [SMEM] + [VMEM] * 4 + [ANY])
        mid = lax.all_to_all(came, "z", 0, 0, tiled=True)
        part = call(functools.partial(chips_back_kernel, g), [block(CHUNK)] * NX,
                    (place, mid, *tables[g]), [SMEM] + [VMEM] * (NX + 1))
        parts.append(
            [lax.ppermute(part[k], "x", ring(NX, -k)) if k else part[k] for k in range(NX)]
        )
    run, count, is_open, users = call(
        in_time_kernel,
        [jax.ShapeDtypeStruct((rows, LANES), F32), small_f, small_f, small],
        (slot, slot, home, account, run_slots, counts, opens, parts[-1][0]),
        [SMEM] + [VMEM] * 6 + [ANY],
        cost=10_000_000_000,
    )
    keep, last = [], []
    for g in range(GROUPS):
        stay, send = call(
            functools.partial(cores_back_kernel, g), [block(HALF)] * 2,
            (place, count, *parts[g], *mine, *got), [SMEM, ANY] + [VMEM] * (3 * NX)
        )
        keep.append(stay)
        last.append(lax.ppermute(send, "c", swap))
    return call(
        finish_kernel,
        jax.ShapeDtypeStruct((rows, LANES), F32),
        (place, users, run, count, is_open, home, account, *keep, *last),
        [SMEM, SMEM] + [VMEM] * (5 + 2 * GROUPS),
        scratch=[pltpu.VMEM((GROUPS * OWNERS, ROWS, LANES), F32), pltpu.VMEM((rows, LANES), F32),
                 pltpu.SemaphoreType.DMA((2 * GROUPS,))],
    )


def solution(mesh):
    split = Mesh(mesh.devices.reshape(-1, NZ, NX, NC), ("y", "z", "x", "c"))
    axes = ("y", "z", "x", "c")
    return jax.shard_map(
        body,
        mesh=split,
        in_specs=(P(axes, None), P(axes, None), P(axes), P(axes)),
        out_specs=P(axes, None),
        check_vma=False,
    )
```

```python
import functools

import jax
import jax.numpy as jnp
from jax import lax
from jax.experimental import pallas as pl
from jax.experimental.pallas import tpu as pltpu
from jax.sharding import Mesh, PartitionSpec as P


LANES = 128
FOUR = 4
TAIL = FOUR * LANES
ROWS = TAIL + 8
ONE = LANES + 8
NH, NL, NX, NC = 4, 2, 4, 2
OWNERS = NH * NL * NX * NC
HALF = OWNERS // NC
CHUNKS = HALF // FOUR
BF16, F32, I32 = jnp.bfloat16, jnp.float32, jnp.int32
VMEM = pl.BlockSpec(memory_space=pltpu.VMEM)
SMEM = pl.BlockSpec(memory_space=pltpu.SMEM)
HBM = pl.BlockSpec(memory_space=pltpu.HBM)
ANY = pl.BlockSpec(memory_space=pl.ANY)


def dot(a, b):
    return lax.dot_general(a, b, (((1,), (0,)), ((), ())), preferred_element_type=F32)


def dot_nt(a, b):
    return lax.dot_general(a, b, (((1,), (1,)), ((), ())), preferred_element_type=F32)


def iota(shape, dim):
    return lax.broadcasted_iota(I32, shape, dim)


def as_bf16(mask):
    return jnp.where(mask, 1.0, 0.0).astype(BF16)


def two_parts(v):
    high = v.astype(BF16)
    low = (v - high.astype(F32)).astype(BF16)
    return jnp.concatenate([high, low], axis=1)


def masked_sum(mask, parts):
    both = dot(mask, parts)
    return both[:, :LANES] + both[:, LANES:]


def call(kernel, out, args, specs, out_specs=None, scratch=(), cost=1_000_000, limit=24, aliases=None):
    return pl.pallas_call(
        kernel,
        out_shape=out,
        in_specs=specs,
        out_specs=out_specs or jax.tree.map(lambda _: VMEM, out),
        scratch_shapes=list(scratch),
        input_output_aliases=aliases or {},
        cost_estimate=pl.CostEstimate(flops=cost, bytes_accessed=1_000_000, transcendentals=0),
        compiler_params=pltpu.CompilerParams(vmem_limit_bytes=limit << 20),
    )(*args)


def block(*lead):
    return jax.ShapeDtypeStruct((*lead, ROWS, LANES), F32)


def one_block(*lead):
    return jax.ShapeDtypeStruct((*lead, ONE, LANES), F32)


def chunk_of(place, dz, dx):
    row = jnp.where(place[2] == 0, dz, 1 - dz)
    return row * NX + lax.rem(place[1] + dx, NX)


def rank_kernel(events, slot_out, acc_out, flag_out, cleared):
    lines = slot_out.shape[0]
    zero = jnp.zeros((LANES, LANES), F32)
    below = as_bf16(iota((LANES, LANES), 0) < iota((LANES, LANES), 1))
    with_total = jnp.concatenate([below, jnp.ones((LANES, LANES), BF16)], axis=1)
    owner_ids = iota((OWNERS, LANES), 0)
    before = jnp.zeros((OWNERS, LANES), F32)
    codes = jnp.zeros((OWNERS, LANES), F32)
    each = cleared.shape[0] // LANES // lines
    for b in range(lines):
        home_row = events[b : b + 1, :]
        account_row = events[lines + b : lines + b + 1, :]
        flag_row = events[2 * lines + b : 2 * lines + b + 1, :]
        chosen = owner_ids == home_row
        counted = dot(as_bf16(chosen), with_total)
        rank = jnp.sum(
            jnp.where(chosen, counted[:, :LANES] + before, 0.0), axis=0, keepdims=True
        )
        before = before + counted[:, LANES:]
        slot_out[b : b + 1, :] = home_row * LANES + rank.astype(I32)
        code = (account_row * 2 + flag_row + 1).astype(F32)
        rank_of = as_bf16(iota((LANES, LANES), 0) == rank.astype(I32))
        codes = codes + dot_nt(jnp.where(chosen, code, 0.0).astype(BF16), rank_of)
        for i in range(each):
            cleared[(b * each + i) * LANES : (b * each + i + 1) * LANES, :] = zero
    code_ids = codes.astype(I32) - 1
    acc_out[...] = jnp.right_shift(code_ids, 1)
    flag_out[...] = jnp.where(code_ids >= 0, jnp.bitwise_and(code_ids, 1), 0).astype(F32)


def spread_kernel(slot_rows, features, cleared, grouped, slots, sem):
    copy = pltpu.make_async_copy(slot_rows, slots, sem)
    copy.start()
    copy.wait()

    def spread(b, _):
        for j in range(LANES):
            grouped[pl.ds(slots[b, j], 1), :] = features[pl.ds(b * LANES + j, 1), :]
        return 0

    lax.fori_loop(0, slot_rows.shape[0], spread, 0)


def after_and_ones():
    after = as_bf16(iota((LANES, LANES), 0) > iota((LANES, LANES), 1))
    return jnp.concatenate([after, jnp.ones((LANES, LANES), BF16)], axis=1)


def cut(v, i):
    return v[i * LANES : (i + 1) * LANES, :]


def counted_rows(counted, flagged):
    count = dot(jnp.concatenate(counted, axis=0), jnp.ones((LANES, LANES), BF16))
    lane = iota((LANES, LANES), 1)
    both = jnp.zeros((LANES, LANES), F32)
    for i in range(8):
        both = jnp.where(lane == i, cut(count, i), both)
        both = jnp.where(lane == 8 + i, cut(flagged, i), both)
    return both.T


def closing_kernel(dx, place, acc_rows, flag_rows, grouped, ready, other, mine):
    sides = after_and_ones()
    for out, half_of in ((other, 1 - place[0]), (mine, place[0])):
        bases = [half_of * HALF + chunk_of(place, dz, dx) * FOUR for dz in range(NL)]
        acc8 = jnp.concatenate([acc_rows[pl.ds(b, FOUR), :] for b in bases], axis=0)
        flag8 = jnp.concatenate([flag_rows[pl.ds(b, FOUR), :] for b in bases], axis=0)
        member = [iota((LANES, LANES), 0) == acc8[i : i + 1, :] for i in range(8)]
        member_flags = [
            jnp.where(member[i], flag8[i : i + 1, :], 0.0).astype(BF16) for i in range(8)
        ]
        flagged = dot(jnp.concatenate(member_flags, axis=0), sides)
        counted = [as_bf16(member[i] & (cut(flagged, i)[:, :LANES] < 0.5)) for i in range(8)]
        rows = counted_rows(counted, flagged[:, LANES:])
        marks = jnp.minimum(rows[8:16, :], 1.0)
        for dz in range(NL):
            for i in range(FOUR):
                at = pl.multiple_of((bases[dz] + i) * LANES, LANES)
                values = two_parts(grouped[pl.ds(at, LANES), :])
                out[dz, i * LANES : (i + 1) * LANES, :] = masked_sum(
                    counted[dz * FOUR + i], values
                )
            own = slice(dz * FOUR, dz * FOUR + FOUR)
            out[dz, TAIL:, :] = jnp.concatenate([rows[own, :], marks[own, :]], axis=0)


def running_kernel(acc_rows, flag_rows, grouped, ready, run, counts, opens):
    sides = after_and_ones()
    up_to = iota((LANES, LANES), 1) <= iota((LANES, LANES), 0)

    def some(g, _):
        rows = pl.ds(pl.multiple_of(g * 8, 8), 8)
        acc8 = acc_rows[rows, :].astype(F32)
        flag8 = flag_rows[rows, :]
        acc_cols = acc8.T
        same = []
        for i in range(8):
            acc_col = jnp.broadcast_to(acc_cols[:, i : i + 1], (LANES, LANES))
            same.append((acc_col == acc8[i : i + 1, :]) & (acc_col >= 0.0) & up_to)
        same_flags = [
            jnp.where(same[i], flag8[i : i + 1, :], 0.0).astype(BF16) for i in range(8)
        ]
        flagged = dot(jnp.concatenate(same_flags, axis=0), sides)
        session = [as_bf16(same[i] & (cut(flagged, i)[:, :LANES] < 0.5)) for i in range(8)]
        for i in range(8):
            at = pl.ds(pl.multiple_of((g * 8 + i) * LANES, LANES), LANES)
            run[at, :] = masked_sum(session[i], two_parts(grouped[at, :]))
        found = counted_rows(session, flagged[:, LANES:])
        counts[rows, :] = found[:8, :]
        opens[rows, :] = jnp.where(found[8:16, :] < 0.5, 1.0, 0.0)
        return 0

    lax.fori_loop(0, OWNERS // 8, some, 0)


def in_time_kernel(
    slots, slot_rows, home, account, run, counts, opens, ready,
    run_out, count_out, open_out, user_out,
):
    lines = home.shape[0]

    def scalars(t, _):
        rows = pl.ds(pl.multiple_of(t * 8, 8), 8)
        home8 = home[rows, :]
        rank = slot_rows[rows, :] - home8 * LANES
        count = jnp.zeros((8, LANES), F32)
        is_open = jnp.zeros((8, LANES), F32)
        for o in range(OWNERS):
            here = home8 == o
            for_count = jnp.broadcast_to(counts[o : o + 1, :], (8, LANES))
            for_open = jnp.broadcast_to(opens[o : o + 1, :], (8, LANES))
            count = jnp.where(here, jnp.take_along_axis(for_count, rank, axis=1), count)
            is_open = jnp.where(here, jnp.take_along_axis(for_open, rank, axis=1), is_open)
        count_out[rows, :] = count
        open_out[rows, :] = is_open
        chunk = jnp.right_shift(home8, 2)
        row = (home8 - chunk * FOUR) * LANES + account[rows, :]
        user_out[rows, :] = chunk * ROWS + jnp.where(is_open > 0.5, row, TAIL + FOUR)
        return 0

    lax.fori_loop(0, lines // 8, scalars, 0)

    def collect(b, _):
        for j in range(LANES):
            run_out[pl.ds(b * LANES + j, 1), :] = run[pl.ds(slots[b, j], 1), :]
        return 0

    lax.fori_loop(0, lines, collect, 0)


def sums_of(chunk, i):
    return chunk[i * LANES : (i + 1) * LANES, :]


def keep_of(tail):
    return (1.0 - tail).T


def joined_sums(keep, i, earlier, later):
    return later + jnp.broadcast_to(keep[:, i : i + 1], (LANES, LANES)) * earlier


def joined_tail(earlier, later):
    marks = jnp.concatenate([later[FOUR:, :], later[:FOUR, :]], axis=0)
    return jnp.where(
        iota((8, LANES), 0) < FOUR, later + (1.0 - marks) * earlier, jnp.maximum(later, earlier)
    )


def joined_one(earlier, later):
    tail, first = later[LANES:, :], earlier[LANES:, :]
    mark = tail[1:2, :]
    sub = iota((8, LANES), 0)
    sums = joined_sums(keep_of(tail), 1, earlier[:LANES, :], later[:LANES, :])
    tail = jnp.where(
        sub == 0, tail + (1.0 - mark) * first, jnp.where(sub == 1, jnp.maximum(tail, first), 0.0)
    )
    return jnp.concatenate([sums, tail], axis=0)


def core_kernel(place, mine, got, *outs):
    first = place[0] == 0
    for dz in range(NL):
        a, b = mine[dz, TAIL:, :], got[dz, TAIL:, :]
        early, late = jnp.where(first, a, b), jnp.where(first, b, a)
        keep = keep_of(late)
        for i in range(FOUR):
            at = slice(i * LANES, (i + 1) * LANES)
            a, b = mine[dz, at, :], got[dz, at, :]
            outs[dz][at, :] = joined_sums(
                keep, FOUR + i, jnp.where(first, a, b), jnp.where(first, b, a)
            )
        outs[dz][TAIL:, :] = joined_tail(early, late)


def row_kernel(place, *refs):
    tables = (refs[:NX], refs[NX : 2 * NX])
    totals = refs[2 * NX + 1 : 2 * NX + 3]
    outs, pair = refs[2 * NX + 3 : 2 * NX + 3 + NH], refs[-1]
    for x in range(NX):

        @pl.when(place[1] == x)
        def _(x=x):
            for dz in range(NL):
                order = [tables[dz][(x - j) % NX] for j in range(NX)]
                tails = [t[TAIL:, :] for t in order]
                keep = [keep_of(t) for t in tails]
                for i in range(FOUR):
                    total = sums_of(order[0], i)
                    for j in range(1, NX):
                        total = joined_sums(keep[j], FOUR + i, total, sums_of(order[j], i))
                    totals[dz][i * LANES : (i + 1) * LANES, :] = total
                tail = tails[0]
                for j in range(1, NX):
                    tail = joined_tail(tail, tails[j])
                totals[dz][TAIL:, :] = tail

    own, near = totals
    first = place[2] == 0
    a, b = own[TAIL:, :], near[TAIL:, :]
    early, late = jnp.where(first, a, b), jnp.where(first, b, a)
    keep = keep_of(late)
    tail = joined_tail(early, late)
    sub = iota((8, LANES), 0)
    for i in range(FOUR):
        a, b = sums_of(own, i), sums_of(near, i)
        pair[i, :LANES, :] = joined_sums(
            keep, FOUR + i, jnp.where(first, a, b), jnp.where(first, b, a)
        )
        pair[i, LANES:, :] = jnp.where(
            sub == 0, tail[i : i + 1, :],
            jnp.where(sub == 1, tail[FOUR + i : FOUR + i + 1, :], 0.0),
        )
    for r in range(NH):
        outs[r][...] = pair[lax.rem(place[3] + r, NH)]


def plane_kernel(place, r0, r1, r2, r3, out):
    rows = (r0, r1, r2, r3)
    for h in range(NH):

        @pl.when(place[3] == h)
        def _(h=h):
            total = rows[h][...]
            for j in range(1, NH):
                total = joined_one(total, rows[(h - j) % NH][...])
            out[...] = total


def rows_back_kernel(place, p1, p2, p3, r0, r1, r2, r3, *outs):
    rows = (r0, r1, r2, r3)
    start = jnp.zeros((ONE, LANES), F32)
    for r, plane in ((2, p3), (1, p2), (0, p1)):
        start = jnp.where(place[4] > r, joined_one(start, plane[...]), start)
    for h in range(NH):

        @pl.when(place[3] == h)
        def _(h=h):
            state = start
            for j in range(NH):
                k = (h - j) % NH
                outs[k][...] = state
                if j < NH - 1:
                    state = joined_one(state, rows[k][...])


def chips_back_kernel(place, e0, e1, e2, e3, own, near, *refs):
    tables, outs = (refs[:NX], refs[NX : 2 * NX]), (refs[2 * NX : 3 * NX], refs[3 * NX : 4 * NX])
    came = refs[-1]
    for r, e in enumerate((e0, e1, e2, e3)):
        came[lax.rem(place[3] + r, NH)] = e[...]
    first = place[2] == 0
    sub = iota((8, LANES), 0)
    tail0 = jnp.zeros((8, LANES), F32)
    for i in range(FOUR):
        tail0 = jnp.where(sub == i, came[i, LANES : LANES + 1, :], tail0)
    between = jnp.where(first, own[TAIL:, :], near[TAIL:, :])
    keep = keep_of(between)
    tail1 = joined_tail(tail0, between)
    for x in range(NX):

        @pl.when(place[1] == x)
        def _(x=x):
            for dz in range(NL):
                order = [(x - j) % NX for j in range(NX)]
                tails = [tables[dz][k][TAIL:, :] for k in order[:-1]]
                keeps = [keep_of(t) for t in tails]
                late = first if dz else jnp.logical_not(first)
                for i in range(FOUR):
                    at = slice(i * LANES, (i + 1) * LANES)
                    state = came[i, :LANES, :]
                    second = joined_sums(
                        keep, FOUR + i, state, jnp.where(first, own[at, :], near[at, :])
                    )
                    state = jnp.where(late, second, state)
                    for j, k in enumerate(order):
                        outs[dz][k][at, :] = state
                        if j < NX - 1:
                            state = joined_sums(
                                keeps[j], FOUR + i, state, sums_of(tables[dz][k], i)
                            )
                tail = jnp.where(late, tail1, tail0)
                for j, k in enumerate(order):
                    outs[dz][k][TAIL:, :] = tail
                    if j < NX - 1:
                        tail = joined_tail(tail, tails[j])


def cores_back_kernel(place, ready, *refs):
    parts, mine, got = refs[:4], refs[4:6], refs[6:8]
    keep_out, send = refs[8:]
    first = place[0] == 0
    counts_only = iota((8, LANES), 0) < FOUR
    for d in range(2):
        for dz in range(NL):
            part, at = parts[2 * d + dz], 2 * d + dz
            core0 = jnp.where(first, mine[d][dz, TAIL:, :], got[d][dz, TAIL:, :])
            keep = keep_of(core0)
            for i in range(FOUR):
                rows = slice(i * LANES, (i + 1) * LANES)
                state = part[rows, :]
                second = joined_sums(
                    keep, FOUR + i, state,
                    jnp.where(first, mine[d][dz, rows, :], got[d][dz, rows, :]),
                )
                keep_out[at, rows, :] = jnp.where(first, state, second)
                send[at, rows, :] = jnp.where(first, second, state)
            state = part[TAIL:, :]
            second = joined_tail(state, core0)
            keep_out[at, TAIL:, :] = jnp.where(counts_only, jnp.where(first, state, second), 0.0)
            send[at, TAIL:, :] = jnp.where(counts_only, jnp.where(first, second, state), 0.0)


BACK = ((2, 0), (1, 3))


def finish_kernel(place, users, run, count, is_open, home, account, *refs):
    sides, (out, table, picked, sems) = refs[:4], refs[4:]
    copies, held = [], []
    for s, side in enumerate(sides):
        half_of = place[0] if s < 2 else 1 - place[0]
        for d in range(2):
            for dz in range(NL):
                at = half_of * CHUNKS + chunk_of(place, dz, BACK[s % 2][d])
                held.append((side, 2 * d + dz, at))
                copies.append(
                    pltpu.make_async_copy(
                        side.at[2 * d + dz], table.at[at], sems.at[4 * s + 2 * d + dz]
                    )
                )
                copies[-1].start()
    lines = home.shape[0]
    flat = table.reshape(NC * CHUNKS * ROWS, LANES)
    scale = []
    for t in range(lines // 8):
        rows = slice(8 * t, 8 * t + 8)
        home8, account8 = home[rows, :], account[rows, :]
        came = jnp.zeros((8, LANES), F32)
        for side, index, at in held:
            for i in range(FOUR):
                row = jnp.broadcast_to(side[index, TAIL + i : TAIL + i + 1, :], (8, LANES))
                found = jnp.take_along_axis(row, account8, axis=1)
                came = jnp.where(home8 == at * FOUR + i, found, came)
        scale.append(1.0 / (count[rows, :] + is_open[rows, :] * came))
    scale = jnp.concatenate(scale, axis=0)
    if lines < LANES:
        scale = jnp.concatenate([scale, jnp.zeros((LANES - lines, LANES), F32)], axis=0)
    scale = scale.T
    for copy in copies:
        copy.wait()

    def pick(b, _):
        for j in range(LANES):
            picked[pl.ds(b * LANES + j, 1), :] = flat[pl.ds(users[b, j], 1), :]
        return 0

    lax.fori_loop(0, lines, pick, 0)
    for b in range(lines):
        at = pl.ds(b * LANES, LANES)
        factor = jnp.broadcast_to(scale[:, b : b + 1], (LANES, LANES))
        out[at, :] = (run[at, :] + picked[at, :]) * factor


def ring(n, k):
    return [(i, (i + k) % n) for i in range(n)]


def body(features, home, account, flags):
    rows = features.shape[0]
    lines = rows // LANES
    home = home.reshape(lines, LANES)
    account = account.reshape(lines, LANES)
    flags = flags.reshape(lines, LANES)
    spot, place = iota((8,), 0), jnp.zeros((8,), I32)
    for n, axis in enumerate(("c", "x", "l", "h", "y")):
        place = jnp.where(spot == n, lax.axis_index(axis).astype(I32), place)
    small = jax.ShapeDtypeStruct((lines, LANES), I32)
    small_f = jax.ShapeDtypeStruct((lines, LANES), F32)
    by_owner = functools.partial(jax.ShapeDtypeStruct, (OWNERS, LANES))
    by_slot = jax.ShapeDtypeStruct((OWNERS * LANES, LANES), F32)
    slot, acc_rows, flag_rows, cleared = call(
        rank_kernel,
        [small, by_owner(I32), by_owner(F32), by_slot],
        (jnp.concatenate([home, account, flags]),),
        [VMEM],
        cost=2_000_000_000,
    )
    grouped = call(
        spread_kernel,
        by_slot,
        (slot, features, cleared),
        [VMEM] * 3,
        scratch=[pltpu.SMEM((lines, LANES), I32), pltpu.SemaphoreType.DMA],
        cost=4_000_000_000,
        aliases={2: 0},
    )
    swap = ring(NC, 1)

    def exchange(v, dz, dx):
        if dz == 0 and dx == 0:
            return v
        pairs = [
            (row * NX + x, (row ^ dz) * NX + (x + dx) % NX) for row in range(NL) for x in range(NX)
        ]
        return lax.ppermute(v, ("l", "x"), pairs)

    order = (2, 1, 3, 0)
    mine, got = [None] * NX, [None] * NX
    tables = [[None] * NX for _ in range(NL)]

    def meet(dx):
        chunks = call(core_kernel, [block()] * NL, (place, mine[dx], got[dx]),
                      [SMEM, VMEM, VMEM], cost=500_000_000)
        for dz in reversed(range(NL)):
            tables[dz][dx] = exchange(chunks[dz], dz, dx)
        return chunks[0]

    met = [acc_rows]
    for at, dx in enumerate(order):
        other, mine[dx] = call(
            functools.partial(closing_kernel, dx),
            [block(NL)] * 2,
            (place, acc_rows, flag_rows, grouped, met[at]),
            [SMEM] + [VMEM] * 3 + [ANY],
            cost=1_500_000_000,
        )
        got[dx] = lax.ppermute(other, "c", swap)
        met.append(meet(order[at - 1]) if at else mine[dx])
    met.append(meet(order[-1]))
    run_slots, counts, opens = call(
        running_kernel,
        [by_slot, by_owner(F32), by_owner(F32)],
        (acc_rows, flag_rows, grouped, met[-1]),
        [VMEM] * 3 + [ANY],
        cost=8_000_000_000,
    )
    own, near, *pairs = call(
        row_kernel,
        [block()] * NL + [one_block()] * NH,
        (place, *tables[0], *tables[1], counts),
        [SMEM] + [VMEM] * (NL * NX) + [ANY],
        scratch=[pltpu.VMEM((NH, ONE, LANES), F32)],
    )
    rows_got = [pairs[0]] + [lax.ppermute(pairs[r], "h", ring(NH, r)) for r in range(1, NH)]
    plane = call(plane_kernel, one_block(), (place, *rows_got), [SMEM] + [VMEM] * NH)
    ny = lax.axis_size("y")
    planes = [
        lax.ppermute(plane, "y", [(i, i + r) for i in range(ny - r)]) for r in range(1, ny)
    ]
    came = call(rows_back_kernel, [one_block()] * NH, (place, *planes, *rows_got),
                [SMEM] + [VMEM] * (3 + NH))
    came = [came[0]] + [lax.ppermute(came[r], "h", ring(NH, -r)) for r in range(1, NH)]
    parts = call(
        chips_back_kernel,
        [block()] * (NL * NX),
        (place, *came, own, near, *tables[0], *tables[1]),
        [SMEM] + [VMEM] * (NH + NL + NL * NX),
        scratch=[pltpu.VMEM((NH, ONE, LANES), F32)],
    )
    parts = [list(parts[:NX]), list(parts[NX:])]
    kept = parts[0][0]
    for dx in (2, 0, 1, 3):
        for dz in reversed(range(NL)):
            parts[dz][dx] = exchange(parts[dz][dx], dz, (NX - dx) % NX)
    run, count, is_open, users = call(
        in_time_kernel,
        [jax.ShapeDtypeStruct((rows, LANES), F32), small_f, small_f, small],
        (slot, slot, home, account, run_slots, counts, opens, kept),
        [SMEM] + [VMEM] * 6 + [ANY],
        cost=10_000_000_000,
    )
    keep, last = [], []
    for dxs in BACK:
        stay, send = call(
            cores_back_kernel,
            [block(4)] * 2,
            (place, keep[-1] if keep else count, *[parts[dz][dx] for dx in dxs for dz in range(NL)],
             *[mine[dx] for dx in dxs], *[got[dx] for dx in dxs]),
            [SMEM, ANY] + [VMEM] * 8,
            cost=500_000_000,
        )
        keep.append(stay)
        last.append(lax.ppermute(send, "c", swap))
    return call(
        finish_kernel,
        jax.ShapeDtypeStruct((rows, LANES), F32),
        (place, users, run, count, is_open, home, account, *keep, *last),
        [SMEM, SMEM] + [VMEM] * 9,
        scratch=[pltpu.VMEM((NC * CHUNKS, ROWS, LANES), F32), pltpu.VMEM((rows, LANES), F32),
                 pltpu.SemaphoreType.DMA((16,))],
    )


def solution(mesh):
    axes = ("y", "h", "l", "x", "c")
    split = Mesh(mesh.devices.reshape(-1, NH, NL, NX, NC), axes)
    return jax.shard_map(
        body,
        mesh=split,
        in_specs=(P(axes, None), P(axes, None), P(axes), P(axes)),
        out_specs=P(axes, None),
        check_vma=False,
    )
```

```python
import functools

import jax
import jax.numpy as jnp
from jax import lax
from jax.experimental import pallas as pl
from jax.experimental.pallas import tpu as pltpu
from jax.sharding import Mesh, PartitionSpec as P


LANES = 128
FOUR = 4
TAIL = FOUR * LANES
ROWS = TAIL + 8
QUARTER = LANES // 4
PIECE = QUARTER + 8
NH, NL, NX, NC = 4, 2, 4, 2
OWNERS = NH * NL * NX * NC
HALF = OWNERS // NC
CHUNKS = HALF // FOUR
BF16, F32, I32 = jnp.bfloat16, jnp.float32, jnp.int32
VMEM = pl.BlockSpec(memory_space=pltpu.VMEM)
SMEM = pl.BlockSpec(memory_space=pltpu.SMEM)
HBM = pl.BlockSpec(memory_space=pltpu.HBM)
ANY = pl.BlockSpec(memory_space=pl.ANY)


def dot(a, b):
    return lax.dot_general(a, b, (((1,), (0,)), ((), ())), preferred_element_type=F32)


def dot_nt(a, b):
    return lax.dot_general(a, b, (((1,), (1,)), ((), ())), preferred_element_type=F32)


def iota(shape, dim):
    return lax.broadcasted_iota(I32, shape, dim)


def as_bf16(mask):
    return jnp.where(mask, 1.0, 0.0).astype(BF16)


def two_parts(v):
    high = v.astype(BF16)
    low = (v - high.astype(F32)).astype(BF16)
    return jnp.concatenate([high, low], axis=1)


def masked_sum(mask, parts):
    both = dot(mask, parts)
    return both[:, :LANES] + both[:, LANES:]


def call(kernel, out, args, specs, out_specs=None, scratch=(), cost=1_000_000, limit=24, aliases=None):
    return pl.pallas_call(
        kernel,
        out_shape=out,
        in_specs=specs,
        out_specs=out_specs or jax.tree.map(lambda _: VMEM, out),
        scratch_shapes=list(scratch),
        input_output_aliases=aliases or {},
        cost_estimate=pl.CostEstimate(flops=cost, bytes_accessed=1_000_000, transcendentals=0),
        compiler_params=pltpu.CompilerParams(vmem_limit_bytes=limit << 20),
    )(*args)


def block(*lead):
    return jax.ShapeDtypeStruct((*lead, ROWS, LANES), F32)


def pieces(n):
    return jax.ShapeDtypeStruct((n, PIECE, LANES), F32)


def chunk_of(place, dz, dx):
    row = jnp.where(place[2] == 0, dz, 1 - dz)
    return row * NX + lax.rem(place[1] + dx, NX)


def rank_kernel(events, slot_out, cleared):
    lines = slot_out.shape[0]
    zero = jnp.zeros((LANES, LANES), F32)
    below = as_bf16(iota((LANES, LANES), 0) < iota((LANES, LANES), 1))
    with_total = jnp.concatenate([below, jnp.ones((LANES, LANES), BF16)], axis=1)
    owner_ids = iota((OWNERS, LANES), 0)
    before = jnp.zeros((OWNERS, LANES), F32)
    each = cleared.shape[0] // LANES // lines
    step = 8
    for b in range(0, lines, step):
        homes = [events[b + i : b + i + 1, :] for i in range(step)]
        chosen = [owner_ids == home for home in homes]
        counted = dot(jnp.concatenate([as_bf16(c) for c in chosen], axis=0), with_total)
        for i in range(step):
            some = counted[i * OWNERS : (i + 1) * OWNERS, :]
            rank = jnp.sum(
                jnp.where(chosen[i], some[:, :LANES] + before, 0.0), axis=0, keepdims=True
            )
            before = before + some[:, LANES:]
            slot_out[b + i : b + i + 1, :] = homes[i] * LANES + rank.astype(I32)
        for i in range(step * each):
            at = (b * each + i) * LANES
            cleared[at : at + LANES, :] = zero


def spread_kernel(
    events, slot_rows, features, cleared, grouped, acc_out, flag_out, slots, codes, sem
):
    copy = pltpu.make_async_copy(slot_rows, slots, sem)
    copy.start()
    lines = slot_rows.shape[0]
    codes[...] = jnp.zeros_like(codes)
    copy.wait()

    def spread(b, _):
        home_row = events[pl.ds(b, 1), :]
        code = (events[pl.ds(lines + b, 1), :] * 2 + events[pl.ds(2 * lines + b, 1), :] + 1)
        rank = slot_rows[pl.ds(b, 1), :] - home_row * LANES
        chosen = iota((OWNERS, LANES), 0) == home_row
        rank_of = as_bf16(iota((LANES, LANES), 0) == rank)
        codes[...] += dot_nt(jnp.where(chosen, code.astype(F32), 0.0).astype(BF16), rank_of)
        for j in range(LANES):
            grouped[pl.ds(slots[b, j], 1), :] = features[pl.ds(b * LANES + j, 1), :]
        return 0

    lax.fori_loop(0, lines, spread, 0)
    code_ids = codes[...].astype(I32) - 1
    acc_out[...] = jnp.right_shift(code_ids, 1)
    flag_out[...] = jnp.where(code_ids >= 0, jnp.bitwise_and(code_ids, 1), 0).astype(F32)


def after_and_ones():
    after = as_bf16(iota((LANES, LANES), 0) > iota((LANES, LANES), 1))
    return jnp.concatenate([after, jnp.ones((LANES, LANES), BF16)], axis=1)


def cut(v, i):
    return v[i * LANES : (i + 1) * LANES, :]


def counted_rows(counted, flagged):
    count = dot(jnp.concatenate(counted, axis=0), jnp.ones((LANES, LANES), BF16))
    lane = iota((LANES, LANES), 1)
    both = jnp.zeros((LANES, LANES), F32)
    for i in range(8):
        both = jnp.where(lane == i, cut(count, i), both)
        both = jnp.where(lane == 8 + i, cut(flagged, i), both)
    return both.T


def closing_kernel(dx, halves, place, acc_rows, flag_rows, grouped, ready, *outs):
    sides = after_and_ones()
    for out, own_half in zip(outs, halves):
        half_of = place[0] if own_half else 1 - place[0]
        bases = [half_of * HALF + chunk_of(place, dz, dx) * FOUR for dz in range(NL)]
        acc8 = jnp.concatenate([acc_rows[pl.ds(b, FOUR), :] for b in bases], axis=0)
        flag8 = jnp.concatenate([flag_rows[pl.ds(b, FOUR), :] for b in bases], axis=0)
        member = [iota((LANES, LANES), 0) == acc8[i : i + 1, :] for i in range(8)]
        member_flags = [
            jnp.where(member[i], flag8[i : i + 1, :], 0.0).astype(BF16) for i in range(8)
        ]
        flagged = dot(jnp.concatenate(member_flags, axis=0), sides)
        counted = [as_bf16(member[i] & (cut(flagged, i)[:, :LANES] < 0.5)) for i in range(8)]
        rows = counted_rows(counted, flagged[:, LANES:])
        marks = jnp.minimum(rows[8:16, :], 1.0)
        for dz in range(NL):
            for i in range(FOUR):
                at = pl.multiple_of((bases[dz] + i) * LANES, LANES)
                values = two_parts(grouped[pl.ds(at, LANES), :])
                out[dz, i * LANES : (i + 1) * LANES, :] = masked_sum(
                    counted[dz * FOUR + i], values
                )
            own = slice(dz * FOUR, dz * FOUR + FOUR)
            out[dz, TAIL:, :] = jnp.concatenate([rows[own, :], marks[own, :]], axis=0)


def running_kernel(acc_rows, flag_rows, grouped, ready, run, counts, opens):
    sides = after_and_ones()
    up_to = iota((LANES, LANES), 1) <= iota((LANES, LANES), 0)

    def some(g, _):
        rows = pl.ds(pl.multiple_of(g * 8, 8), 8)
        acc8 = acc_rows[rows, :].astype(F32)
        flag8 = flag_rows[rows, :]
        acc_cols = acc8.T
        same = []
        for i in range(8):
            acc_col = jnp.broadcast_to(acc_cols[:, i : i + 1], (LANES, LANES))
            same.append((acc_col == acc8[i : i + 1, :]) & (acc_col >= 0.0) & up_to)
        same_flags = [
            jnp.where(same[i], flag8[i : i + 1, :], 0.0).astype(BF16) for i in range(8)
        ]
        flagged = dot(jnp.concatenate(same_flags, axis=0), sides)
        session = [as_bf16(same[i] & (cut(flagged, i)[:, :LANES] < 0.5)) for i in range(8)]
        for i in range(8):
            at = pl.ds(pl.multiple_of((g * 8 + i) * LANES, LANES), LANES)
            run[at, :] = masked_sum(session[i], two_parts(grouped[at, :]))
        found = counted_rows(session, flagged[:, LANES:])
        counts[rows, :] = found[:8, :]
        opens[rows, :] = jnp.where(found[8:16, :] < 0.5, 1.0, 0.0)
        return 0

    lax.fori_loop(0, OWNERS // 8, some, 0)


def in_time_kernel(
    slots, slot_rows, home, account, run, counts, opens, ready,
    run_out, count_out, open_out, user_out,
):
    lines = home.shape[0]

    def scalars(t, _):
        rows = pl.ds(pl.multiple_of(t * 8, 8), 8)
        home8 = home[rows, :]
        rank = slot_rows[rows, :] - home8 * LANES
        count = jnp.zeros((8, LANES), F32)
        is_open = jnp.zeros((8, LANES), F32)
        for o in range(OWNERS):
            here = home8 == o
            for_count = jnp.broadcast_to(counts[o : o + 1, :], (8, LANES))
            for_open = jnp.broadcast_to(opens[o : o + 1, :], (8, LANES))
            count = jnp.where(here, jnp.take_along_axis(for_count, rank, axis=1), count)
            is_open = jnp.where(here, jnp.take_along_axis(for_open, rank, axis=1), is_open)
        count_out[rows, :] = count
        open_out[rows, :] = is_open
        chunk = jnp.right_shift(home8, 2)
        row = (home8 - chunk * FOUR) * LANES + account[rows, :]
        user_out[rows, :] = chunk * ROWS + jnp.where(is_open > 0.5, row, TAIL + FOUR)
        return 0

    lax.fori_loop(0, lines // 8, scalars, 0)

    def collect(b, _):
        for j in range(LANES):
            run_out[pl.ds(b * LANES + j, 1), :] = run[pl.ds(slots[b, j], 1), :]
        return 0

    lax.fori_loop(0, lines, collect, 0)


def sums_of(chunk, i):
    return chunk[i * LANES : (i + 1) * LANES, :]


def keep_of(tail):
    return (1.0 - tail).T


def joined_sums(keep, i, earlier, later):
    return later + jnp.broadcast_to(keep[:, i : i + 1], (LANES, LANES)) * earlier


def joined_tail(earlier, later):
    marks = jnp.concatenate([later[FOUR:, :], later[:FOUR, :]], axis=0)
    return jnp.where(
        iota((8, LANES), 0) < FOUR, later + (1.0 - marks) * earlier, jnp.maximum(later, earlier)
    )


def core_kernel(place, mine, got, *outs):
    first = place[0] == 0
    for dz in range(NL):
        a, b = mine[dz, TAIL:, :], got[dz, TAIL:, :]
        early, late = jnp.where(first, a, b), jnp.where(first, b, a)
        keep = keep_of(late)
        for i in range(FOUR):
            at = slice(i * LANES, (i + 1) * LANES)
            a, b = mine[dz, at, :], got[dz, at, :]
            outs[dz][at, :] = joined_sums(
                keep, FOUR + i, jnp.where(first, a, b), jnp.where(first, b, a)
            )
        outs[dz][TAIL:, :] = joined_tail(early, late)


def row_kernel(place, *refs):
    tables = (refs[:NX], refs[NX : 2 * NX])
    totals, out = refs[2 * NX + 1 : 2 * NX + 3], refs[-1]
    for x in range(NX):

        @pl.when(place[1] == x)
        def _(x=x):
            for dz in range(NL):
                order = [tables[dz][(x - j) % NX] for j in range(NX)]
                tails = [t[TAIL:, :] for t in order]
                keep = [keep_of(t) for t in tails]
                for i in range(FOUR):
                    total = sums_of(order[0], i)
                    for j in range(1, NX):
                        total = joined_sums(keep[j], FOUR + i, total, sums_of(order[j], i))
                    totals[dz][i * LANES : (i + 1) * LANES, :] = total
                tail = tails[0]
                for j in range(1, NX):
                    tail = joined_tail(tail, tails[j])
                totals[dz][TAIL:, :] = tail

    own, near = totals
    first = place[2] == 0
    a, b = own[TAIL:, :], near[TAIL:, :]
    early, late = jnp.where(first, a, b), jnp.where(first, b, a)
    keep = keep_of(late)
    tail = joined_tail(early, late)
    sub = iota((8, LANES), 0)
    for i in range(FOUR):
        a, b = sums_of(own, i), sums_of(near, i)
        total = joined_sums(keep, FOUR + i, jnp.where(first, a, b), jnp.where(first, b, a))
        ends = jnp.where(
            sub == 0, tail[i : i + 1, :],
            jnp.where(sub == 1, tail[FOUR + i : FOUR + i + 1, :], 0.0),
        )
        for q in range(4):
            out[4 * i + q, :QUARTER, :] = total[q * QUARTER : (q + 1) * QUARTER, :]
            out[4 * i + q, QUARTER:, :] = ends


def scan_kernel(place, rows, out, keeps):
    n = rows.shape[0]
    marks = jnp.concatenate([rows[r, QUARTER + 1 : QUARTER + 2, :] for r in range(n)], axis=0)
    keeps[...] = (1.0 - marks).T
    keep = keeps[pl.ds(pl.multiple_of(place[3] * QUARTER, QUARTER), QUARTER), :]
    sub = iota((8, LANES), 0)
    state, tail = jnp.zeros((QUARTER, LANES), F32), jnp.zeros((8, LANES), F32)
    for r in range(n):
        out[r, :QUARTER, :] = state
        out[r, QUARTER:, :] = tail
        ends = rows[r, QUARTER:, :]
        state = rows[r, :QUARTER, :] + jnp.broadcast_to(keep[:, r : r + 1], state.shape) * state
        tail = jnp.where(sub == 0, ends + (1.0 - ends[1:2, :]) * tail, 0.0)


def chips_back_kernel(place, came, own, near, *refs):
    tables, outs = (refs[:NX], refs[NX : 2 * NX]), (refs[2 * NX : 3 * NX], refs[3 * NX : 4 * NX])
    first = place[2] == 0
    sub = iota((8, LANES), 0)
    tail0 = jnp.zeros((8, LANES), F32)
    for i in range(FOUR):
        tail0 = jnp.where(sub == i, came[4 * i, QUARTER : QUARTER + 1, :], tail0)
    between = jnp.where(first, own[TAIL:, :], near[TAIL:, :])
    keep = keep_of(between)
    tail1 = joined_tail(tail0, between)
    for x in range(NX):

        @pl.when(place[1] == x)
        def _(x=x):
            for dz in range(NL):
                order = [(x - j) % NX for j in range(NX)]
                tails = [tables[dz][k][TAIL:, :] for k in order[:-1]]
                keeps = [keep_of(t) for t in tails]
                late = first if dz else jnp.logical_not(first)
                for i in range(FOUR):
                    at = slice(i * LANES, (i + 1) * LANES)
                    state = jnp.concatenate(
                        [came[4 * i + q, :QUARTER, :] for q in range(4)], axis=0
                    )
                    second = joined_sums(
                        keep, FOUR + i, state, jnp.where(first, own[at, :], near[at, :])
                    )
                    state = jnp.where(late, second, state)
                    for j, k in enumerate(order):
                        outs[dz][k][at, :] = state
                        if j < NX - 1:
                            state = joined_sums(
                                keeps[j], FOUR + i, state, sums_of(tables[dz][k], i)
                            )
                tail = jnp.where(late, tail1, tail0)
                for j, k in enumerate(order):
                    outs[dz][k][TAIL:, :] = tail
                    if j < NX - 1:
                        tail = joined_tail(tail, tails[j])


def cores_back_kernel(place, ready, *refs):
    n = (len(refs) - 2) // 4
    parts, mine, got = refs[: 2 * n], refs[2 * n : 3 * n], refs[3 * n : 4 * n]
    keep_out, send = refs[4 * n :]
    first = place[0] == 0
    counts_only = iota((8, LANES), 0) < FOUR
    for d in range(n):
        for dz in range(NL):
            part, at = parts[2 * d + dz], 2 * d + dz
            core0 = jnp.where(first, mine[d][dz, TAIL:, :], got[d][dz, TAIL:, :])
            keep = keep_of(core0)
            for i in range(FOUR):
                rows = slice(i * LANES, (i + 1) * LANES)
                state = part[rows, :]
                second = joined_sums(
                    keep, FOUR + i, state,
                    jnp.where(first, mine[d][dz, rows, :], got[d][dz, rows, :]),
                )
                keep_out[at, rows, :] = jnp.where(first, state, second)
                send[at, rows, :] = jnp.where(first, second, state)
            state = part[TAIL:, :]
            second = joined_tail(state, core0)
            keep_out[at, TAIL:, :] = jnp.where(counts_only, jnp.where(first, state, second), 0.0)
            send[at, TAIL:, :] = jnp.where(counts_only, jnp.where(first, second, state), 0.0)


BACK = ((2, 0), (1,), (3,))


def finish_kernel(place, users, run, count, is_open, home, account, *refs):
    n = len(BACK)
    sides = refs[: 2 * n]
    out, table, scale, even, odd, even_out, odd_out, sems, out_sems = refs[2 * n :]
    copies, held = [], []
    for s, side in enumerate(sides):
        half_of = place[0] if s < n else 1 - place[0]
        for d, dx in enumerate(BACK[s % n]):
            for dz in range(NL):
                at = half_of * CHUNKS + chunk_of(place, dz, dx)
                held.append((side, 2 * d + dz, at))
                copies.append(
                    pltpu.make_async_copy(
                        side.at[2 * d + dz], table.at[at], sems.at[len(copies)]
                    )
                )
                copies[-1].start()
    lines = home.shape[0]
    flat = table.reshape(NC * CHUNKS * ROWS, LANES)
    for t in range(lines // 8):
        rows = slice(8 * t, 8 * t + 8)
        home8, account8 = home[rows, :], account[rows, :]
        came = jnp.zeros((8, LANES), F32)
        for side, index, at in held:
            for i in range(FOUR):
                row = jnp.broadcast_to(side[index, TAIL + i : TAIL + i + 1, :], (8, LANES))
                found = jnp.take_along_axis(row, account8, axis=1)
                came = jnp.where(home8 == at * FOUR + i, found, came)
        scale[rows, :] = 1.0 / (count[rows, :] + is_open[rows, :] * came)
    for copy in copies:
        copy.wait()

    def pick(b, to):
        for j in range(LANES):
            to[j : j + 1, :] = flat[pl.ds(users[b, j], 1), :]

    def leave(b, k):
        at = pl.multiple_of(b * LANES, LANES)
        return pltpu.make_async_copy(
            (even_out, odd_out)[k], out.at[pl.ds(at, LANES), :], out_sems.at[k]
        )

    def scaled(b, picked, k):
        at = pl.ds(pl.multiple_of(b * LANES, LANES), LANES)
        factor = jnp.broadcast_to(scale[pl.ds(b, 1), :], (LANES, LANES)).T
        (even_out, odd_out)[k][...] = (run[at, :] + picked[...]) * factor
        leave(b, k).start()

    pick(0, even)
    pick(1, odd)
    scaled(0, even, 0)

    def two(g, _):
        b = 2 * g
        pick(b, even)
        pl.when(g > 1)(lambda: leave(b - 3, 1).wait())
        scaled(b - 1, odd, 1)
        pick(b + 1, odd)
        leave(b - 2, 0).wait()
        scaled(b, even, 0)
        return 0

    lax.fori_loop(1, lines // 2, two, 0)
    leave(lines - 3, 1).wait()
    scaled(lines - 1, odd, 1)
    leave(lines - 2, 0).wait()
    leave(lines - 1, 1).wait()


def ring(n, k):
    return [(i, (i + k) % n) for i in range(n)]


def body(features, home, account, flags):
    rows = features.shape[0]
    lines = rows // LANES
    home = home.reshape(lines, LANES)
    account = account.reshape(lines, LANES)
    flags = flags.reshape(lines, LANES)
    spot, place = iota((8,), 0), jnp.zeros((8,), I32)
    for n, axis in enumerate(("c", "x", "l", "h", "y")):
        place = jnp.where(spot == n, lax.axis_index(axis).astype(I32), place)
    small = jax.ShapeDtypeStruct((lines, LANES), I32)
    small_f = jax.ShapeDtypeStruct((lines, LANES), F32)
    by_owner = functools.partial(jax.ShapeDtypeStruct, (OWNERS, LANES))
    by_slot = jax.ShapeDtypeStruct((OWNERS * LANES, LANES), F32)
    events = jnp.concatenate([home, account, flags])
    slot, cleared = call(rank_kernel, [small, by_slot], (events,), [VMEM], cost=2_000_000_000)
    grouped, acc_rows, flag_rows = call(
        spread_kernel,
        [by_slot, by_owner(I32), by_owner(F32)],
        (events, slot, features, cleared),
        [VMEM] * 4,
        scratch=[pltpu.SMEM((lines, LANES), I32), pltpu.VMEM((OWNERS, LANES), F32),
                 pltpu.SemaphoreType.DMA],
        cost=4_000_000_000,
        aliases={3: 0},
    )
    swap = ring(NC, 1)

    def exchange(v, dz, dx):
        if dz == 0 and dx == 0:
            return v
        pairs = [
            (row * NX + x, (row ^ dz) * NX + (x + dx) % NX) for row in range(NL) for x in range(NX)
        ]
        return lax.ppermute(v, ("l", "x"), pairs)

    order = (2, 1, 3, 0)
    mine, got = [None] * NX, [None] * NX
    tables = [[None] * NX for _ in range(NL)]

    def meet(dx):
        chunks = call(core_kernel, [block()] * NL, (place, mine[dx], got[dx]),
                      [SMEM, VMEM, VMEM], cost=500_000_000)
        for dz in reversed(range(NL)):
            tables[dz][dx] = exchange(chunks[dz], dz, dx)
        return chunks[0]

    def close(dx, halves, ready):
        return call(
            functools.partial(closing_kernel, dx, halves),
            [block(NL)] * len(halves),
            (place, acc_rows, flag_rows, grouped, ready),
            [SMEM] + [VMEM] * 3 + [ANY],
            cost=800_000_000 * len(halves),
        )

    met = [acc_rows]
    for at, dx in enumerate(order):
        if at:
            other, mine[dx] = close(dx, (0, 1), met[at])
        else:
            (other,) = close(dx, (0,), met[at])
        got[dx] = lax.ppermute(other, "c", swap)
        if at == 0:
            (mine[dx],) = close(dx, (1,), other)
        met.append(meet(order[at - 1]) if at else mine[dx])
    met.append(meet(order[-1]))
    run_slots, counts, opens = call(
        running_kernel,
        [by_slot, by_owner(F32), by_owner(F32)],
        (acc_rows, flag_rows, grouped, met[-1]),
        [VMEM] * 3 + [ANY],
        cost=8_000_000_000,
    )
    own, near, total = call(
        row_kernel,
        [block()] * NL + [pieces(16)],
        (place, *tables[0], *tables[1], counts),
        [SMEM] + [VMEM] * (NL * NX) + [ANY],
    )
    total = lax.all_to_all(total, ("y", "h"), 0, 0, tiled=True)
    came = call(scan_kernel, pieces(16), (place, total), [SMEM, VMEM],
                scratch=[pltpu.VMEM((LANES, 16), F32)])
    came = lax.all_to_all(came, ("y", "h"), 0, 0, tiled=True)
    parts = call(
        chips_back_kernel,
        [block()] * (NL * NX),
        (place, came, own, near, *tables[0], *tables[1]),
        [SMEM] + [VMEM] * (1 + NL + NL * NX),
    )
    parts = [list(parts[:NX]), list(parts[NX:])]
    kept = parts[0][0]
    for dx in (2, 0, 1, 3):
        for dz in reversed(range(NL)):
            parts[dz][dx] = exchange(parts[dz][dx], dz, (NX - dx) % NX)
    run, count, is_open, users = call(
        in_time_kernel,
        [jax.ShapeDtypeStruct((rows, LANES), F32), small_f, small_f, small],
        (slot, slot, home, account, run_slots, counts, opens, kept),
        [SMEM] + [VMEM] * 6 + [ANY],
        cost=10_000_000_000,
    )
    keep, last = [], []
    for dxs in BACK:
        stay, send = call(
            cores_back_kernel,
            [block(2 * len(dxs))] * 2,
            (place, keep[-1] if keep else count, *[parts[dz][dx] for dx in dxs for dz in range(NL)],
             *[mine[dx] for dx in dxs], *[got[dx] for dx in dxs]),
            [SMEM, ANY] + [VMEM] * (4 * len(dxs)),
            cost=500_000_000,
        )
        keep.append(stay)
        last.append(lax.ppermute(send, "c", swap))
    line = pltpu.VMEM((LANES, LANES), F32)
    return call(
        finish_kernel,
        jax.ShapeDtypeStruct((rows, LANES), F32),
        (place, users, run, count, is_open, home, account, *keep, *last),
        [SMEM, SMEM] + [VMEM] * (5 + 2 * len(BACK)),
        out_specs=ANY,
        scratch=[pltpu.VMEM((NC * CHUNKS, ROWS, LANES), F32), pltpu.VMEM((lines, LANES), F32),
                 line, line, line, line, pltpu.SemaphoreType.DMA((16,)),
                 pltpu.SemaphoreType.DMA((2,))],
    )


def solution(mesh):
    axes = ("y", "h", "l", "x", "c")
    split = Mesh(mesh.devices.reshape(-1, NH, NL, NX, NC), axes)
    return jax.shard_map(
        body,
        mesh=split,
        in_specs=(P(axes, None), P(axes, None), P(axes), P(axes)),
        out_specs=P(axes, None),
        check_vma=False,
    )
```

```python
import functools

import jax
import jax.numpy as jnp
from jax import lax
from jax.experimental import pallas as pl
from jax.experimental.pallas import tpu as pltpu
from jax.sharding import Mesh, PartitionSpec as P


LANES = 128
FOUR = 4
TAIL = FOUR * LANES
ROWS = TAIL + 8
ONE = LANES + 8
NH, NL, NX, NC = 4, 2, 4, 2
OWNERS = NH * NL * NX * NC
HALF = OWNERS // NC
CHUNKS = HALF // FOUR
BF16, F32, I32 = jnp.bfloat16, jnp.float32, jnp.int32
VMEM = pl.BlockSpec(memory_space=pltpu.VMEM)
SMEM = pl.BlockSpec(memory_space=pltpu.SMEM)
HBM = pl.BlockSpec(memory_space=pltpu.HBM)
ANY = pl.BlockSpec(memory_space=pl.ANY)


def dot(a, b):
    return lax.dot_general(a, b, (((1,), (0,)), ((), ())), preferred_element_type=F32)


def dot_nt(a, b):
    return lax.dot_general(a, b, (((1,), (1,)), ((), ())), preferred_element_type=F32)


def iota(shape, dim):
    return lax.broadcasted_iota(I32, shape, dim)


def as_bf16(mask):
    return jnp.where(mask, 1.0, 0.0).astype(BF16)


def two_parts(v):
    high = v.astype(BF16)
    low = (v - high.astype(F32)).astype(BF16)
    return jnp.concatenate([high, low], axis=1)


def masked_sum(mask, parts):
    both = dot(mask, parts)
    return both[:, :LANES] + both[:, LANES:]


def call(kernel, out, args, specs, out_specs=None, scratch=(), cost=1_000_000, limit=24, aliases=None):
    return pl.pallas_call(
        kernel,
        out_shape=out,
        in_specs=specs,
        out_specs=out_specs or jax.tree.map(lambda _: VMEM, out),
        scratch_shapes=list(scratch),
        input_output_aliases=aliases or {},
        cost_estimate=pl.CostEstimate(flops=cost, bytes_accessed=1_000_000, transcendentals=0),
        compiler_params=pltpu.CompilerParams(vmem_limit_bytes=limit << 20),
    )(*args)


def block(*lead):
    return jax.ShapeDtypeStruct((*lead, ROWS, LANES), F32)


def one_block(*lead):
    return jax.ShapeDtypeStruct((*lead, ONE, LANES), F32)


def chunk_of(place, dz, dx):
    row = jnp.where(place[2] == 0, dz, 1 - dz)
    return row * NX + lax.rem(place[1] + dx, NX)


def rank_kernel(events, slot_out, acc_out, flag_out, cleared):
    lines = slot_out.shape[0]
    zero = jnp.zeros((LANES, LANES), F32)
    below = as_bf16(iota((LANES, LANES), 0) < iota((LANES, LANES), 1))
    with_total = jnp.concatenate([below, jnp.ones((LANES, LANES), BF16)], axis=1)
    owner_ids = iota((OWNERS, LANES), 0)
    before = jnp.zeros((OWNERS, LANES), F32)
    codes = jnp.zeros((OWNERS, LANES), F32)
    each = cleared.shape[0] // LANES // lines
    step = 8
    for b in range(0, lines, step):
        homes = [events[b + i : b + i + 1, :] for i in range(step)]
        chosen = [owner_ids == home for home in homes]
        counted = dot(jnp.concatenate([as_bf16(c) for c in chosen], axis=0), with_total)
        coded, rank_of = [], []
        for i in range(step):
            some = counted[i * OWNERS : (i + 1) * OWNERS, :]
            rank = jnp.sum(
                jnp.where(chosen[i], some[:, :LANES] + before, 0.0), axis=0, keepdims=True
            ).astype(I32)
            before = before + some[:, LANES:]
            slot_out[b + i : b + i + 1, :] = homes[i] * LANES + rank
            account = events[lines + b + i : lines + b + i + 1, :]
            flag = events[2 * lines + b + i : 2 * lines + b + i + 1, :]
            code = (account * 2 + flag + 1).astype(F32)
            coded.append(jnp.where(chosen[i], code, 0.0).astype(BF16))
            rank_of.append(as_bf16(iota((LANES, LANES), 0) == rank))
        codes = codes + dot_nt(
            jnp.concatenate(coded, axis=1), jnp.concatenate(rank_of, axis=1)
        )
        for i in range(step * each):
            at = (b * each + i) * LANES
            cleared[at : at + LANES, :] = zero
    code_ids = codes.astype(I32) - 1
    acc_out[...] = jnp.right_shift(code_ids, 1)
    flag_out[...] = jnp.where(code_ids >= 0, jnp.bitwise_and(code_ids, 1), 0).astype(F32)


def spread_kernel(slot_rows, features, cleared, grouped, slots, sem):
    copy = pltpu.make_async_copy(slot_rows, slots, sem)
    copy.start()
    copy.wait()

    def spread(b, _):
        for j in range(LANES):
            grouped[pl.ds(slots[b, j], 1), :] = features[pl.ds(b * LANES + j, 1), :]
        return 0

    lax.fori_loop(0, slot_rows.shape[0], spread, 0)


def after_and_ones():
    after = as_bf16(iota((LANES, LANES), 0) > iota((LANES, LANES), 1))
    return jnp.concatenate([after, jnp.ones((LANES, LANES), BF16)], axis=1)


def cut(v, i):
    return v[i * LANES : (i + 1) * LANES, :]


def counted_rows(counted, flagged):
    count = dot(jnp.concatenate(counted, axis=0), jnp.ones((LANES, LANES), BF16))
    lane = iota((LANES, LANES), 1)
    both = jnp.zeros((LANES, LANES), F32)
    for i in range(8):
        both = jnp.where(lane == i, cut(count, i), both)
        both = jnp.where(lane == 8 + i, cut(flagged, i), both)
    return both.T


def closing_kernel(dx, place, acc_rows, flag_rows, grouped, ready, other, mine):
    sides = after_and_ones()
    for out, half_of in ((other, 1 - place[0]), (mine, place[0])):
        bases = [half_of * HALF + chunk_of(place, dz, dx) * FOUR for dz in range(NL)]
        acc8 = jnp.concatenate([acc_rows[pl.ds(b, FOUR), :] for b in bases], axis=0)
        flag8 = jnp.concatenate([flag_rows[pl.ds(b, FOUR), :] for b in bases], axis=0)
        member = [iota((LANES, LANES), 0) == acc8[i : i + 1, :] for i in range(8)]
        member_flags = [
            jnp.where(member[i], flag8[i : i + 1, :], 0.0).astype(BF16) for i in range(8)
        ]
        flagged = dot(jnp.concatenate(member_flags, axis=0), sides)
        counted = [as_bf16(member[i] & (cut(flagged, i)[:, :LANES] < 0.5)) for i in range(8)]
        rows = counted_rows(counted, flagged[:, LANES:])
        marks = jnp.minimum(rows[8:16, :], 1.0)
        for dz in range(NL):
            for i in range(FOUR):
                at = pl.multiple_of((bases[dz] + i) * LANES, LANES)
                values = two_parts(grouped[pl.ds(at, LANES), :])
                out[dz, i * LANES : (i + 1) * LANES, :] = masked_sum(
                    counted[dz * FOUR + i], values
                )
            own = slice(dz * FOUR, dz * FOUR + FOUR)
            out[dz, TAIL:, :] = jnp.concatenate([rows[own, :], marks[own, :]], axis=0)


def running_kernel(acc_rows, flag_rows, grouped, ready, run, counts, opens):
    sides = after_and_ones()
    up_to = iota((LANES, LANES), 1) <= iota((LANES, LANES), 0)

    def some(g, _):
        rows = pl.ds(pl.multiple_of(g * 8, 8), 8)
        acc8 = acc_rows[rows, :].astype(F32)
        flag8 = flag_rows[rows, :]
        acc_cols = acc8.T
        same = []
        for i in range(8):
            acc_col = jnp.broadcast_to(acc_cols[:, i : i + 1], (LANES, LANES))
            same.append((acc_col == acc8[i : i + 1, :]) & (acc_col >= 0.0) & up_to)
        same_flags = [
            jnp.where(same[i], flag8[i : i + 1, :], 0.0).astype(BF16) for i in range(8)
        ]
        flagged = dot(jnp.concatenate(same_flags, axis=0), sides)
        session = [as_bf16(same[i] & (cut(flagged, i)[:, :LANES] < 0.5)) for i in range(8)]
        for i in range(8):
            at = pl.ds(pl.multiple_of((g * 8 + i) * LANES, LANES), LANES)
            run[at, :] = masked_sum(session[i], two_parts(grouped[at, :]))
        found = counted_rows(session, flagged[:, LANES:])
        counts[rows, :] = found[:8, :]
        opens[rows, :] = jnp.where(found[8:16, :] < 0.5, 1.0, 0.0)
        return 0

    lax.fori_loop(0, OWNERS // 8, some, 0)


def in_time_kernel(
    slots, slot_rows, home, account, run, counts, opens, ready,
    run_out, count_out, open_out, user_out,
):
    lines = home.shape[0]

    def scalars(t, _):
        rows = pl.ds(pl.multiple_of(t * 8, 8), 8)
        home8 = home[rows, :]
        rank = slot_rows[rows, :] - home8 * LANES
        count = jnp.zeros((8, LANES), F32)
        is_open = jnp.zeros((8, LANES), F32)
        for o in range(OWNERS):
            here = home8 == o
            for_count = jnp.broadcast_to(counts[o : o + 1, :], (8, LANES))
            for_open = jnp.broadcast_to(opens[o : o + 1, :], (8, LANES))
            count = jnp.where(here, jnp.take_along_axis(for_count, rank, axis=1), count)
            is_open = jnp.where(here, jnp.take_along_axis(for_open, rank, axis=1), is_open)
        count_out[rows, :] = count
        open_out[rows, :] = is_open
        chunk = jnp.right_shift(home8, 2)
        row = (home8 - chunk * FOUR) * LANES + account[rows, :]
        user_out[rows, :] = chunk * ROWS + jnp.where(is_open > 0.5, row, TAIL + FOUR)
        return 0

    lax.fori_loop(0, lines // 8, scalars, 0)

    def collect(b, _):
        for j in range(LANES):
            run_out[pl.ds(b * LANES + j, 1), :] = run[pl.ds(slots[b, j], 1), :]
        return 0

    lax.fori_loop(0, lines, collect, 0)


def sums_of(chunk, i):
    return chunk[i * LANES : (i + 1) * LANES, :]


def keep_of(tail):
    return (1.0 - tail).T


def joined_sums(keep, i, earlier, later):
    return later + jnp.broadcast_to(keep[:, i : i + 1], (LANES, LANES)) * earlier


def joined_tail(earlier, later):
    marks = jnp.concatenate([later[FOUR:, :], later[:FOUR, :]], axis=0)
    return jnp.where(
        iota((8, LANES), 0) < FOUR, later + (1.0 - marks) * earlier, jnp.maximum(later, earlier)
    )


def joined_one(earlier, later):
    tail, first = later[LANES:, :], earlier[LANES:, :]
    mark = tail[1:2, :]
    sub = iota((8, LANES), 0)
    sums = joined_sums(keep_of(tail), 1, earlier[:LANES, :], later[:LANES, :])
    tail = jnp.where(
        sub == 0, tail + (1.0 - mark) * first, jnp.where(sub == 1, jnp.maximum(tail, first), 0.0)
    )
    return jnp.concatenate([sums, tail], axis=0)


def core_kernel(place, mine, got, *outs):
    first = place[0] == 0
    for dz in range(NL):
        a, b = mine[dz, TAIL:, :], got[dz, TAIL:, :]
        early, late = jnp.where(first, a, b), jnp.where(first, b, a)
        keep = keep_of(late)
        for i in range(FOUR):
            at = slice(i * LANES, (i + 1) * LANES)
            a, b = mine[dz, at, :], got[dz, at, :]
            outs[dz][at, :] = joined_sums(
                keep, FOUR + i, jnp.where(first, a, b), jnp.where(first, b, a)
            )
        outs[dz][TAIL:, :] = joined_tail(early, late)


def row_kernel(place, *refs):
    tables = (refs[:NX], refs[NX : 2 * NX])
    totals = refs[2 * NX + 1 : 2 * NX + 3]
    outs, pair = refs[2 * NX + 3 : 2 * NX + 3 + NH], refs[-1]
    for x in range(NX):

        @pl.when(place[1] == x)
        def _(x=x):
            for dz in range(NL):
                order = [tables[dz][(x - j) % NX] for j in range(NX)]
                tails = [t[TAIL:, :] for t in order]
                keep = [keep_of(t) for t in tails]
                for i in range(FOUR):
                    total = sums_of(order[0], i)
                    for j in range(1, NX):
                        total = joined_sums(keep[j], FOUR + i, total, sums_of(order[j], i))
                    totals[dz][i * LANES : (i + 1) * LANES, :] = total
                tail = tails[0]
                for j in range(1, NX):
                    tail = joined_tail(tail, tails[j])
                totals[dz][TAIL:, :] = tail

    own, near = totals
    first = place[2] == 0
    a, b = own[TAIL:, :], near[TAIL:, :]
    early, late = jnp.where(first, a, b), jnp.where(first, b, a)
    keep = keep_of(late)
    tail = joined_tail(early, late)
    sub = iota((8, LANES), 0)
    for i in range(FOUR):
        a, b = sums_of(own, i), sums_of(near, i)
        pair[i, :LANES, :] = joined_sums(
            keep, FOUR + i, jnp.where(first, a, b), jnp.where(first, b, a)
        )
        pair[i, LANES:, :] = jnp.where(
            sub == 0, tail[i : i + 1, :],
            jnp.where(sub == 1, tail[FOUR + i : FOUR + i + 1, :], 0.0),
        )
    for r in range(NH):
        outs[r][...] = pair[lax.rem(place[3] + r, NH)]


def plane_kernel(place, r0, r1, r2, r3, out):
    rows = (r0, r1, r2, r3)
    for h in range(NH):

        @pl.when(place[3] == h)
        def _(h=h):
            total = rows[h][...]
            for j in range(1, NH):
                total = joined_one(total, rows[(h - j) % NH][...])
            out[...] = total


def rows_back_kernel(place, p1, p2, p3, r0, r1, r2, r3, *outs):
    rows = (r0, r1, r2, r3)
    start = jnp.zeros((ONE, LANES), F32)
    for r, plane in ((2, p3), (1, p2), (0, p1)):
        start = jnp.where(place[4] > r, joined_one(start, plane[...]), start)
    for h in range(NH):

        @pl.when(place[3] == h)
        def _(h=h):
            state = start
            for j in range(NH):
                k = (h - j) % NH
                outs[k][...] = state
                if j < NH - 1:
                    state = joined_one(state, rows[k][...])


def chips_back_kernel(place, e0, e1, e2, e3, own, near, *refs):
    tables, outs = (refs[:NX], refs[NX : 2 * NX]), (refs[2 * NX : 3 * NX], refs[3 * NX : 4 * NX])
    came = refs[-1]
    for r, e in enumerate((e0, e1, e2, e3)):
        came[lax.rem(place[3] + r, NH)] = e[...]
    first = place[2] == 0
    sub = iota((8, LANES), 0)
    tail0 = jnp.zeros((8, LANES), F32)
    for i in range(FOUR):
        tail0 = jnp.where(sub == i, came[i, LANES : LANES + 1, :], tail0)
    between = jnp.where(first, own[TAIL:, :], near[TAIL:, :])
    keep = keep_of(between)
    tail1 = joined_tail(tail0, between)
    for x in range(NX):

        @pl.when(place[1] == x)
        def _(x=x):
            for dz in range(NL):
                order = [(x - j) % NX for j in range(NX)]
                tails = [tables[dz][k][TAIL:, :] for k in order[:-1]]
                keeps = [keep_of(t) for t in tails]
                late = first if dz else jnp.logical_not(first)
                for i in range(FOUR):
                    at = slice(i * LANES, (i + 1) * LANES)
                    state = came[i, :LANES, :]
                    second = joined_sums(
                        keep, FOUR + i, state, jnp.where(first, own[at, :], near[at, :])
                    )
                    state = jnp.where(late, second, state)
                    for j, k in enumerate(order):
                        outs[dz][k][at, :] = state
                        if j < NX - 1:
                            state = joined_sums(
                                keeps[j], FOUR + i, state, sums_of(tables[dz][k], i)
                            )
                tail = jnp.where(late, tail1, tail0)
                for j, k in enumerate(order):
                    outs[dz][k][TAIL:, :] = tail
                    if j < NX - 1:
                        tail = joined_tail(tail, tails[j])


def cores_back_kernel(place, ready, *refs):
    n = (len(refs) - 2) // 4
    parts, mine, got = refs[: 2 * n], refs[2 * n : 3 * n], refs[3 * n : 4 * n]
    keep_out, send = refs[4 * n :]
    first = place[0] == 0
    counts_only = iota((8, LANES), 0) < FOUR
    for d in range(n):
        for dz in range(NL):
            part, at = parts[2 * d + dz], 2 * d + dz
            core0 = jnp.where(first, mine[d][dz, TAIL:, :], got[d][dz, TAIL:, :])
            keep = keep_of(core0)
            for i in range(FOUR):
                rows = slice(i * LANES, (i + 1) * LANES)
                state = part[rows, :]
                second = joined_sums(
                    keep, FOUR + i, state,
                    jnp.where(first, mine[d][dz, rows, :], got[d][dz, rows, :]),
                )
                keep_out[at, rows, :] = jnp.where(first, state, second)
                send[at, rows, :] = jnp.where(first, second, state)
            state = part[TAIL:, :]
            second = joined_tail(state, core0)
            keep_out[at, TAIL:, :] = jnp.where(counts_only, jnp.where(first, state, second), 0.0)
            send[at, TAIL:, :] = jnp.where(counts_only, jnp.where(first, second, state), 0.0)


BACK = ((2, 0), (1,), (3,))


def lookup(home8, account8, held, came):
    for tail, at in held:
        for i in range(FOUR):
            row = jnp.broadcast_to(tail[i : i + 1, :], (8, LANES))
            found = jnp.take_along_axis(row, account8, axis=1)
            came = jnp.where(home8 == at * FOUR + i, found, came)
    return came


def held_parts(place, dxs, side, own_half):
    half_of = place[0] if own_half else 1 - place[0]
    return [
        (side, 2 * d + dz, half_of * CHUNKS + chunk_of(place, dz, dx))
        for d, dx in enumerate(dxs)
        for dz in range(NL)
    ]


def gather_kernel(place, home, account, *refs):
    n = len(BACK)
    sides, (table, counts, sems) = refs[: n + 1], refs[n + 1 :]
    held = []
    for s, side in enumerate(sides):
        held += held_parts(place, BACK[s % n], side, s < n)
    copies = [
        pltpu.make_async_copy(side.at[k], table.at[at], sems.at[i])
        for i, (side, k, at) in enumerate(held)
    ]
    for copy in copies:
        copy.start()
    tails = [(side[k, TAIL:, :], at) for side, k, at in held]
    for t in range(home.shape[0] // 8):
        rows = slice(8 * t, 8 * t + 8)
        counts[rows, :] = lookup(
            home[rows, :], account[rows, :], tails, jnp.zeros((8, LANES), F32)
        )
    for copy in copies:
        copy.wait()


def finish_kernel(
    place, users, run, count, is_open, home, account, counts, table_in, got1, got2,
    table, out, picked, sems, out_sems,
):
    held = []
    for s, side in ((1, got1), (2, got2)):
        held += held_parts(place, BACK[s], side, False)
    copies = [
        pltpu.make_async_copy(side.at[k], table.at[at], sems.at[i])
        for i, (side, k, at) in enumerate(held)
    ]
    for copy in copies:
        copy.start()
    lines = home.shape[0]
    flat = table.reshape(NC * CHUNKS * ROWS, LANES)
    tails = [(side[k, TAIL:, :], at) for side, k, at in held]
    scale = []
    for t in range(lines // 8):
        rows = slice(8 * t, 8 * t + 8)
        came = lookup(home[rows, :], account[rows, :], tails, counts[rows, :])
        scale.append(1.0 / (count[rows, :] + is_open[rows, :] * came))
    scale = jnp.concatenate(scale, axis=0)
    if lines < LANES:
        scale = jnp.concatenate([scale, jnp.zeros((LANES - lines, LANES), F32)], axis=0)
    scale = scale.T
    for copy in copies:
        copy.wait()

    def pick(b, _):
        for j in range(LANES):
            picked[pl.ds(b * LANES + j, 1), :] = flat[pl.ds(users[b, j], 1), :]
        return 0

    lax.fori_loop(0, lines, pick, 0)
    group = lines // 8
    leaving = []
    for b in range(lines):
        at = pl.ds(b * LANES, LANES)
        factor = jnp.broadcast_to(scale[:, b : b + 1], (LANES, LANES))
        picked[at, :] = (run[at, :] + picked[at, :]) * factor
        if b % group == group - 1:
            rows = pl.ds((b - group + 1) * LANES, group * LANES)
            leaving.append(
                pltpu.make_async_copy(
                    picked.at[rows, :], out.at[rows, :], out_sems.at[len(leaving)]
                )
            )
            leaving[-1].start()
    for copy in leaving:
        copy.wait()


def ring(n, k):
    return [(i, (i + k) % n) for i in range(n)]


def body(features, home, account, flags):
    rows = features.shape[0]
    lines = rows // LANES
    home = home.reshape(lines, LANES)
    account = account.reshape(lines, LANES)
    flags = flags.reshape(lines, LANES)
    spot, place = iota((8,), 0), jnp.zeros((8,), I32)
    for n, axis in enumerate(("c", "x", "l", "h", "y")):
        place = jnp.where(spot == n, lax.axis_index(axis).astype(I32), place)
    small = jax.ShapeDtypeStruct((lines, LANES), I32)
    small_f = jax.ShapeDtypeStruct((lines, LANES), F32)
    by_owner = functools.partial(jax.ShapeDtypeStruct, (OWNERS, LANES))
    by_slot = jax.ShapeDtypeStruct((OWNERS * LANES, LANES), F32)
    slot, acc_rows, flag_rows, cleared = call(
        rank_kernel,
        [small, by_owner(I32), by_owner(F32), by_slot],
        (jnp.concatenate([home, account, flags]),),
        [VMEM],
        cost=2_000_000_000,
    )
    grouped = call(
        spread_kernel,
        by_slot,
        (slot, features, cleared),
        [VMEM] * 3,
        scratch=[pltpu.SMEM((lines, LANES), I32), pltpu.SemaphoreType.DMA],
        cost=4_000_000_000,
        aliases={2: 0},
    )
    swap = ring(NC, 1)

    def exchange(v, dz, dx):
        if dz == 0 and dx == 0:
            return v
        pairs = [
            (row * NX + x, (row ^ dz) * NX + (x + dx) % NX) for row in range(NL) for x in range(NX)
        ]
        return lax.ppermute(v, ("l", "x"), pairs)

    order = (2, 1, 3, 0)
    mine, got = [None] * NX, [None] * NX
    tables = [[None] * NX for _ in range(NL)]

    def meet(dx):
        chunks = call(core_kernel, [block()] * NL, (place, mine[dx], got[dx]),
                      [SMEM, VMEM, VMEM], cost=500_000_000)
        for dz in reversed(range(NL)):
            tables[dz][dx] = exchange(chunks[dz], dz, dx)
        return chunks[0]

    met = [acc_rows]
    for at, dx in enumerate(order):
        other, mine[dx] = call(
            functools.partial(closing_kernel, dx),
            [block(NL)] * 2,
            (place, acc_rows, flag_rows, grouped, met[at]),
            [SMEM] + [VMEM] * 3 + [ANY],
            cost=1_500_000_000,
        )
        got[dx] = lax.ppermute(other, "c", swap)
        met.append(meet(order[at - 1]) if at else mine[dx])
    met.append(meet(order[-1]))
    run_slots, counts, opens = call(
        running_kernel,
        [by_slot, by_owner(F32), by_owner(F32)],
        (acc_rows, flag_rows, grouped, met[-1]),
        [VMEM] * 3 + [ANY],
        cost=8_000_000_000,
    )
    own, near, *pairs = call(
        row_kernel,
        [block()] * NL + [one_block()] * NH,
        (place, *tables[0], *tables[1], counts),
        [SMEM] + [VMEM] * (NL * NX) + [ANY],
        scratch=[pltpu.VMEM((NH, ONE, LANES), F32)],
    )
    rows_got = list(pairs)
    for r in (1, 3, 2):
        rows_got[r] = lax.ppermute(pairs[r], "h", ring(NH, r))
    plane = call(plane_kernel, one_block(), (place, *rows_got), [SMEM] + [VMEM] * NH)
    ny = lax.axis_size("y")
    planes = [
        lax.ppermute(plane, "y", [(i, i + r) for i in range(ny - r)]) for r in range(1, ny)
    ]
    came = call(rows_back_kernel, [one_block()] * NH, (place, *planes, *rows_got),
                [SMEM] + [VMEM] * (3 + NH))
    came = list(came)
    for r in (1, 3, 2):
        came[r] = lax.ppermute(came[r], "h", ring(NH, -r))
    parts = call(
        chips_back_kernel,
        [block()] * (NL * NX),
        (place, *came, own, near, *tables[0], *tables[1]),
        [SMEM] + [VMEM] * (NH + NL + NL * NX),
        scratch=[pltpu.VMEM((NH, ONE, LANES), F32)],
    )
    parts = [list(parts[:NX]), list(parts[NX:])]
    kept = parts[0][0]
    for dx in (2, 0, 1, 3):
        for dz in reversed(range(NL)):
            parts[dz][dx] = exchange(parts[dz][dx], dz, (NX - dx) % NX)
    run, count, is_open, users = call(
        in_time_kernel,
        [jax.ShapeDtypeStruct((rows, LANES), F32), small_f, small_f, small],
        (slot, slot, home, account, run_slots, counts, opens, kept),
        [SMEM] + [VMEM] * 6 + [ANY],
        cost=10_000_000_000,
    )
    keep, last = [], []
    for dxs in BACK:
        stay, send = call(
            cores_back_kernel,
            [block(2 * len(dxs))] * 2,
            (place, keep[-1] if keep else count, *[parts[dz][dx] for dx in dxs for dz in range(NL)],
             *[mine[dx] for dx in dxs], *[got[dx] for dx in dxs]),
            [SMEM, ANY] + [VMEM] * (4 * len(dxs)),
            cost=500_000_000,
        )
        keep.append(stay)
        last.append(lax.ppermute(send, "c", swap))
    table, came_counts = call(
        gather_kernel,
        [block(NC * CHUNKS), small_f],
        (place, home, account, *keep, last[0]),
        [SMEM] + [VMEM] * 6,
        scratch=[pltpu.SemaphoreType.DMA((12,))],
        cost=2_000_000_000,
    )
    _, result = call(
        finish_kernel,
        [block(NC * CHUNKS), jax.ShapeDtypeStruct((rows, LANES), F32)],
        (place, users, run, count, is_open, home, account, came_counts, table, *last[1:]),
        [SMEM, SMEM] + [VMEM] * 9,
        out_specs=[VMEM, ANY],
        scratch=[pltpu.VMEM((rows, LANES), F32), pltpu.SemaphoreType.DMA((4,)),
                 pltpu.SemaphoreType.DMA((8,))],
        aliases={8: 0},
    )
    return result


def solution(mesh):
    axes = ("y", "h", "l", "x", "c")
    split = Mesh(mesh.devices.reshape(-1, NH, NL, NX, NC), axes)
    return jax.shard_map(
        body,
        mesh=split,
        in_specs=(P(axes, None), P(axes, None), P(axes), P(axes)),
        out_specs=P(axes, None),
        check_vma=False,
    )
```

```python
import functools

import jax
import jax.numpy as jnp
from jax import lax
from jax.experimental import pallas as pl
from jax.experimental.pallas import tpu as pltpu
from jax.sharding import Mesh, PartitionSpec as P


LANES = 128
FOUR = 4
TAIL = FOUR * LANES
ROWS = TAIL + 8
ONE = LANES + 8
NH, NL, NX, NC = 4, 2, 4, 2
OWNERS = NH * NL * NX * NC
HALF = OWNERS // NC
CHUNKS = HALF // FOUR
BF16, F32, I32 = jnp.bfloat16, jnp.float32, jnp.int32
VMEM = pl.BlockSpec(memory_space=pltpu.VMEM)
SMEM = pl.BlockSpec(memory_space=pltpu.SMEM)
HBM = pl.BlockSpec(memory_space=pltpu.HBM)
ANY = pl.BlockSpec(memory_space=pl.ANY)


def dot(a, b):
    return lax.dot_general(a, b, (((1,), (0,)), ((), ())), preferred_element_type=F32)


def dot_nt(a, b):
    return lax.dot_general(a, b, (((1,), (1,)), ((), ())), preferred_element_type=F32)


def iota(shape, dim):
    return lax.broadcasted_iota(I32, shape, dim)


def as_bf16(mask):
    return jnp.where(mask, 1.0, 0.0).astype(BF16)


def two_parts(v):
    high = v.astype(BF16)
    low = (v - high.astype(F32)).astype(BF16)
    return jnp.concatenate([high, low], axis=1)


def masked_sum(mask, parts):
    both = dot(mask, parts)
    return both[:, :LANES] + both[:, LANES:]


def call(kernel, out, args, specs, out_specs=None, scratch=(), cost=1_000_000, limit=24, aliases=None):
    return pl.pallas_call(
        kernel,
        out_shape=out,
        in_specs=specs,
        out_specs=out_specs or jax.tree.map(lambda _: VMEM, out),
        scratch_shapes=list(scratch),
        input_output_aliases=aliases or {},
        cost_estimate=pl.CostEstimate(flops=cost, bytes_accessed=1_000_000, transcendentals=0),
        compiler_params=pltpu.CompilerParams(vmem_limit_bytes=limit << 20),
    )(*args)


class Place:
    def __getitem__(self, n):
        return lax.axis_index(("c", "x", "l", "h", "y")[n])


PLACE = Place()


def block(*lead):
    return jax.ShapeDtypeStruct((*lead, ROWS, LANES), F32)


def one_block(*lead):
    return jax.ShapeDtypeStruct((*lead, ONE, LANES), F32)


def chunk_of(dz, dx):
    row = jnp.where(PLACE[2] == 0, dz, 1 - dz)
    return row * NX + lax.rem(PLACE[1] + dx, NX)


def rank_kernel(events, slot_out, acc_out, flag_out, cleared):
    lines = slot_out.shape[0]
    zero = jnp.zeros((LANES, LANES), F32)
    below = as_bf16(iota((LANES, LANES), 0) < iota((LANES, LANES), 1))
    with_total = jnp.concatenate([below, jnp.ones((LANES, LANES), BF16)], axis=1)
    owner_ids = iota((OWNERS, LANES), 0)
    before = jnp.zeros((OWNERS, LANES), F32)
    codes = jnp.zeros((OWNERS, LANES), F32)
    each = cleared.shape[0] // LANES // lines
    step = 8
    for b in range(0, lines, step):
        homes = [events[b + i : b + i + 1, :] for i in range(step)]
        chosen = [owner_ids == home for home in homes]
        counted = dot(jnp.concatenate([as_bf16(c) for c in chosen], axis=0), with_total)
        coded, rank_of = [], []
        for i in range(step):
            some = counted[i * OWNERS : (i + 1) * OWNERS, :]
            rank = jnp.sum(
                jnp.where(chosen[i], some[:, :LANES] + before, 0.0), axis=0, keepdims=True
            ).astype(I32)
            before = before + some[:, LANES:]
            slot_out[b + i : b + i + 1, :] = homes[i] * LANES + rank
            account = events[lines + b + i : lines + b + i + 1, :]
            flag = events[2 * lines + b + i : 2 * lines + b + i + 1, :]
            code = (account * 2 + flag + 1).astype(F32)
            coded.append(jnp.where(chosen[i], code, 0.0).astype(BF16))
            rank_of.append(as_bf16(iota((LANES, LANES), 0) == rank))
        codes = codes + dot_nt(
            jnp.concatenate(coded, axis=1), jnp.concatenate(rank_of, axis=1)
        )
        for i in range(step * each):
            at = (b * each + i) * LANES
            cleared[at : at + LANES, :] = zero
    code_ids = codes.astype(I32) - 1
    acc_out[...] = jnp.right_shift(code_ids, 1)
    flag_out[...] = jnp.where(code_ids >= 0, jnp.bitwise_and(code_ids, 1), 0).astype(F32)


def spread_kernel(slot_rows, features, cleared, grouped, slots, sem):
    copy = pltpu.make_async_copy(slot_rows, slots, sem)
    copy.start()
    copy.wait()

    def spread(b, _):
        for j in range(LANES):
            grouped[pl.ds(slots[b, j], 1), :] = features[pl.ds(b * LANES + j, 1), :]
        return 0

    lax.fori_loop(0, slot_rows.shape[0], spread, 0)


def after_and_ones():
    after = as_bf16(iota((LANES, LANES), 0) > iota((LANES, LANES), 1))
    return jnp.concatenate([after, jnp.ones((LANES, LANES), BF16)], axis=1)


def cut(v, i):
    return v[i * LANES : (i + 1) * LANES, :]


def counted_rows(counted, flagged):
    count = dot(jnp.concatenate(counted, axis=0), jnp.ones((LANES, LANES), BF16))
    lane = iota((LANES, LANES), 1)
    both = jnp.zeros((LANES, LANES), F32)
    for i in range(8):
        both = jnp.where(lane == i, cut(count, i), both)
        both = jnp.where(lane == 8 + i, cut(flagged, i), both)
    return both.T


def closing_kernel(dx, acc_rows, flag_rows, grouped, ready, other, mine):
    sides = after_and_ones()
    for out, half_of in ((other, 1 - PLACE[0]), (mine, PLACE[0])):
        bases = [half_of * HALF + chunk_of(dz, dx) * FOUR for dz in range(NL)]
        acc8 = jnp.concatenate([acc_rows[pl.ds(b, FOUR), :] for b in bases], axis=0)
        flag8 = jnp.concatenate([flag_rows[pl.ds(b, FOUR), :] for b in bases], axis=0)
        member = [iota((LANES, LANES), 0) == acc8[i : i + 1, :] for i in range(8)]
        member_flags = [
            jnp.where(member[i], flag8[i : i + 1, :], 0.0).astype(BF16) for i in range(8)
        ]
        flagged = dot(jnp.concatenate(member_flags, axis=0), sides)
        counted = [as_bf16(member[i] & (cut(flagged, i)[:, :LANES] < 0.5)) for i in range(8)]
        rows = counted_rows(counted, flagged[:, LANES:])
        marks = jnp.minimum(rows[8:16, :], 1.0)
        for dz in range(NL):
            for i in range(FOUR):
                at = pl.multiple_of((bases[dz] + i) * LANES, LANES)
                values = two_parts(grouped[pl.ds(at, LANES), :])
                out[dz, i * LANES : (i + 1) * LANES, :] = masked_sum(
                    counted[dz * FOUR + i], values
                )
            own = slice(dz * FOUR, dz * FOUR + FOUR)
            out[dz, TAIL:, :] = jnp.concatenate([rows[own, :], marks[own, :]], axis=0)


def running_kernel(acc_rows, flag_rows, grouped, ready, run, counts, opens):
    sides = after_and_ones()
    up_to = iota((LANES, LANES), 1) <= iota((LANES, LANES), 0)

    def some(g, _):
        rows = pl.ds(pl.multiple_of(g * 8, 8), 8)
        acc8 = acc_rows[rows, :].astype(F32)
        flag8 = flag_rows[rows, :]
        acc_cols = acc8.T
        same = []
        for i in range(8):
            acc_col = jnp.broadcast_to(acc_cols[:, i : i + 1], (LANES, LANES))
            same.append((acc_col == acc8[i : i + 1, :]) & (acc_col >= 0.0) & up_to)
        same_flags = [
            jnp.where(same[i], flag8[i : i + 1, :], 0.0).astype(BF16) for i in range(8)
        ]
        flagged = dot(jnp.concatenate(same_flags, axis=0), sides)
        session = [as_bf16(same[i] & (cut(flagged, i)[:, :LANES] < 0.5)) for i in range(8)]
        for i in range(8):
            at = pl.ds(pl.multiple_of((g * 8 + i) * LANES, LANES), LANES)
            run[at, :] = masked_sum(session[i], two_parts(grouped[at, :]))
        found = counted_rows(session, flagged[:, LANES:])
        counts[rows, :] = found[:8, :]
        opens[rows, :] = jnp.where(found[8:16, :] < 0.5, 1.0, 0.0)
        return 0

    lax.fori_loop(0, OWNERS // 8, some, 0)


def in_time_kernel(
    slots, slot_rows, home, account, run, counts, opens, ready,
    run_out, count_out, open_out, user_out,
):
    lines = home.shape[0]

    def scalars(t, _):
        rows = pl.ds(pl.multiple_of(t * 8, 8), 8)
        home8 = home[rows, :]
        rank = slot_rows[rows, :] - home8 * LANES
        count = jnp.zeros((8, LANES), F32)
        is_open = jnp.zeros((8, LANES), F32)
        for o in range(OWNERS):
            here = home8 == o
            for_count = jnp.broadcast_to(counts[o : o + 1, :], (8, LANES))
            for_open = jnp.broadcast_to(opens[o : o + 1, :], (8, LANES))
            count = jnp.where(here, jnp.take_along_axis(for_count, rank, axis=1), count)
            is_open = jnp.where(here, jnp.take_along_axis(for_open, rank, axis=1), is_open)
        count_out[rows, :] = count
        open_out[rows, :] = is_open
        chunk = jnp.right_shift(home8, 2)
        row = (home8 - chunk * FOUR) * LANES + account[rows, :]
        user_out[rows, :] = chunk * ROWS + jnp.where(is_open > 0.5, row, TAIL + FOUR)
        return 0

    lax.fori_loop(0, lines // 8, scalars, 0)

    def collect(b, _):
        for j in range(LANES):
            run_out[pl.ds(b * LANES + j, 1), :] = run[pl.ds(slots[b, j], 1), :]
        return 0

    lax.fori_loop(0, lines, collect, 0)


def sums_of(chunk, i):
    return chunk[i * LANES : (i + 1) * LANES, :]


def keep_of(tail):
    return (1.0 - tail).T


def joined_sums(keep, i, earlier, later):
    return later + jnp.broadcast_to(keep[:, i : i + 1], (LANES, LANES)) * earlier


def joined_tail(earlier, later):
    marks = jnp.concatenate([later[FOUR:, :], later[:FOUR, :]], axis=0)
    return jnp.where(
        iota((8, LANES), 0) < FOUR, later + (1.0 - marks) * earlier, jnp.maximum(later, earlier)
    )


def joined_one(earlier, later):
    tail, first = later[LANES:, :], earlier[LANES:, :]
    mark = tail[1:2, :]
    sub = iota((8, LANES), 0)
    sums = joined_sums(keep_of(tail), 1, earlier[:LANES, :], later[:LANES, :])
    tail = jnp.where(
        sub == 0, tail + (1.0 - mark) * first, jnp.where(sub == 1, jnp.maximum(tail, first), 0.0)
    )
    return jnp.concatenate([sums, tail], axis=0)


def core_kernel(mine, got, *outs):
    first = PLACE[0] == 0
    for dz in range(NL):
        a, b = mine[dz, TAIL:, :], got[dz, TAIL:, :]
        early, late = jnp.where(first, a, b), jnp.where(first, b, a)
        keep = keep_of(late)
        for i in range(FOUR):
            at = slice(i * LANES, (i + 1) * LANES)
            a, b = mine[dz, at, :], got[dz, at, :]
            outs[dz][at, :] = joined_sums(
                keep, FOUR + i, jnp.where(first, a, b), jnp.where(first, b, a)
            )
        outs[dz][TAIL:, :] = joined_tail(early, late)


def row_kernel(*refs):
    tables = (refs[:NX], refs[NX : 2 * NX])
    totals = refs[2 * NX + 1 : 2 * NX + 3]
    outs, pair = refs[2 * NX + 3 : 2 * NX + 3 + NH], refs[-1]
    for x in range(NX):

        @pl.when(PLACE[1] == x)
        def _(x=x):
            for dz in range(NL):
                order = [tables[dz][(x - j) % NX] for j in range(NX)]
                tails = [t[TAIL:, :] for t in order]
                keep = [keep_of(t) for t in tails]
                for i in range(FOUR):
                    total = sums_of(order[0], i)
                    for j in range(1, NX):
                        total = joined_sums(keep[j], FOUR + i, total, sums_of(order[j], i))
                    totals[dz][i * LANES : (i + 1) * LANES, :] = total
                tail = tails[0]
                for j in range(1, NX):
                    tail = joined_tail(tail, tails[j])
                totals[dz][TAIL:, :] = tail

    own, near = totals
    first = PLACE[2] == 0
    a, b = own[TAIL:, :], near[TAIL:, :]
    early, late = jnp.where(first, a, b), jnp.where(first, b, a)
    keep = keep_of(late)
    tail = joined_tail(early, late)
    sub = iota((8, LANES), 0)
    for i in range(FOUR):
        a, b = sums_of(own, i), sums_of(near, i)
        pair[i, :LANES, :] = joined_sums(
            keep, FOUR + i, jnp.where(first, a, b), jnp.where(first, b, a)
        )
        pair[i, LANES:, :] = jnp.where(
            sub == 0, tail[i : i + 1, :],
            jnp.where(sub == 1, tail[FOUR + i : FOUR + i + 1, :], 0.0),
        )
    for r in range(NH):
        outs[r][...] = pair[lax.rem(PLACE[3] + r, NH)]


def plane_kernel(r0, r1, r2, r3, out):
    rows = (r0, r1, r2, r3)
    for h in range(NH):

        @pl.when(PLACE[3] == h)
        def _(h=h):
            total = rows[h][...]
            for j in range(1, NH):
                total = joined_one(total, rows[(h - j) % NH][...])
            out[...] = total


def rows_back_kernel(p1, p2, p3, r0, r1, r2, r3, *outs):
    rows = (r0, r1, r2, r3)
    start = jnp.zeros((ONE, LANES), F32)
    for r, plane in ((2, p3), (1, p2), (0, p1)):
        start = jnp.where(PLACE[4] > r, joined_one(start, plane[...]), start)
    for h in range(NH):

        @pl.when(PLACE[3] == h)
        def _(h=h):
            state = start
            for j in range(NH):
                k = (h - j) % NH
                outs[k][...] = state
                if j < NH - 1:
                    state = joined_one(state, rows[k][...])


def chips_back_kernel(e0, e1, e2, e3, own, near, *refs):
    tables, outs = (refs[:NX], refs[NX : 2 * NX]), (refs[2 * NX : 3 * NX], refs[3 * NX : 4 * NX])
    came = refs[-1]
    for r, e in enumerate((e0, e1, e2, e3)):
        came[lax.rem(PLACE[3] + r, NH)] = e[...]
    first = PLACE[2] == 0
    sub = iota((8, LANES), 0)
    tail0 = jnp.zeros((8, LANES), F32)
    for i in range(FOUR):
        tail0 = jnp.where(sub == i, came[i, LANES : LANES + 1, :], tail0)
    between = jnp.where(first, own[TAIL:, :], near[TAIL:, :])
    keep = keep_of(between)
    tail1 = joined_tail(tail0, between)
    for x in range(NX):

        @pl.when(PLACE[1] == x)
        def _(x=x):
            for dz in range(NL):
                order = [(x - j) % NX for j in range(NX)]
                tails = [tables[dz][k][TAIL:, :] for k in order[:-1]]
                keeps = [keep_of(t) for t in tails]
                late = first if dz else jnp.logical_not(first)
                for i in range(FOUR):
                    at = slice(i * LANES, (i + 1) * LANES)
                    state = came[i, :LANES, :]
                    second = joined_sums(
                        keep, FOUR + i, state, jnp.where(first, own[at, :], near[at, :])
                    )
                    state = jnp.where(late, second, state)
                    for j, k in enumerate(order):
                        outs[dz][k][at, :] = state
                        if j < NX - 1:
                            state = joined_sums(
                                keeps[j], FOUR + i, state, sums_of(tables[dz][k], i)
                            )
                tail = jnp.where(late, tail1, tail0)
                for j, k in enumerate(order):
                    outs[dz][k][TAIL:, :] = tail
                    if j < NX - 1:
                        tail = joined_tail(tail, tails[j])


def cores_back_kernel(ready, *refs):
    n = (len(refs) - 2) // 4
    parts, mine, got = refs[: 2 * n], refs[2 * n : 3 * n], refs[3 * n : 4 * n]
    keep_out, send = refs[4 * n :]
    first = PLACE[0] == 0
    counts_only = iota((8, LANES), 0) < FOUR
    for d in range(n):
        for dz in range(NL):
            part, at = parts[2 * d + dz], 2 * d + dz
            core0 = jnp.where(first, mine[d][dz, TAIL:, :], got[d][dz, TAIL:, :])
            keep = keep_of(core0)
            for i in range(FOUR):
                rows = slice(i * LANES, (i + 1) * LANES)
                state = part[rows, :]
                second = joined_sums(
                    keep, FOUR + i, state,
                    jnp.where(first, mine[d][dz, rows, :], got[d][dz, rows, :]),
                )
                keep_out[at, rows, :] = jnp.where(first, state, second)
                send[at, rows, :] = jnp.where(first, second, state)
            state = part[TAIL:, :]
            second = joined_tail(state, core0)
            keep_out[at, TAIL:, :] = jnp.where(counts_only, jnp.where(first, state, second), 0.0)
            send[at, TAIL:, :] = jnp.where(counts_only, jnp.where(first, second, state), 0.0)


BACK = ((2, 0), (1,), (3,))


def lookup(home8, account8, held, came):
    for tail, at in held:
        for i in range(FOUR):
            row = jnp.broadcast_to(tail[i : i + 1, :], (8, LANES))
            found = jnp.take_along_axis(row, account8, axis=1)
            came = jnp.where(home8 == at * FOUR + i, found, came)
    return came


def held_parts(dxs, side, own_half):
    half_of = PLACE[0] if own_half else 1 - PLACE[0]
    return [
        (side, 2 * d + dz, half_of * CHUNKS + chunk_of(dz, dx))
        for d, dx in enumerate(dxs)
        for dz in range(NL)
    ]


def gather_kernel(home, account, *refs):
    n = len(BACK)
    sides, (table, counts, sems) = refs[: n + 1], refs[n + 1 :]
    held = []
    for s, side in enumerate(sides):
        held += held_parts(BACK[s % n], side, s < n)
    copies = [
        pltpu.make_async_copy(side.at[k], table.at[at], sems.at[i])
        for i, (side, k, at) in enumerate(held)
    ]
    for copy in copies:
        copy.start()
    tails = [(side[k, TAIL:, :], at) for side, k, at in held]
    for t in range(home.shape[0] // 8):
        rows = slice(8 * t, 8 * t + 8)
        counts[rows, :] = lookup(
            home[rows, :], account[rows, :], tails, jnp.zeros((8, LANES), F32)
        )
    for copy in copies:
        copy.wait()


def finish_kernel(
    user_rows, run, count, is_open, home, account, counts, table_in, got1, got2,
    table, out, picked, users, sems, out_sems,
):
    listed = pltpu.make_async_copy(user_rows, users, sems.at[4])
    listed.start()
    held = []
    for s, side in ((1, got1), (2, got2)):
        held += held_parts(BACK[s], side, False)
    copies = [
        pltpu.make_async_copy(side.at[k], table.at[at], sems.at[i])
        for i, (side, k, at) in enumerate(held)
    ]
    for copy in copies:
        copy.start()
    lines = home.shape[0]
    flat = table.reshape(NC * CHUNKS * ROWS, LANES)
    tails = [(side[k, TAIL:, :], at) for side, k, at in held]
    scale = []
    for t in range(lines // 8):
        rows = slice(8 * t, 8 * t + 8)
        came = lookup(home[rows, :], account[rows, :], tails, counts[rows, :])
        scale.append(1.0 / (count[rows, :] + is_open[rows, :] * came))
    scale = jnp.concatenate(scale, axis=0)
    if lines < LANES:
        scale = jnp.concatenate([scale, jnp.zeros((LANES - lines, LANES), F32)], axis=0)
    scale = scale.T
    for copy in (*copies, listed):
        copy.wait()

    def pick(b, _):
        for j in range(LANES):
            picked[pl.ds(b * LANES + j, 1), :] = flat[pl.ds(users[b, j], 1), :]
        return 0

    lax.fori_loop(0, lines, pick, 0)
    group = lines // 8
    leaving = []
    for b in range(lines):
        at = pl.ds(b * LANES, LANES)
        factor = jnp.broadcast_to(scale[:, b : b + 1], (LANES, LANES))
        picked[at, :] = (run[at, :] + picked[at, :]) * factor
        if b % group == group - 1:
            rows = pl.ds((b - group + 1) * LANES, group * LANES)
            leaving.append(
                pltpu.make_async_copy(
                    picked.at[rows, :], out.at[rows, :], out_sems.at[len(leaving)]
                )
            )
            leaving[-1].start()
    for copy in leaving:
        copy.wait()


def ring(n, k):
    return [(i, (i + k) % n) for i in range(n)]


def body(features, home, account, flags):
    rows = features.shape[0]
    lines = rows // LANES
    home = home.reshape(lines, LANES)
    account = account.reshape(lines, LANES)
    flags = flags.reshape(lines, LANES)
    small = jax.ShapeDtypeStruct((lines, LANES), I32)
    small_f = jax.ShapeDtypeStruct((lines, LANES), F32)
    by_owner = functools.partial(jax.ShapeDtypeStruct, (OWNERS, LANES))
    by_slot = jax.ShapeDtypeStruct((OWNERS * LANES, LANES), F32)
    slot, acc_rows, flag_rows, cleared = call(
        rank_kernel,
        [small, by_owner(I32), by_owner(F32), by_slot],
        (jnp.concatenate([home, account, flags]),),
        [VMEM],
        cost=2_000_000_000,
    )
    grouped = call(
        spread_kernel,
        by_slot,
        (slot, features, cleared),
        [VMEM] * 3,
        scratch=[pltpu.SMEM((lines, LANES), I32), pltpu.SemaphoreType.DMA],
        cost=4_000_000_000,
        aliases={2: 0},
    )
    swap = ring(NC, 1)

    def exchange(v, dz, dx):
        if dz == 0 and dx == 0:
            return v
        pairs = [
            (row * NX + x, (row ^ dz) * NX + (x + dx) % NX) for row in range(NL) for x in range(NX)
        ]
        return lax.ppermute(v, ("l", "x"), pairs)

    order = (2, 1, 3, 0)
    mine, got = [None] * NX, [None] * NX
    tables = [[None] * NX for _ in range(NL)]

    def meet(dx):
        chunks = call(core_kernel, [block()] * NL, (mine[dx], got[dx]),
                      [VMEM, VMEM], cost=500_000_000)
        for dz in reversed(range(NL)):
            tables[dz][dx] = exchange(chunks[dz], dz, dx)
        return chunks[0]

    met = [acc_rows]
    for at, dx in enumerate(order):
        other, mine[dx] = call(
            functools.partial(closing_kernel, dx),
            [block(NL)] * 2,
            (acc_rows, flag_rows, grouped, met[at]),
            [VMEM] * 3 + [ANY],
            cost=1_500_000_000,
        )
        got[dx] = lax.ppermute(other, "c", swap)
        met.append(meet(order[at - 1]) if at else mine[dx])
    met.append(meet(order[-1]))
    run_slots, counts, opens = call(
        running_kernel,
        [by_slot, by_owner(F32), by_owner(F32)],
        (acc_rows, flag_rows, grouped, met[-1]),
        [VMEM] * 3 + [ANY],
        cost=8_000_000_000,
    )
    own, near, *pairs = call(
        row_kernel,
        [block()] * NL + [one_block()] * NH,
        (*tables[0], *tables[1], counts),
        [VMEM] * (NL * NX) + [ANY],
        scratch=[pltpu.VMEM((NH, ONE, LANES), F32)],
    )
    rows_got = list(pairs)
    for r in (1, 3, 2):
        rows_got[r] = lax.ppermute(pairs[r], "h", ring(NH, r))
    plane = call(plane_kernel, one_block(), tuple(rows_got), [VMEM] * NH)
    ny = lax.axis_size("y")
    planes = [
        lax.ppermute(plane, "y", [(i, i + r) for i in range(ny - r)]) for r in range(1, ny)
    ]
    came = call(rows_back_kernel, [one_block()] * NH, (*planes, *rows_got),
                [VMEM] * (3 + NH))
    came = list(came)
    for r in (1, 3, 2):
        came[r] = lax.ppermute(came[r], "h", ring(NH, -r))
    parts = call(
        chips_back_kernel,
        [block()] * (NL * NX),
        (*came, own, near, *tables[0], *tables[1]),
        [VMEM] * (NH + NL + NL * NX),
        scratch=[pltpu.VMEM((NH, ONE, LANES), F32)],
    )
    parts = [list(parts[:NX]), list(parts[NX:])]
    kept = parts[0][0]
    for dx in (2, 0, 1, 3):
        for dz in reversed(range(NL)):
            parts[dz][dx] = exchange(parts[dz][dx], dz, (NX - dx) % NX)
    run, count, is_open, users = call(
        in_time_kernel,
        [jax.ShapeDtypeStruct((rows, LANES), F32), small_f, small_f, small],
        (slot, slot, home, account, run_slots, counts, opens, kept),
        [SMEM] + [VMEM] * 6 + [ANY],
        cost=10_000_000_000,
    )
    keep, last = [], []
    for dxs in BACK:
        stay, send = call(
            cores_back_kernel,
            [block(2 * len(dxs))] * 2,
            (keep[-1] if keep else count, *[parts[dz][dx] for dx in dxs for dz in range(NL)],
             *[mine[dx] for dx in dxs], *[got[dx] for dx in dxs]),
            [ANY] + [VMEM] * (4 * len(dxs)),
            cost=500_000_000,
        )
        keep.append(stay)
        last.append(lax.ppermute(send, "c", swap))
    table, came_counts = call(
        gather_kernel,
        [block(NC * CHUNKS), small_f],
        (home, account, *keep, last[0]),
        [VMEM] * 6,
        scratch=[pltpu.SemaphoreType.DMA((12,))],
        cost=2_000_000_000,
    )
    _, result = call(
        finish_kernel,
        [block(NC * CHUNKS), jax.ShapeDtypeStruct((rows, LANES), F32)],
        (users, run, count, is_open, home, account, came_counts, table, *last[1:]),
        [VMEM] * 10,
        out_specs=[VMEM, ANY],
        scratch=[pltpu.VMEM((rows, LANES), F32), pltpu.SMEM((lines, LANES), I32),
                 pltpu.SemaphoreType.DMA((5,)),
                 pltpu.SemaphoreType.DMA((8,))],
        aliases={7: 0},
    )
    return result


def solution(mesh):
    axes = ("y", "h", "l", "x", "c")
    split = Mesh(mesh.devices.reshape(-1, NH, NL, NX, NC), axes)
    return jax.shard_map(
        body,
        mesh=split,
        in_specs=(P(axes, None), P(axes, None), P(axes), P(axes)),
        out_specs=P(axes, None),
        check_vma=False,
    )
```

```python
import functools

import jax
import jax.numpy as jnp
from jax import lax
from jax.experimental import pallas as pl
from jax.experimental.pallas import tpu as pltpu
from jax.sharding import Mesh, PartitionSpec as P


LANES = 128
FOUR = 4
TAIL = FOUR * LANES
ROWS = TAIL + 8
ONE = LANES + 8
NH, NL, NX, NC = 4, 2, 4, 2
OWNERS = NH * NL * NX * NC
HALF = OWNERS // NC
CHUNKS = HALF // FOUR
BF16, F32, I32 = jnp.bfloat16, jnp.float32, jnp.int32
VMEM = pl.BlockSpec(memory_space=pltpu.VMEM)
SMEM = pl.BlockSpec(memory_space=pltpu.SMEM)
HBM = pl.BlockSpec(memory_space=pltpu.HBM)
ANY = pl.BlockSpec(memory_space=pl.ANY)


def dot(a, b):
    return lax.dot_general(a, b, (((1,), (0,)), ((), ())), preferred_element_type=F32)


def dot_nt(a, b):
    return lax.dot_general(a, b, (((1,), (1,)), ((), ())), preferred_element_type=F32)


def iota(shape, dim):
    return lax.broadcasted_iota(I32, shape, dim)


def as_bf16(mask):
    return jnp.where(mask, 1.0, 0.0).astype(BF16)


def two_parts(v):
    high = v.astype(BF16)
    low = (v - high.astype(F32)).astype(BF16)
    return jnp.concatenate([high, low], axis=1)


def masked_sum(mask, parts):
    both = dot(mask, parts)
    return both[:, :LANES] + both[:, LANES:]


def call(kernel, out, args, specs, out_specs=None, scratch=(), cost=1_000_000, limit=24, aliases=None):
    return pl.pallas_call(
        kernel,
        out_shape=out,
        in_specs=specs,
        out_specs=out_specs or jax.tree.map(lambda _: VMEM, out),
        scratch_shapes=list(scratch),
        input_output_aliases=aliases or {},
        cost_estimate=pl.CostEstimate(flops=cost, bytes_accessed=1_000_000, transcendentals=0),
        compiler_params=pltpu.CompilerParams(vmem_limit_bytes=limit << 20),
    )(*args)


class Place:
    def __getitem__(self, n):
        return lax.axis_index(("c", "x", "l", "h", "y")[n])


PLACE = Place()


def block(*lead):
    return jax.ShapeDtypeStruct((*lead, ROWS, LANES), F32)


def one_block(*lead):
    return jax.ShapeDtypeStruct((*lead, ONE, LANES), F32)


def chunk_of(dz, dx):
    return (PLACE[2] ^ dz) * NX + (PLACE[1] ^ dx)


def rank_kernel(events, slot_out, acc_out, flag_out):
    lines = slot_out.shape[0]
    below = as_bf16(iota((LANES, LANES), 0) < iota((LANES, LANES), 1))
    with_total = jnp.concatenate([below, jnp.ones((LANES, LANES), BF16)], axis=1)
    owner_ids = iota((OWNERS, LANES), 0)
    before = jnp.zeros((OWNERS, LANES), F32)
    codes = jnp.zeros((OWNERS, LANES), F32)
    step = 8
    for b in range(0, lines, step):
        homes = [events[b + i : b + i + 1, :] for i in range(step)]
        chosen = [owner_ids == home for home in homes]
        counted = dot(jnp.concatenate([as_bf16(c) for c in chosen], axis=0), with_total)
        coded, rank_of = [], []
        for i in range(step):
            some = counted[i * OWNERS : (i + 1) * OWNERS, :]
            rank = jnp.sum(
                jnp.where(chosen[i], some[:, :LANES] + before, 0.0), axis=0, keepdims=True
            ).astype(I32)
            before = before + some[:, LANES:]
            slot_out[b + i : b + i + 1, :] = homes[i] * LANES + rank
            account = events[lines + b + i : lines + b + i + 1, :]
            flag = events[2 * lines + b + i : 2 * lines + b + i + 1, :]
            code = (account * 2 + flag + 1).astype(F32)
            coded.append(jnp.where(chosen[i], code, 0.0).astype(BF16))
            rank_of.append(as_bf16(iota((LANES, LANES), 0) == rank))
        codes = codes + dot_nt(
            jnp.concatenate(coded, axis=1), jnp.concatenate(rank_of, axis=1)
        )
    code_ids = codes.astype(I32) - 1
    acc_out[...] = jnp.right_shift(code_ids, 1)
    flag_out[...] = jnp.where(code_ids >= 0, jnp.bitwise_and(code_ids, 1), 0).astype(F32)


def spread_kernel(slot_rows, features, grouped, slots, sem):
    copy = pltpu.make_async_copy(slot_rows, slots, sem)
    copy.start()
    zero = jnp.zeros((LANES, LANES), F32)

    def clear(o, _):
        grouped[pl.ds(pl.multiple_of(o * LANES, LANES), LANES), :] = zero
        return 0

    lax.fori_loop(0, OWNERS, clear, 0)
    copy.wait()

    def spread(b, _):
        for j in range(LANES):
            grouped[pl.ds(slots[b, j], 1), :] = features[pl.ds(b * LANES + j, 1), :]
        return 0

    lax.fori_loop(0, slot_rows.shape[0], spread, 0)


def after_and_ones():
    after = as_bf16(iota((LANES, LANES), 0) > iota((LANES, LANES), 1))
    return jnp.concatenate([after, jnp.ones((LANES, LANES), BF16)], axis=1)


def cut(v, i):
    return v[i * LANES : (i + 1) * LANES, :]


def counted_rows(counted, flagged):
    count = dot(jnp.concatenate(counted, axis=0), jnp.ones((LANES, LANES), BF16))
    lane = iota((LANES, LANES), 1)
    both = jnp.zeros((LANES, LANES), F32)
    for i in range(8):
        both = jnp.where(lane == i, cut(count, i), both)
        both = jnp.where(lane == 8 + i, cut(flagged, i), both)
    return both.T


def closing_kernel(dx, acc_rows, flag_rows, grouped, ready, other, mine):
    sides = after_and_ones()
    for out, half_of in ((other, 1 - PLACE[0]), (mine, PLACE[0])):
        bases = [half_of * HALF + chunk_of(dz, dx) * FOUR for dz in range(NL)]
        acc8 = jnp.concatenate([acc_rows[pl.ds(b, FOUR), :] for b in bases], axis=0)
        flag8 = jnp.concatenate([flag_rows[pl.ds(b, FOUR), :] for b in bases], axis=0)
        member = [iota((LANES, LANES), 0) == acc8[i : i + 1, :] for i in range(8)]
        member_flags = [
            jnp.where(member[i], flag8[i : i + 1, :], 0.0).astype(BF16) for i in range(8)
        ]
        flagged = dot(jnp.concatenate(member_flags, axis=0), sides)
        counted = [as_bf16(member[i] & (cut(flagged, i)[:, :LANES] < 0.5)) for i in range(8)]
        rows = counted_rows(counted, flagged[:, LANES:])
        marks = jnp.minimum(rows[8:16, :], 1.0)
        for dz in range(NL):
            for i in range(FOUR):
                at = pl.multiple_of((bases[dz] + i) * LANES, LANES)
                values = two_parts(grouped[pl.ds(at, LANES), :])
                out[dz, i * LANES : (i + 1) * LANES, :] = masked_sum(
                    counted[dz * FOUR + i], values
                )
            own = slice(dz * FOUR, dz * FOUR + FOUR)
            out[dz, TAIL:, :] = jnp.concatenate([rows[own, :], marks[own, :]], axis=0)


def running_kernel(acc_rows, flag_rows, grouped, ready, run, counts, opens):
    sides = after_and_ones()
    up_to = iota((LANES, LANES), 1) <= iota((LANES, LANES), 0)

    def some(g, _):
        rows = pl.ds(pl.multiple_of(g * 8, 8), 8)
        acc8 = acc_rows[rows, :].astype(F32)
        flag8 = flag_rows[rows, :]
        acc_cols = acc8.T
        same = []
        for i in range(8):
            acc_col = jnp.broadcast_to(acc_cols[:, i : i + 1], (LANES, LANES))
            same.append((acc_col == acc8[i : i + 1, :]) & (acc_col >= 0.0) & up_to)
        same_flags = [
            jnp.where(same[i], flag8[i : i + 1, :], 0.0).astype(BF16) for i in range(8)
        ]
        flagged = dot(jnp.concatenate(same_flags, axis=0), sides)
        session = [as_bf16(same[i] & (cut(flagged, i)[:, :LANES] < 0.5)) for i in range(8)]
        for i in range(8):
            at = pl.ds(pl.multiple_of((g * 8 + i) * LANES, LANES), LANES)
            run[at, :] = masked_sum(session[i], two_parts(grouped[at, :]))
        found = counted_rows(session, flagged[:, LANES:])
        counts[rows, :] = found[:8, :]
        opens[rows, :] = jnp.where(found[8:16, :] < 0.5, 1.0, 0.0)
        return 0

    lax.fori_loop(0, OWNERS // 8, some, 0)


def in_time_kernel(
    slots, slot_rows, home, account, run, counts, opens, ready,
    run_out, count_out, open_out, user_out,
):
    lines = home.shape[0]

    def scalars(t, _):
        rows = pl.ds(pl.multiple_of(t * 8, 8), 8)
        home8 = home[rows, :]
        rank = slot_rows[rows, :] - home8 * LANES
        count = jnp.zeros((8, LANES), F32)
        is_open = jnp.zeros((8, LANES), F32)
        for o in range(OWNERS):
            here = home8 == o
            for_count = jnp.broadcast_to(counts[o : o + 1, :], (8, LANES))
            for_open = jnp.broadcast_to(opens[o : o + 1, :], (8, LANES))
            count = jnp.where(here, jnp.take_along_axis(for_count, rank, axis=1), count)
            is_open = jnp.where(here, jnp.take_along_axis(for_open, rank, axis=1), is_open)
        count_out[rows, :] = count
        open_out[rows, :] = is_open
        chunk = jnp.right_shift(home8, 2)
        row = (home8 - chunk * FOUR) * LANES + account[rows, :]
        user_out[rows, :] = chunk * ROWS + jnp.where(is_open > 0.5, row, TAIL + FOUR)
        return 0

    lax.fori_loop(0, lines // 8, scalars, 0)

    def collect(b, _):
        for j in range(LANES):
            run_out[pl.ds(b * LANES + j, 1), :] = run[pl.ds(slots[b, j], 1), :]
        return 0

    lax.fori_loop(0, lines, collect, 0)


def sums_of(chunk, i):
    return chunk[i * LANES : (i + 1) * LANES, :]


def keep_of(tail):
    return (1.0 - tail).T


def joined_sums(keep, i, earlier, later):
    return later + jnp.broadcast_to(keep[:, i : i + 1], (LANES, LANES)) * earlier


def joined_tail(earlier, later):
    marks = jnp.concatenate([later[FOUR:, :], later[:FOUR, :]], axis=0)
    return jnp.where(
        iota((8, LANES), 0) < FOUR, later + (1.0 - marks) * earlier, jnp.maximum(later, earlier)
    )


def joined_one(earlier, later):
    tail, first = later[LANES:, :], earlier[LANES:, :]
    mark = tail[1:2, :]
    sub = iota((8, LANES), 0)
    sums = joined_sums(keep_of(tail), 1, earlier[:LANES, :], later[:LANES, :])
    tail = jnp.where(
        sub == 0, tail + (1.0 - mark) * first, jnp.where(sub == 1, jnp.maximum(tail, first), 0.0)
    )
    return jnp.concatenate([sums, tail], axis=0)


def core_kernel(mine, got, *outs):
    first = PLACE[0] == 0
    for dz in range(NL):
        a, b = mine[dz, TAIL:, :], got[dz, TAIL:, :]
        early, late = jnp.where(first, a, b), jnp.where(first, b, a)
        keep = keep_of(late)
        for i in range(FOUR):
            at = slice(i * LANES, (i + 1) * LANES)
            a, b = mine[dz, at, :], got[dz, at, :]
            outs[dz][at, :] = joined_sums(
                keep, FOUR + i, jnp.where(first, a, b), jnp.where(first, b, a)
            )
        outs[dz][TAIL:, :] = joined_tail(early, late)


def row_kernel(*refs):
    tables = (refs[:NX], refs[NX : 2 * NX])
    totals = refs[2 * NX + 1 : 2 * NX + 3]
    outs, pair = refs[2 * NX + 3 : 2 * NX + 3 + NH], refs[-1]
    for x in range(NX):

        @pl.when(PLACE[1] == x)
        def _(x=x):
            for dz in range(NL):
                order = [tables[dz][x ^ j] for j in range(NX)]
                tails = [t[TAIL:, :] for t in order]
                keep = [keep_of(t) for t in tails]
                for i in range(FOUR):
                    total = sums_of(order[0], i)
                    for j in range(1, NX):
                        total = joined_sums(keep[j], FOUR + i, total, sums_of(order[j], i))
                    totals[dz][i * LANES : (i + 1) * LANES, :] = total
                tail = tails[0]
                for j in range(1, NX):
                    tail = joined_tail(tail, tails[j])
                totals[dz][TAIL:, :] = tail

    own, near = totals
    first = PLACE[2] == 0
    a, b = own[TAIL:, :], near[TAIL:, :]
    early, late = jnp.where(first, a, b), jnp.where(first, b, a)
    keep = keep_of(late)
    tail = joined_tail(early, late)
    sub = iota((8, LANES), 0)
    for i in range(FOUR):
        a, b = sums_of(own, i), sums_of(near, i)
        pair[i, :LANES, :] = joined_sums(
            keep, FOUR + i, jnp.where(first, a, b), jnp.where(first, b, a)
        )
        pair[i, LANES:, :] = jnp.where(
            sub == 0, tail[i : i + 1, :],
            jnp.where(sub == 1, tail[FOUR + i : FOUR + i + 1, :], 0.0),
        )
    for r in range(NH):
        outs[r][...] = pair[PLACE[3] ^ r]


def plane_kernel(r0, r1, r2, r3, out):
    rows = (r0, r1, r2, r3)
    for h in range(NH):

        @pl.when(PLACE[3] == h)
        def _(h=h):
            total = rows[h][...]
            for j in range(1, NH):
                total = joined_one(total, rows[h ^ j][...])
            out[...] = total


def rows_back_kernel(p1, p2, p3, r0, r1, r2, r3, *outs):
    rows = (r0, r1, r2, r3)
    start = jnp.zeros((ONE, LANES), F32)
    for r, plane in ((2, p3), (1, p2), (0, p1)):
        start = jnp.where(PLACE[4] > r, joined_one(start, plane[...]), start)
    for h in range(NH):

        @pl.when(PLACE[3] == h)
        def _(h=h):
            state = start
            for j in range(NH):
                k = h ^ j
                outs[k][...] = state
                if j < NH - 1:
                    state = joined_one(state, rows[k][...])


def chips_back_kernel(e0, e1, e2, e3, own, near, *refs):
    tables, outs = (refs[:NX], refs[NX : 2 * NX]), (refs[2 * NX : 3 * NX], refs[3 * NX : 4 * NX])
    came = refs[-1]
    for r, e in enumerate((e0, e1, e2, e3)):
        came[PLACE[3] ^ r] = e[...]
    first = PLACE[2] == 0
    sub = iota((8, LANES), 0)
    tail0 = jnp.zeros((8, LANES), F32)
    for i in range(FOUR):
        tail0 = jnp.where(sub == i, came[i, LANES : LANES + 1, :], tail0)
    between = jnp.where(first, own[TAIL:, :], near[TAIL:, :])
    keep = keep_of(between)
    tail1 = joined_tail(tail0, between)
    for x in range(NX):

        @pl.when(PLACE[1] == x)
        def _(x=x):
            for dz in range(NL):
                order = [x ^ j for j in range(NX)]
                tails = [tables[dz][k][TAIL:, :] for k in order[:-1]]
                keeps = [keep_of(t) for t in tails]
                late = first if dz else jnp.logical_not(first)
                for i in range(FOUR):
                    at = slice(i * LANES, (i + 1) * LANES)
                    state = came[i, :LANES, :]
                    second = joined_sums(
                        keep, FOUR + i, state, jnp.where(first, own[at, :], near[at, :])
                    )
                    state = jnp.where(late, second, state)
                    for j, k in enumerate(order):
                        outs[dz][k][at, :] = state
                        if j < NX - 1:
                            state = joined_sums(
                                keeps[j], FOUR + i, state, sums_of(tables[dz][k], i)
                            )
                tail = jnp.where(late, tail1, tail0)
                for j, k in enumerate(order):
                    outs[dz][k][TAIL:, :] = tail
                    if j < NX - 1:
                        tail = joined_tail(tail, tails[j])


def cores_back_kernel(ready, *refs):
    n = (len(refs) - 2) // 4
    parts, mine, got = refs[: 2 * n], refs[2 * n : 3 * n], refs[3 * n : 4 * n]
    keep_out, send = refs[4 * n :]
    first = PLACE[0] == 0
    counts_only = iota((8, LANES), 0) < FOUR
    for d in range(n):
        for dz in range(NL):
            part, at = parts[2 * d + dz], 2 * d + dz
            core0 = jnp.where(first, mine[d][dz, TAIL:, :], got[d][dz, TAIL:, :])
            keep = keep_of(core0)
            for i in range(FOUR):
                rows = slice(i * LANES, (i + 1) * LANES)
                state = part[rows, :]
                second = joined_sums(
                    keep, FOUR + i, state,
                    jnp.where(first, mine[d][dz, rows, :], got[d][dz, rows, :]),
                )
                keep_out[at, rows, :] = jnp.where(first, state, second)
                send[at, rows, :] = jnp.where(first, second, state)
            state = part[TAIL:, :]
            second = joined_tail(state, core0)
            keep_out[at, TAIL:, :] = jnp.where(counts_only, jnp.where(first, state, second), 0.0)
            send[at, TAIL:, :] = jnp.where(counts_only, jnp.where(first, second, state), 0.0)


BACK = ((2, 0), (1,), (3,))


def lookup(home8, account8, held, came):
    for tail, at in held:
        for i in range(FOUR):
            row = jnp.broadcast_to(tail[i : i + 1, :], (8, LANES))
            found = jnp.take_along_axis(row, account8, axis=1)
            came = jnp.where(home8 == at * FOUR + i, found, came)
    return came


def held_parts(dxs, side, own_half):
    half_of = PLACE[0] if own_half else 1 - PLACE[0]
    return [
        (side, 2 * d + dz, half_of * CHUNKS + chunk_of(dz, dx))
        for d, dx in enumerate(dxs)
        for dz in range(NL)
    ]


def gather_kernel(home, account, *refs):
    n = len(BACK)
    sides, (table, counts, sems) = refs[: n + 1], refs[n + 1 :]
    held = []
    for s, side in enumerate(sides):
        held += held_parts(BACK[s % n], side, s < n)
    copies = [
        pltpu.make_async_copy(side.at[k], table.at[at], sems.at[i])
        for i, (side, k, at) in enumerate(held)
    ]
    for copy in copies:
        copy.start()
    tails = [(side[k, TAIL:, :], at) for side, k, at in held]
    for t in range(home.shape[0] // 8):
        rows = slice(8 * t, 8 * t + 8)
        counts[rows, :] = lookup(
            home[rows, :], account[rows, :], tails, jnp.zeros((8, LANES), F32)
        )
    for copy in copies:
        copy.wait()


def finish_kernel(
    user_rows, run, count, is_open, home, account, counts, table_in, got1, got2,
    table, out, picked, users, sems, out_sems,
):
    listed = pltpu.make_async_copy(user_rows, users, sems.at[4])
    listed.start()
    held = []
    for s, side in ((1, got1), (2, got2)):
        held += held_parts(BACK[s], side, False)
    copies = [
        pltpu.make_async_copy(side.at[k], table.at[at], sems.at[i])
        for i, (side, k, at) in enumerate(held)
    ]
    for copy in copies:
        copy.start()
    lines = home.shape[0]
    flat = table.reshape(NC * CHUNKS * ROWS, LANES)
    tails = [(side[k, TAIL:, :], at) for side, k, at in held]
    scale = []
    for t in range(lines // 8):
        rows = slice(8 * t, 8 * t + 8)
        came = lookup(home[rows, :], account[rows, :], tails, counts[rows, :])
        scale.append(1.0 / (count[rows, :] + is_open[rows, :] * came))
    scale = jnp.concatenate(scale, axis=0)
    if lines < LANES:
        scale = jnp.concatenate([scale, jnp.zeros((LANES - lines, LANES), F32)], axis=0)
    scale = scale.T
    for copy in (*copies, listed):
        copy.wait()

    group = 4

    def leave(g):
        rows = pl.ds(pl.multiple_of(g * group * LANES, group * LANES), group * LANES)
        return pltpu.make_async_copy(picked.at[rows, :], out.at[rows, :], out_sems.at[g])

    def lines_of(g, scale):
        for b in range(group):
            for j in range(LANES):
                at = (g * group + b) * LANES + j
                picked[pl.ds(at, 1), :] = flat[pl.ds(users[g * group + b, j], 1), :]
        for b in range(group):
            at = pl.ds(pl.multiple_of((g * group + b) * LANES, LANES), LANES)
            factor = jnp.broadcast_to(scale[:, b : b + 1], (LANES, LANES))
            picked[at, :] = (run[at, :] + picked[at, :]) * factor
        leave(g).start()
        return pltpu.roll(scale, LANES - group, 1)

    lax.fori_loop(0, lines // group, lines_of, scale)
    for g in range(lines // group):
        leave(g).wait()


def swapped(n, k):
    return [(i, i ^ k) for i in range(n)]


def body(features, home, account, flags):
    rows = features.shape[0]
    lines = rows // LANES
    home = home.reshape(lines, LANES)
    account = account.reshape(lines, LANES)
    flags = flags.reshape(lines, LANES)
    small = jax.ShapeDtypeStruct((lines, LANES), I32)
    small_f = jax.ShapeDtypeStruct((lines, LANES), F32)
    by_owner = functools.partial(jax.ShapeDtypeStruct, (OWNERS, LANES))
    by_slot = jax.ShapeDtypeStruct((OWNERS * LANES, LANES), F32)
    slot, acc_rows, flag_rows = call(
        rank_kernel,
        [small, by_owner(I32), by_owner(F32)],
        (jnp.concatenate([home, account, flags]),),
        [VMEM],
        cost=2_000_000_000,
    )
    grouped = call(
        spread_kernel,
        by_slot,
        (slot, features),
        [VMEM] * 2,
        scratch=[pltpu.SMEM((lines, LANES), I32), pltpu.SemaphoreType.DMA],
        cost=4_000_000_000,
    )
    swap = swapped(NC, 1)

    def exchange(v, dz, dx):
        if dz == 0 and dx == 0:
            return v
        return lax.ppermute(v, ("l", "x"), swapped(NL * NX, dz * NX + dx))

    order = (2, 1, 3, 0)
    mine, got = [None] * NX, [None] * NX
    tables = [[None] * NX for _ in range(NL)]

    def meet(dx):
        chunks = call(core_kernel, [block()] * NL, (mine[dx], got[dx]),
                      [VMEM, VMEM], cost=500_000_000)
        for dz in reversed(range(NL)):
            tables[dz][dx] = exchange(chunks[dz], dz, dx)
        return chunks[0]

    met = [acc_rows]
    for at, dx in enumerate(order):
        other, mine[dx] = call(
            functools.partial(closing_kernel, dx),
            [block(NL)] * 2,
            (acc_rows, flag_rows, grouped, met[at]),
            [VMEM] * 3 + [ANY],
            cost=1_500_000_000,
        )
        got[dx] = lax.ppermute(other, "c", swap)
        met.append(meet(order[at - 1]) if at else mine[dx])
    met.append(meet(order[-1]))
    run_slots, counts, opens = call(
        running_kernel,
        [by_slot, by_owner(F32), by_owner(F32)],
        (acc_rows, flag_rows, grouped, met[-1]),
        [VMEM] * 3 + [ANY],
        cost=8_000_000_000,
    )
    own, near, *pairs = call(
        row_kernel,
        [block()] * NL + [one_block()] * NH,
        (*tables[0], *tables[1], counts),
        [VMEM] * (NL * NX) + [ANY],
        scratch=[pltpu.VMEM((NH, ONE, LANES), F32)],
    )
    rows_got = list(pairs)
    for r in (1, 3, 2):
        rows_got[r] = lax.ppermute(pairs[r], "h", swapped(NH, r))
    plane = call(plane_kernel, one_block(), tuple(rows_got), [VMEM] * NH)
    ny = lax.axis_size("y")
    planes = [
        lax.ppermute(plane, "y", [(i, i + r) for i in range(ny - r)]) for r in range(1, ny)
    ]
    came = call(rows_back_kernel, [one_block()] * NH, (*planes, *rows_got),
                [VMEM] * (3 + NH))
    came = list(came)
    for r in (1, 3, 2):
        came[r] = lax.ppermute(came[r], "h", swapped(NH, r))
    parts = call(
        chips_back_kernel,
        [block()] * (NL * NX),
        (*came, own, near, *tables[0], *tables[1]),
        [VMEM] * (NH + NL + NL * NX),
        scratch=[pltpu.VMEM((NH, ONE, LANES), F32)],
    )
    parts = [list(parts[:NX]), list(parts[NX:])]
    kept = parts[0][0]
    for dx in (2, 0, 1, 3):
        for dz in reversed(range(NL)):
            parts[dz][dx] = exchange(parts[dz][dx], dz, dx)
    run, count, is_open, users = call(
        in_time_kernel,
        [jax.ShapeDtypeStruct((rows, LANES), F32), small_f, small_f, small],
        (slot, slot, home, account, run_slots, counts, opens, kept),
        [SMEM] + [VMEM] * 6 + [ANY],
        cost=10_000_000_000,
    )
    keep, last = [], []
    for dxs in BACK:
        stay, send = call(
            cores_back_kernel,
            [block(2 * len(dxs))] * 2,
            (keep[-1] if keep else count, *[parts[dz][dx] for dx in dxs for dz in range(NL)],
             *[mine[dx] for dx in dxs], *[got[dx] for dx in dxs]),
            [ANY] + [VMEM] * (4 * len(dxs)),
            cost=500_000_000,
        )
        keep.append(stay)
        last.append(lax.ppermute(send, "c", swap))
    table, came_counts = call(
        gather_kernel,
        [block(NC * CHUNKS), small_f],
        (home, account, *keep, last[0]),
        [VMEM] * 6,
        scratch=[pltpu.SemaphoreType.DMA((12,))],
        cost=2_000_000_000,
    )
    _, result = call(
        finish_kernel,
        [block(NC * CHUNKS), jax.ShapeDtypeStruct((rows, LANES), F32)],
        (users, run, count, is_open, home, account, came_counts, table, *last[1:]),
        [VMEM] * 10,
        out_specs=[VMEM, ANY],
        scratch=[pltpu.VMEM((rows, LANES), F32), pltpu.SMEM((lines, LANES), I32),
                 pltpu.SemaphoreType.DMA((5,)),
                 pltpu.SemaphoreType.DMA((8,))],
        aliases={7: 0},
    )
    return result


def solution(mesh):
    axes = ("y", "h", "l", "x", "c")
    split = Mesh(mesh.devices.reshape(-1, NH, NL, NX, NC), axes)
    return jax.shard_map(
        body,
        mesh=split,
        in_specs=(P(axes, None), P(axes, None), P(axes), P(axes)),
        out_specs=P(axes, None),
        check_vma=False,
    )
```

```python
import functools

import jax
import jax.numpy as jnp
from jax import lax
from jax.experimental import pallas as pl
from jax.experimental.pallas import tpu as pltpu
from jax.sharding import Mesh, PartitionSpec as P


LANES = 128
FOUR = 4
TAIL = FOUR * LANES
ROWS = TAIL + 8
ONE = LANES + 8
NH, NL, NX, NC = 4, 2, 4, 2
OWNERS = NH * NL * NX * NC
HALF = OWNERS // NC
CHUNKS = HALF // FOUR
BF16, F32, I32 = jnp.bfloat16, jnp.float32, jnp.int32
VMEM = pl.BlockSpec(memory_space=pltpu.VMEM)
SMEM = pl.BlockSpec(memory_space=pltpu.SMEM)
HBM = pl.BlockSpec(memory_space=pltpu.HBM)
ANY = pl.BlockSpec(memory_space=pl.ANY)


def dot(a, b):
    return lax.dot_general(a, b, (((1,), (0,)), ((), ())), preferred_element_type=F32)


def dot_nt(a, b):
    return lax.dot_general(a, b, (((1,), (1,)), ((), ())), preferred_element_type=F32)


def iota(shape, dim):
    return lax.broadcasted_iota(I32, shape, dim)


def as_bf16(mask):
    return jnp.where(mask, 1.0, 0.0).astype(BF16)


def two_parts(v):
    high = v.astype(BF16)
    low = (v - high.astype(F32)).astype(BF16)
    return jnp.concatenate([high, low], axis=1)


def masked_sum(mask, parts):
    both = dot(mask, parts)
    return both[:, :LANES] + both[:, LANES:]


def call(kernel, out, args, specs, out_specs=None, scratch=(), cost=1_000_000, limit=24, aliases=None):
    return pl.pallas_call(
        kernel,
        out_shape=out,
        in_specs=specs,
        out_specs=out_specs or jax.tree.map(lambda _: VMEM, out),
        scratch_shapes=list(scratch),
        input_output_aliases=aliases or {},
        cost_estimate=pl.CostEstimate(flops=cost, bytes_accessed=1_000_000, transcendentals=0),
        compiler_params=pltpu.CompilerParams(vmem_limit_bytes=limit << 20),
    )(*args)


class Place:
    def __getitem__(self, n):
        return lax.axis_index(("c", "x", "l", "h", "y")[n])


PLACE = Place()


def block(*lead):
    return jax.ShapeDtypeStruct((*lead, ROWS, LANES), F32)


def one_block(*lead):
    return jax.ShapeDtypeStruct((*lead, ONE, LANES), F32)


def chunk_of(dz, dx):
    return (PLACE[2] ^ dz) * NX + lax.rem(PLACE[1] + dx, NX)


def rank_kernel(events, slot_out, acc_out, flag_out):
    lines = slot_out.shape[0]
    below = as_bf16(iota((LANES, LANES), 0) < iota((LANES, LANES), 1))
    with_total = jnp.concatenate([below, jnp.ones((LANES, LANES), BF16)], axis=1)
    owner_ids = iota((OWNERS, LANES), 0)
    before = jnp.zeros((OWNERS, LANES), F32)
    codes = jnp.zeros((OWNERS, LANES), F32)
    step = 8
    for b in range(0, lines, step):
        homes = [events[b + i : b + i + 1, :] for i in range(step)]
        chosen = [owner_ids == home for home in homes]
        counted = dot(jnp.concatenate([as_bf16(c) for c in chosen], axis=0), with_total)
        coded, rank_of = [], []
        for i in range(step):
            some = counted[i * OWNERS : (i + 1) * OWNERS, :]
            rank = jnp.sum(
                jnp.where(chosen[i], some[:, :LANES] + before, 0.0), axis=0, keepdims=True
            ).astype(I32)
            before = before + some[:, LANES:]
            slot_out[b + i : b + i + 1, :] = homes[i] * LANES + rank
            account = events[lines + b + i : lines + b + i + 1, :]
            flag = events[2 * lines + b + i : 2 * lines + b + i + 1, :]
            code = (account * 2 + flag + 1).astype(F32)
            coded.append(jnp.where(chosen[i], code, 0.0).astype(BF16))
            rank_of.append(as_bf16(iota((LANES, LANES), 0) == rank))
        codes = codes + dot_nt(
            jnp.concatenate(coded, axis=1), jnp.concatenate(rank_of, axis=1)
        )
    code_ids = codes.astype(I32) - 1
    acc_out[...] = jnp.right_shift(code_ids, 1)
    flag_out[...] = jnp.where(code_ids >= 0, jnp.bitwise_and(code_ids, 1), 0).astype(F32)


def spread_kernel(slot_rows, features, grouped, slots, sem):
    copy = pltpu.make_async_copy(slot_rows, slots, sem)
    copy.start()
    zero = jnp.zeros((LANES, LANES), F32)

    def clear(o, _):
        grouped[pl.ds(pl.multiple_of(o * LANES, LANES), LANES), :] = zero
        return 0

    lax.fori_loop(0, OWNERS, clear, 0)
    copy.wait()

    for b in range(slot_rows.shape[0]):
        for j in range(LANES):
            at = b * LANES + j
            grouped[pl.ds(slots[b, j], 1), :] = features[at : at + 1, :]


def after_and_ones():
    after = as_bf16(iota((LANES, LANES), 0) > iota((LANES, LANES), 1))
    return jnp.concatenate([after, jnp.ones((LANES, LANES), BF16)], axis=1)


def cut(v, i):
    return v[i * LANES : (i + 1) * LANES, :]


def counted_rows(counted, flagged):
    count = dot(jnp.concatenate(counted, axis=0), jnp.ones((LANES, LANES), BF16))
    lane = iota((LANES, LANES), 1)
    both = jnp.zeros((LANES, LANES), F32)
    for i in range(8):
        both = jnp.where(lane == i, cut(count, i), both)
        both = jnp.where(lane == 8 + i, cut(flagged, i), both)
    return both.T


def closing_kernel(dx, acc_rows, flag_rows, grouped, ready, other, mine):
    sides = after_and_ones()
    for out, half_of in ((other, 1 - PLACE[0]), (mine, PLACE[0])):
        bases = [half_of * HALF + chunk_of(dz, dx) * FOUR for dz in range(NL)]
        acc8 = jnp.concatenate([acc_rows[pl.ds(b, FOUR), :] for b in bases], axis=0)
        flag8 = jnp.concatenate([flag_rows[pl.ds(b, FOUR), :] for b in bases], axis=0)
        member = [iota((LANES, LANES), 0) == acc8[i : i + 1, :] for i in range(8)]
        member_flags = [
            jnp.where(member[i], flag8[i : i + 1, :], 0.0).astype(BF16) for i in range(8)
        ]
        flagged = dot(jnp.concatenate(member_flags, axis=0), sides)
        counted = [as_bf16(member[i] & (cut(flagged, i)[:, :LANES] < 0.5)) for i in range(8)]
        rows = counted_rows(counted, flagged[:, LANES:])
        marks = jnp.minimum(rows[8:16, :], 1.0)
        for dz in range(NL):
            for i in range(FOUR):
                at = pl.multiple_of((bases[dz] + i) * LANES, LANES)
                values = two_parts(grouped[pl.ds(at, LANES), :])
                out[dz, i * LANES : (i + 1) * LANES, :] = masked_sum(
                    counted[dz * FOUR + i], values
                )
            own = slice(dz * FOUR, dz * FOUR + FOUR)
            out[dz, TAIL:, :] = jnp.concatenate([rows[own, :], marks[own, :]], axis=0)


def running_kernel(acc_rows, flag_rows, grouped, ready, run, counts, opens):
    sides = after_and_ones()
    up_to = iota((LANES, LANES), 1) <= iota((LANES, LANES), 0)

    def some(g, _):
        rows = pl.ds(pl.multiple_of(g * 8, 8), 8)
        acc8 = acc_rows[rows, :].astype(F32)
        flag8 = flag_rows[rows, :]
        acc_cols = acc8.T
        same = []
        for i in range(8):
            acc_col = jnp.broadcast_to(acc_cols[:, i : i + 1], (LANES, LANES))
            same.append((acc_col == acc8[i : i + 1, :]) & (acc_col >= 0.0) & up_to)
        same_flags = [
            jnp.where(same[i], flag8[i : i + 1, :], 0.0).astype(BF16) for i in range(8)
        ]
        flagged = dot(jnp.concatenate(same_flags, axis=0), sides)
        session = [as_bf16(same[i] & (cut(flagged, i)[:, :LANES] < 0.5)) for i in range(8)]
        for i in range(8):
            at = pl.ds(pl.multiple_of((g * 8 + i) * LANES, LANES), LANES)
            run[at, :] = masked_sum(session[i], two_parts(grouped[at, :]))
        found = counted_rows(session, flagged[:, LANES:])
        counts[rows, :] = found[:8, :]
        opens[rows, :] = jnp.where(found[8:16, :] < 0.5, 1.0, 0.0)
        return 0

    lax.fori_loop(0, OWNERS // 8, some, 0)


def in_time_kernel(
    slots, slot_rows, home, account, run, counts, opens, ready,
    run_out, count_out, open_out, user_out,
):
    lines = home.shape[0]

    def scalars(t, _):
        rows = pl.ds(pl.multiple_of(t * 8, 8), 8)
        home8 = home[rows, :]
        rank = slot_rows[rows, :] - home8 * LANES
        count = jnp.zeros((8, LANES), F32)
        is_open = jnp.zeros((8, LANES), F32)
        for o in range(OWNERS):
            here = home8 == o
            for_count = jnp.broadcast_to(counts[o : o + 1, :], (8, LANES))
            for_open = jnp.broadcast_to(opens[o : o + 1, :], (8, LANES))
            count = jnp.where(here, jnp.take_along_axis(for_count, rank, axis=1), count)
            is_open = jnp.where(here, jnp.take_along_axis(for_open, rank, axis=1), is_open)
        count_out[rows, :] = count
        open_out[rows, :] = is_open
        chunk = jnp.right_shift(home8, 2)
        row = (home8 - chunk * FOUR) * LANES + account[rows, :]
        user_out[rows, :] = chunk * ROWS + jnp.where(is_open > 0.5, row, TAIL + FOUR)
        return 0

    lax.fori_loop(0, lines // 8, scalars, 0)

    def collect(b, _):
        for j in range(LANES):
            run_out[pl.ds(b * LANES + j, 1), :] = run[pl.ds(slots[b, j], 1), :]
        return 0

    lax.fori_loop(0, lines, collect, 0)


def sums_of(chunk, i):
    return chunk[i * LANES : (i + 1) * LANES, :]


def keep_of(tail):
    return (1.0 - tail).T


def joined_sums(keep, i, earlier, later):
    return later + jnp.broadcast_to(keep[:, i : i + 1], (LANES, LANES)) * earlier


def joined_tail(earlier, later):
    marks = jnp.concatenate([later[FOUR:, :], later[:FOUR, :]], axis=0)
    return jnp.where(
        iota((8, LANES), 0) < FOUR, later + (1.0 - marks) * earlier, jnp.maximum(later, earlier)
    )


def joined_one(earlier, later):
    tail, first = later[LANES:, :], earlier[LANES:, :]
    mark = tail[1:2, :]
    sub = iota((8, LANES), 0)
    sums = joined_sums(keep_of(tail), 1, earlier[:LANES, :], later[:LANES, :])
    tail = jnp.where(
        sub == 0, tail + (1.0 - mark) * first, jnp.where(sub == 1, jnp.maximum(tail, first), 0.0)
    )
    return jnp.concatenate([sums, tail], axis=0)


def core_kernel(mine, got, *outs):
    first = PLACE[0] == 0
    for dz in range(NL):
        a, b = mine[dz, TAIL:, :], got[dz, TAIL:, :]
        early, late = jnp.where(first, a, b), jnp.where(first, b, a)
        keep = keep_of(late)
        for i in range(FOUR):
            at = slice(i * LANES, (i + 1) * LANES)
            a, b = mine[dz, at, :], got[dz, at, :]
            outs[dz][at, :] = joined_sums(
                keep, FOUR + i, jnp.where(first, a, b), jnp.where(first, b, a)
            )
        outs[dz][TAIL:, :] = joined_tail(early, late)


def row_kernel(*refs):
    tables = (refs[:NX], refs[NX : 2 * NX])
    totals = refs[2 * NX + 1 : 2 * NX + 3]
    outs, pair = refs[2 * NX + 3 : 2 * NX + 3 + NH], refs[-1]
    for x in range(NX):

        @pl.when(PLACE[1] == x)
        def _(x=x):
            for dz in range(NL):
                order = [tables[dz][(x - j) % NX] for j in range(NX)]
                tails = [t[TAIL:, :] for t in order]
                keep = [keep_of(t) for t in tails]
                for i in range(FOUR):
                    total = sums_of(order[0], i)
                    for j in range(1, NX):
                        total = joined_sums(keep[j], FOUR + i, total, sums_of(order[j], i))
                    totals[dz][i * LANES : (i + 1) * LANES, :] = total
                tail = tails[0]
                for j in range(1, NX):
                    tail = joined_tail(tail, tails[j])
                totals[dz][TAIL:, :] = tail

    own, near = totals
    first = PLACE[2] == 0
    a, b = own[TAIL:, :], near[TAIL:, :]
    early, late = jnp.where(first, a, b), jnp.where(first, b, a)
    keep = keep_of(late)
    tail = joined_tail(early, late)
    sub = iota((8, LANES), 0)
    for i in range(FOUR):
        a, b = sums_of(own, i), sums_of(near, i)
        pair[i, :LANES, :] = joined_sums(
            keep, FOUR + i, jnp.where(first, a, b), jnp.where(first, b, a)
        )
        pair[i, LANES:, :] = jnp.where(
            sub == 0, tail[i : i + 1, :],
            jnp.where(sub == 1, tail[FOUR + i : FOUR + i + 1, :], 0.0),
        )
    for r in range(NH):
        outs[r][...] = pair[PLACE[3] ^ r]


def plane_kernel(r0, r1, r2, r3, out):
    rows = (r0, r1, r2, r3)
    for h in range(NH):

        @pl.when(PLACE[3] == h)
        def _(h=h):
            total = rows[h][...]
            for j in range(1, NH):
                total = joined_one(total, rows[h ^ j][...])
            out[...] = total


def rows_back_kernel(p1, p2, p3, r0, r1, r2, r3, *outs):
    rows = (r0, r1, r2, r3)
    start = jnp.zeros((ONE, LANES), F32)
    for r, plane in ((2, p3), (1, p2), (0, p1)):
        start = jnp.where(PLACE[4] > r, joined_one(start, plane[...]), start)
    for h in range(NH):

        @pl.when(PLACE[3] == h)
        def _(h=h):
            state = start
            for j in range(NH):
                k = h ^ j
                outs[k][...] = state
                if j < NH - 1:
                    state = joined_one(state, rows[k][...])


def chips_back_kernel(e0, e1, e2, e3, own, near, *refs):
    tables, outs = (refs[:NX], refs[NX : 2 * NX]), (refs[2 * NX : 3 * NX], refs[3 * NX : 4 * NX])
    came = refs[-1]
    for r, e in enumerate((e0, e1, e2, e3)):
        came[PLACE[3] ^ r] = e[...]
    first = PLACE[2] == 0
    sub = iota((8, LANES), 0)
    tail0 = jnp.zeros((8, LANES), F32)
    for i in range(FOUR):
        tail0 = jnp.where(sub == i, came[i, LANES : LANES + 1, :], tail0)
    between = jnp.where(first, own[TAIL:, :], near[TAIL:, :])
    keep = keep_of(between)
    tail1 = joined_tail(tail0, between)
    for x in range(NX):

        @pl.when(PLACE[1] == x)
        def _(x=x):
            for dz in range(NL):
                order = [(x - j) % NX for j in range(NX)]
                tails = [tables[dz][k][TAIL:, :] for k in order[:-1]]
                keeps = [keep_of(t) for t in tails]
                late = first if dz else jnp.logical_not(first)
                for i in range(FOUR):
                    at = slice(i * LANES, (i + 1) * LANES)
                    state = came[i, :LANES, :]
                    second = joined_sums(
                        keep, FOUR + i, state, jnp.where(first, own[at, :], near[at, :])
                    )
                    state = jnp.where(late, second, state)
                    for j, k in enumerate(order):
                        outs[dz][k][at, :] = state
                        if j < NX - 1:
                            state = joined_sums(
                                keeps[j], FOUR + i, state, sums_of(tables[dz][k], i)
                            )
                tail = jnp.where(late, tail1, tail0)
                for j, k in enumerate(order):
                    outs[dz][k][TAIL:, :] = tail
                    if j < NX - 1:
                        tail = joined_tail(tail, tails[j])


def cores_back_kernel(ready, *refs):
    n = (len(refs) - 2) // 4
    parts, mine, got = refs[: 2 * n], refs[2 * n : 3 * n], refs[3 * n : 4 * n]
    keep_out, send = refs[4 * n :]
    first = PLACE[0] == 0
    counts_only = iota((8, LANES), 0) < FOUR
    for d in range(n):
        for dz in range(NL):
            part, at = parts[2 * d + dz], 2 * d + dz
            core0 = jnp.where(first, mine[d][dz, TAIL:, :], got[d][dz, TAIL:, :])
            keep = keep_of(core0)
            for i in range(FOUR):
                rows = slice(i * LANES, (i + 1) * LANES)
                state = part[rows, :]
                second = joined_sums(
                    keep, FOUR + i, state,
                    jnp.where(first, mine[d][dz, rows, :], got[d][dz, rows, :]),
                )
                keep_out[at, rows, :] = jnp.where(first, state, second)
                send[at, rows, :] = jnp.where(first, second, state)
            state = part[TAIL:, :]
            second = joined_tail(state, core0)
            keep_out[at, TAIL:, :] = jnp.where(counts_only, jnp.where(first, state, second), 0.0)
            send[at, TAIL:, :] = jnp.where(counts_only, jnp.where(first, second, state), 0.0)


BACK = ((2, 0), (1,), (3,))


def lookup(home8, account8, held, came):
    for tail, at in held:
        for i in range(FOUR):
            row = jnp.broadcast_to(tail[i : i + 1, :], (8, LANES))
            found = jnp.take_along_axis(row, account8, axis=1)
            came = jnp.where(home8 == at * FOUR + i, found, came)
    return came


def held_parts(dxs, side, own_half):
    half_of = PLACE[0] if own_half else 1 - PLACE[0]
    return [
        (side, 2 * d + dz, half_of * CHUNKS + chunk_of(dz, dx))
        for d, dx in enumerate(dxs)
        for dz in range(NL)
    ]


def gather_kernel(home, account, *refs):
    n = len(BACK)
    sides, (table, counts, sems) = refs[: n + 1], refs[n + 1 :]
    held = []
    for s, side in enumerate(sides):
        held += held_parts(BACK[s % n], side, s < n)
    copies = [
        pltpu.make_async_copy(side.at[k], table.at[at], sems.at[i])
        for i, (side, k, at) in enumerate(held)
    ]
    for copy in copies:
        copy.start()
    tails = [(side[k, TAIL:, :], at) for side, k, at in held]
    for t in range(home.shape[0] // 8):
        rows = slice(8 * t, 8 * t + 8)
        counts[rows, :] = lookup(
            home[rows, :], account[rows, :], tails, jnp.zeros((8, LANES), F32)
        )
    for copy in copies:
        copy.wait()


def finish_kernel(
    user_rows, run, count, is_open, home, account, counts, table_in, got1, got2,
    table, out, picked, users, sems, out_sems,
):
    listed = pltpu.make_async_copy(user_rows, users, sems.at[4])
    listed.start()
    held = []
    for s, side in ((1, got1), (2, got2)):
        held += held_parts(BACK[s], side, False)
    copies = [
        pltpu.make_async_copy(side.at[k], table.at[at], sems.at[i])
        for i, (side, k, at) in enumerate(held)
    ]
    for copy in copies:
        copy.start()
    lines = home.shape[0]
    flat = table.reshape(NC * CHUNKS * ROWS, LANES)
    tails = [(side[k, TAIL:, :], at) for side, k, at in held]
    scale = []
    for t in range(lines // 8):
        rows = slice(8 * t, 8 * t + 8)
        came = lookup(home[rows, :], account[rows, :], tails, counts[rows, :])
        scale.append(1.0 / (count[rows, :] + is_open[rows, :] * came))
    scale = jnp.concatenate(scale, axis=0)
    if lines < LANES:
        scale = jnp.concatenate([scale, jnp.zeros((LANES - lines, LANES), F32)], axis=0)
    scale = scale.T
    for copy in (*copies, listed):
        copy.wait()

    group = 4

    def leave(g):
        rows = pl.ds(pl.multiple_of(g * group * LANES, group * LANES), group * LANES)
        return pltpu.make_async_copy(picked.at[rows, :], out.at[rows, :], out_sems.at[g])

    def lines_of(g, scale):
        for b in range(group):
            for j in range(LANES):
                at = (g * group + b) * LANES + j
                picked[pl.ds(at, 1), :] = flat[pl.ds(users[g * group + b, j], 1), :]
        for b in range(group):
            at = pl.ds(pl.multiple_of((g * group + b) * LANES, LANES), LANES)
            factor = jnp.broadcast_to(scale[:, b : b + 1], (LANES, LANES))
            picked[at, :] = (run[at, :] + picked[at, :]) * factor
        leave(g).start()
        return pltpu.roll(scale, LANES - group, 1)

    lax.fori_loop(0, lines // group, lines_of, scale)
    for g in range(lines // group):
        leave(g).wait()


def swapped(n, k):
    return [(i, i ^ k) for i in range(n)]


def body(features, home, account, flags):
    rows = features.shape[0]
    lines = rows // LANES
    home = home.reshape(lines, LANES)
    account = account.reshape(lines, LANES)
    flags = flags.reshape(lines, LANES)
    small = jax.ShapeDtypeStruct((lines, LANES), I32)
    small_f = jax.ShapeDtypeStruct((lines, LANES), F32)
    by_owner = functools.partial(jax.ShapeDtypeStruct, (OWNERS, LANES))
    by_slot = jax.ShapeDtypeStruct((OWNERS * LANES, LANES), F32)
    slot, acc_rows, flag_rows = call(
        rank_kernel,
        [small, by_owner(I32), by_owner(F32)],
        (jnp.concatenate([home, account, flags]),),
        [VMEM],
        cost=2_000_000_000,
    )
    grouped = call(
        spread_kernel,
        by_slot,
        (slot, features),
        [VMEM] * 2,
        scratch=[pltpu.SMEM((lines, LANES), I32), pltpu.SemaphoreType.DMA],
        cost=4_000_000_000,
    )
    swap = swapped(NC, 1)

    def exchange(v, dz, dx):
        if dz == 0 and dx == 0:
            return v
        pairs = [
            (row * NX + x, (row ^ dz) * NX + (x + dx) % NX) for row in range(NL) for x in range(NX)
        ]
        return lax.ppermute(v, ("l", "x"), pairs)

    order = (2, 1, 3, 0)
    mine, got = [None] * NX, [None] * NX
    tables = [[None] * NX for _ in range(NL)]

    def meet(dx):
        chunks = call(core_kernel, [block()] * NL, (mine[dx], got[dx]),
                      [VMEM, VMEM], cost=500_000_000)
        for dz in reversed(range(NL)):
            tables[dz][dx] = exchange(chunks[dz], dz, dx)
        return chunks[0]

    met = [acc_rows]
    for at, dx in enumerate(order):
        other, mine[dx] = call(
            functools.partial(closing_kernel, dx),
            [block(NL)] * 2,
            (acc_rows, flag_rows, grouped, met[at]),
            [VMEM] * 3 + [ANY],
            cost=1_500_000_000,
        )
        got[dx] = lax.ppermute(other, "c", swap)
        met.append(meet(order[at - 1]) if at else mine[dx])
    met.append(meet(order[-1]))
    run_slots, counts, opens = call(
        running_kernel,
        [by_slot, by_owner(F32), by_owner(F32)],
        (acc_rows, flag_rows, grouped, met[-1]),
        [VMEM] * 3 + [ANY],
        cost=8_000_000_000,
    )
    own, near, *pairs = call(
        row_kernel,
        [block()] * NL + [one_block()] * NH,
        (*tables[0], *tables[1], counts),
        [VMEM] * (NL * NX) + [ANY],
        scratch=[pltpu.VMEM((NH, ONE, LANES), F32)],
    )
    rows_got = list(pairs)
    for r in (1, 3, 2):
        rows_got[r] = lax.ppermute(pairs[r], "h", swapped(NH, r))
    plane = call(plane_kernel, one_block(), tuple(rows_got), [VMEM] * NH)
    ny = lax.axis_size("y")
    planes = [
        lax.ppermute(plane, "y", [(i, i + r) for i in range(ny - r)]) for r in range(1, ny)
    ]
    came = call(rows_back_kernel, [one_block()] * NH, (*planes, *rows_got),
                [VMEM] * (3 + NH))
    came = list(came)
    for r in (1, 3, 2):
        came[r] = lax.ppermute(came[r], "h", swapped(NH, r))
    parts = call(
        chips_back_kernel,
        [block()] * (NL * NX),
        (*came, own, near, *tables[0], *tables[1]),
        [VMEM] * (NH + NL + NL * NX),
        scratch=[pltpu.VMEM((NH, ONE, LANES), F32)],
    )
    parts = [list(parts[:NX]), list(parts[NX:])]
    kept = parts[0][0]
    for dx in (2, 0, 1, 3):
        for dz in reversed(range(NL)):
            parts[dz][dx] = exchange(parts[dz][dx], dz, (NX - dx) % NX)
    run, count, is_open, users = call(
        in_time_kernel,
        [jax.ShapeDtypeStruct((rows, LANES), F32), small_f, small_f, small],
        (slot, slot, home, account, run_slots, counts, opens, kept),
        [SMEM] + [VMEM] * 6 + [ANY],
        cost=10_000_000_000,
    )
    keep, last = [], []
    for dxs in BACK:
        stay, send = call(
            cores_back_kernel,
            [block(2 * len(dxs))] * 2,
            (keep[-1] if keep else count, *[parts[dz][dx] for dx in dxs for dz in range(NL)],
             *[mine[dx] for dx in dxs], *[got[dx] for dx in dxs]),
            [ANY] + [VMEM] * (4 * len(dxs)),
            cost=500_000_000,
        )
        keep.append(stay)
        last.append(lax.ppermute(send, "c", swap))
    table, came_counts = call(
        gather_kernel,
        [block(NC * CHUNKS), small_f],
        (home, account, *keep, last[0]),
        [VMEM] * 6,
        scratch=[pltpu.SemaphoreType.DMA((12,))],
        cost=2_000_000_000,
    )
    _, result = call(
        finish_kernel,
        [block(NC * CHUNKS), jax.ShapeDtypeStruct((rows, LANES), F32)],
        (users, run, count, is_open, home, account, came_counts, table, *last[1:]),
        [VMEM] * 10,
        out_specs=[VMEM, ANY],
        scratch=[pltpu.VMEM((rows, LANES), F32), pltpu.SMEM((lines, LANES), I32),
                 pltpu.SemaphoreType.DMA((5,)),
                 pltpu.SemaphoreType.DMA((8,))],
        aliases={7: 0},
    )
    return result


def solution(mesh):
    axes = ("y", "h", "l", "x", "c")
    split = Mesh(mesh.devices.reshape(-1, NH, NL, NX, NC), axes)
    return jax.shard_map(
        body,
        mesh=split,
        in_specs=(P(axes, None), P(axes, None), P(axes), P(axes)),
        out_specs=P(axes, None),
        check_vma=False,
    )
```

```python
import functools

import jax
import jax.numpy as jnp
from jax import lax
from jax.experimental import pallas as pl
from jax.experimental.pallas import tpu as pltpu
from jax.sharding import Mesh, PartitionSpec as P


LANES = 128
FOUR = 4
TAIL = FOUR * LANES
ROWS = TAIL + 8
ONE = LANES + 8
NH, NL, NX, NC = 4, 2, 4, 2
OWNERS = NH * NL * NX * NC
HALF = OWNERS // NC
CHUNKS = HALF // FOUR
BF16, F32, I32 = jnp.bfloat16, jnp.float32, jnp.int32
VMEM = pl.BlockSpec(memory_space=pltpu.VMEM)
SMEM = pl.BlockSpec(memory_space=pltpu.SMEM)
HBM = pl.BlockSpec(memory_space=pltpu.HBM)
ANY = pl.BlockSpec(memory_space=pl.ANY)


def dot(a, b):
    return lax.dot_general(a, b, (((1,), (0,)), ((), ())), preferred_element_type=F32)


def dot_nt(a, b):
    return lax.dot_general(a, b, (((1,), (1,)), ((), ())), preferred_element_type=F32)


def iota(shape, dim):
    return lax.broadcasted_iota(I32, shape, dim)


def as_bf16(mask):
    return jnp.where(mask, 1.0, 0.0).astype(BF16)


def two_parts(v):
    high = v.astype(BF16)
    low = (v - high.astype(F32)).astype(BF16)
    return jnp.concatenate([high, low], axis=1)


def masked_sum(mask, parts):
    both = dot(mask, parts)
    return both[:, :LANES] + both[:, LANES:]


def call(kernel, out, args, specs, out_specs=None, scratch=(), cost=1_000_000, limit=24, aliases=None):
    return pl.pallas_call(
        kernel,
        out_shape=out,
        in_specs=specs,
        out_specs=out_specs or jax.tree.map(lambda _: VMEM, out),
        scratch_shapes=list(scratch),
        input_output_aliases=aliases or {},
        cost_estimate=pl.CostEstimate(flops=cost, bytes_accessed=1_000_000, transcendentals=0),
        compiler_params=pltpu.CompilerParams(vmem_limit_bytes=limit << 20),
    )(*args)


class Place:
    def __getitem__(self, n):
        return lax.axis_index(("c", "x", "l", "h", "y")[n])


PLACE = Place()


def block(*lead):
    return jax.ShapeDtypeStruct((*lead, ROWS, LANES), F32)


def one_block(*lead):
    return jax.ShapeDtypeStruct((*lead, ONE, LANES), F32)


def chunk_of(dz, dx):
    return (PLACE[2] ^ dz) * NX + lax.rem(PLACE[1] + dx, NX)


def rank_kernel(events, slot_out, acc_out, flag_out):
    lines = slot_out.shape[0]
    below = as_bf16(iota((LANES, LANES), 0) < iota((LANES, LANES), 1))
    with_total = jnp.concatenate([below, jnp.ones((LANES, LANES), BF16)], axis=1)
    owner_ids = iota((OWNERS, LANES), 0)
    before = jnp.zeros((OWNERS, LANES), F32)
    codes = jnp.zeros((OWNERS, LANES), F32)
    step = 8
    for b in range(0, lines, step):
        homes = [events[b + i : b + i + 1, :] for i in range(step)]
        chosen = [owner_ids == home for home in homes]
        counted = dot(jnp.concatenate([as_bf16(c) for c in chosen], axis=0), with_total)
        coded, rank_of = [], []
        for i in range(step):
            some = counted[i * OWNERS : (i + 1) * OWNERS, :]
            rank = jnp.sum(
                jnp.where(chosen[i], some[:, :LANES] + before, 0.0), axis=0, keepdims=True
            ).astype(I32)
            before = before + some[:, LANES:]
            slot_out[b + i : b + i + 1, :] = homes[i] * LANES + rank
            account = events[lines + b + i : lines + b + i + 1, :]
            flag = events[2 * lines + b + i : 2 * lines + b + i + 1, :]
            code = (account * 2 + flag + 1).astype(F32)
            coded.append(jnp.where(chosen[i], code, 0.0).astype(BF16))
            rank_of.append(as_bf16(iota((LANES, LANES), 0) == rank))
        codes = codes + dot_nt(
            jnp.concatenate(coded, axis=1), jnp.concatenate(rank_of, axis=1)
        )
    code_ids = codes.astype(I32) - 1
    acc_out[...] = jnp.right_shift(code_ids, 1)
    flag_out[...] = jnp.where(code_ids >= 0, jnp.bitwise_and(code_ids, 1), 0).astype(F32)


def spread_kernel(slot_rows, features, grouped, slots, sem):
    copy = pltpu.make_async_copy(slot_rows, slots, sem)
    copy.start()
    zero = jnp.zeros((LANES, LANES), F32)

    def clear(o, _):
        grouped[pl.ds(pl.multiple_of(o * LANES, LANES), LANES), :] = zero
        return 0

    lax.fori_loop(0, OWNERS, clear, 0)
    copy.wait()

    for b in range(slot_rows.shape[0]):
        for j in range(LANES):
            at = b * LANES + j
            grouped[pl.ds(slots[b, j], 1), :] = features[at : at + 1, :]


def after_and_ones():
    after = as_bf16(iota((LANES, LANES), 0) > iota((LANES, LANES), 1))
    return jnp.concatenate([after, jnp.ones((LANES, LANES), BF16)], axis=1)


def cut(v, i):
    return v[i * LANES : (i + 1) * LANES, :]


def counted_rows(counted, flagged):
    count = dot(jnp.concatenate(counted, axis=0), jnp.ones((LANES, LANES), BF16))
    lane = iota((LANES, LANES), 1)
    both = jnp.zeros((LANES, LANES), F32)
    for i in range(8):
        both = jnp.where(lane == i, cut(count, i), both)
        both = jnp.where(lane == 8 + i, cut(flagged, i), both)
    return both.T


def closing_kernel(dx, acc_rows, flag_rows, grouped, ready, other, mine):
    sides = after_and_ones()
    for out, half_of in ((other, 1 - PLACE[0]), (mine, PLACE[0])):
        bases = [half_of * HALF + chunk_of(dz, dx) * FOUR for dz in range(NL)]
        acc8 = jnp.concatenate([acc_rows[pl.ds(b, FOUR), :] for b in bases], axis=0)
        flag8 = jnp.concatenate([flag_rows[pl.ds(b, FOUR), :] for b in bases], axis=0)
        member = [iota((LANES, LANES), 0) == acc8[i : i + 1, :] for i in range(8)]
        member_flags = [
            jnp.where(member[i], flag8[i : i + 1, :], 0.0).astype(BF16) for i in range(8)
        ]
        flagged = dot(jnp.concatenate(member_flags, axis=0), sides)
        counted = [as_bf16(member[i] & (cut(flagged, i)[:, :LANES] < 0.5)) for i in range(8)]
        rows = counted_rows(counted, flagged[:, LANES:])
        marks = jnp.minimum(rows[8:16, :], 1.0)
        for dz in range(NL):
            for i in range(FOUR):
                at = pl.multiple_of((bases[dz] + i) * LANES, LANES)
                values = two_parts(grouped[pl.ds(at, LANES), :])
                out[dz, i * LANES : (i + 1) * LANES, :] = masked_sum(
                    counted[dz * FOUR + i], values
                )
            own = slice(dz * FOUR, dz * FOUR + FOUR)
            out[dz, TAIL:, :] = jnp.concatenate([rows[own, :], marks[own, :]], axis=0)


def running_kernel(acc_rows, flag_rows, grouped, ready, run, counts, opens):
    sides = after_and_ones()
    up_to = iota((LANES, LANES), 1) <= iota((LANES, LANES), 0)

    def some(g, _):
        rows = pl.ds(pl.multiple_of(g * 8, 8), 8)
        acc8 = acc_rows[rows, :].astype(F32)
        flag8 = flag_rows[rows, :]
        acc_cols = acc8.T
        same = []
        for i in range(8):
            acc_col = jnp.broadcast_to(acc_cols[:, i : i + 1], (LANES, LANES))
            same.append((acc_col == acc8[i : i + 1, :]) & (acc_col >= 0.0) & up_to)
        same_flags = [
            jnp.where(same[i], flag8[i : i + 1, :], 0.0).astype(BF16) for i in range(8)
        ]
        flagged = dot(jnp.concatenate(same_flags, axis=0), sides)
        session = [as_bf16(same[i] & (cut(flagged, i)[:, :LANES] < 0.5)) for i in range(8)]
        for i in range(8):
            at = pl.ds(pl.multiple_of((g * 8 + i) * LANES, LANES), LANES)
            run[at, :] = masked_sum(session[i], two_parts(grouped[at, :]))
        found = counted_rows(session, flagged[:, LANES:])
        counts[rows, :] = found[:8, :]
        opens[rows, :] = jnp.where(found[8:16, :] < 0.5, 1.0, 0.0)
        return 0

    lax.fori_loop(0, OWNERS // 8, some, 0)


def in_time_kernel(
    slots, slot_rows, home, account, run, counts, opens, ready,
    run_out, count_out, open_out, user_out,
):
    lines = home.shape[0]

    def scalars(t, _):
        rows = pl.ds(pl.multiple_of(t * 8, 8), 8)
        home8 = home[rows, :]
        rank = slot_rows[rows, :] - home8 * LANES
        count = jnp.zeros((8, LANES), F32)
        is_open = jnp.zeros((8, LANES), F32)
        for o in range(OWNERS):
            here = home8 == o
            for_count = jnp.broadcast_to(counts[o : o + 1, :], (8, LANES))
            for_open = jnp.broadcast_to(opens[o : o + 1, :], (8, LANES))
            count = jnp.where(here, jnp.take_along_axis(for_count, rank, axis=1), count)
            is_open = jnp.where(here, jnp.take_along_axis(for_open, rank, axis=1), is_open)
        count_out[rows, :] = count
        open_out[rows, :] = is_open
        chunk = jnp.right_shift(home8, 2)
        row = (home8 - chunk * FOUR) * LANES + account[rows, :]
        user = chunk * ROWS + jnp.where(is_open > 0.5, row, TAIL + FOUR)
        for half in range(2):
            at = pl.ds(pl.multiple_of(t * 16 + half * 8, 8), 4)
            user_out[at, :] = user[half * 4 : half * 4 + 4, :]
        return 0

    lax.fori_loop(0, lines // 8, scalars, 0)

    def collect(b, _):
        for j in range(LANES):
            run_out[pl.ds(b * LANES + j, 1), :] = run[pl.ds(slots[b, j], 1), :]
        return 0

    lax.fori_loop(0, lines, collect, 0)


def sums_of(chunk, i):
    return chunk[i * LANES : (i + 1) * LANES, :]


def keep_of(tail):
    return (1.0 - tail).T


def joined_sums(keep, i, earlier, later):
    return later + jnp.broadcast_to(keep[:, i : i + 1], (LANES, LANES)) * earlier


def joined_tail(earlier, later):
    marks = jnp.concatenate([later[FOUR:, :], later[:FOUR, :]], axis=0)
    return jnp.where(
        iota((8, LANES), 0) < FOUR, later + (1.0 - marks) * earlier, jnp.maximum(later, earlier)
    )


def joined_one(earlier, later):
    tail, first = later[LANES:, :], earlier[LANES:, :]
    mark = tail[1:2, :]
    sub = iota((8, LANES), 0)
    sums = joined_sums(keep_of(tail), 1, earlier[:LANES, :], later[:LANES, :])
    tail = jnp.where(
        sub == 0, tail + (1.0 - mark) * first, jnp.where(sub == 1, jnp.maximum(tail, first), 0.0)
    )
    return jnp.concatenate([sums, tail], axis=0)


def core_kernel(mine, got, *outs):
    first = PLACE[0] == 0
    for dz in range(NL):
        a, b = mine[dz, TAIL:, :], got[dz, TAIL:, :]
        early, late = jnp.where(first, a, b), jnp.where(first, b, a)
        keep = keep_of(late)
        for i in range(FOUR):
            at = slice(i * LANES, (i + 1) * LANES)
            a, b = mine[dz, at, :], got[dz, at, :]
            outs[dz][at, :] = joined_sums(
                keep, FOUR + i, jnp.where(first, a, b), jnp.where(first, b, a)
            )
        outs[dz][TAIL:, :] = joined_tail(early, late)


def row_kernel(*refs):
    tables = (refs[:NX], refs[NX : 2 * NX])
    totals = refs[2 * NX + 1 : 2 * NX + 3]
    outs, pair = refs[2 * NX + 3 : 2 * NX + 3 + NH], refs[-1]
    for x in range(NX):

        @pl.when(PLACE[1] == x)
        def _(x=x):
            for dz in range(NL):
                order = [tables[dz][(x - j) % NX] for j in range(NX)]
                tails = [t[TAIL:, :] for t in order]
                keep = [keep_of(t) for t in tails]
                for i in range(FOUR):
                    total = sums_of(order[0], i)
                    for j in range(1, NX):
                        total = joined_sums(keep[j], FOUR + i, total, sums_of(order[j], i))
                    totals[dz][i * LANES : (i + 1) * LANES, :] = total
                tail = tails[0]
                for j in range(1, NX):
                    tail = joined_tail(tail, tails[j])
                totals[dz][TAIL:, :] = tail

    own, near = totals
    first = PLACE[2] == 0
    a, b = own[TAIL:, :], near[TAIL:, :]
    early, late = jnp.where(first, a, b), jnp.where(first, b, a)
    keep = keep_of(late)
    tail = joined_tail(early, late)
    sub = iota((8, LANES), 0)
    for i in range(FOUR):
        a, b = sums_of(own, i), sums_of(near, i)
        pair[i, :LANES, :] = joined_sums(
            keep, FOUR + i, jnp.where(first, a, b), jnp.where(first, b, a)
        )
        pair[i, LANES:, :] = jnp.where(
            sub == 0, tail[i : i + 1, :],
            jnp.where(sub == 1, tail[FOUR + i : FOUR + i + 1, :], 0.0),
        )
    for r in range(NH):
        outs[r][...] = pair[PLACE[3] ^ r]


def plane_kernel(r0, r1, r2, r3, out):
    rows = (r0, r1, r2, r3)
    for h in range(NH):

        @pl.when(PLACE[3] == h)
        def _(h=h):
            total = rows[h][...]
            for j in range(1, NH):
                total = joined_one(total, rows[h ^ j][...])
            out[...] = total


def rows_back_kernel(p1, p2, p3, r0, r1, r2, r3, *outs):
    rows = (r0, r1, r2, r3)
    start = jnp.zeros((ONE, LANES), F32)
    for r, plane in ((2, p3), (1, p2), (0, p1)):
        start = jnp.where(PLACE[4] > r, joined_one(start, plane[...]), start)
    for h in range(NH):

        @pl.when(PLACE[3] == h)
        def _(h=h):
            state = start
            for j in range(NH):
                k = h ^ j
                outs[k][...] = state
                if j < NH - 1:
                    state = joined_one(state, rows[k][...])


def chips_back_kernel(e0, e1, e2, e3, own, near, *refs):
    tables, outs = (refs[:NX], refs[NX : 2 * NX]), (refs[2 * NX : 3 * NX], refs[3 * NX : 4 * NX])
    came = refs[-1]
    for r, e in enumerate((e0, e1, e2, e3)):
        came[PLACE[3] ^ r] = e[...]
    first = PLACE[2] == 0
    sub = iota((8, LANES), 0)
    tail0 = jnp.zeros((8, LANES), F32)
    for i in range(FOUR):
        tail0 = jnp.where(sub == i, came[i, LANES : LANES + 1, :], tail0)
    between = jnp.where(first, own[TAIL:, :], near[TAIL:, :])
    keep = keep_of(between)
    tail1 = joined_tail(tail0, between)
    for x in range(NX):

        @pl.when(PLACE[1] == x)
        def _(x=x):
            for dz in range(NL):
                order = [(x - j) % NX for j in range(NX)]
                tails = [tables[dz][k][TAIL:, :] for k in order[:-1]]
                keeps = [keep_of(t) for t in tails]
                late = first if dz else jnp.logical_not(first)
                for i in range(FOUR):
                    at = slice(i * LANES, (i + 1) * LANES)
                    state = came[i, :LANES, :]
                    second = joined_sums(
                        keep, FOUR + i, state, jnp.where(first, own[at, :], near[at, :])
                    )
                    state = jnp.where(late, second, state)
                    for j, k in enumerate(order):
                        outs[dz][k][at, :] = state
                        if j < NX - 1:
                            state = joined_sums(
                                keeps[j], FOUR + i, state, sums_of(tables[dz][k], i)
                            )
                tail = jnp.where(late, tail1, tail0)
                for j, k in enumerate(order):
                    outs[dz][k][TAIL:, :] = tail
                    if j < NX - 1:
                        tail = joined_tail(tail, tails[j])


def cores_back_kernel(ready, *refs):
    n = (len(refs) - 2) // 4
    parts, mine, got = refs[: 2 * n], refs[2 * n : 3 * n], refs[3 * n : 4 * n]
    keep_out, send = refs[4 * n :]
    first = PLACE[0] == 0
    counts_only = iota((8, LANES), 0) < FOUR
    for d in range(n):
        for dz in range(NL):
            part, at = parts[2 * d + dz], 2 * d + dz
            core0 = jnp.where(first, mine[d][dz, TAIL:, :], got[d][dz, TAIL:, :])
            keep = keep_of(core0)
            for i in range(FOUR):
                rows = slice(i * LANES, (i + 1) * LANES)
                state = part[rows, :]
                second = joined_sums(
                    keep, FOUR + i, state,
                    jnp.where(first, mine[d][dz, rows, :], got[d][dz, rows, :]),
                )
                keep_out[at, rows, :] = jnp.where(first, state, second)
                send[at, rows, :] = jnp.where(first, second, state)
            state = part[TAIL:, :]
            second = joined_tail(state, core0)
            keep_out[at, TAIL:, :] = jnp.where(counts_only, jnp.where(first, state, second), 0.0)
            send[at, TAIL:, :] = jnp.where(counts_only, jnp.where(first, second, state), 0.0)


BACK = ((2, 0), (1,), (3,))


def lookup(home8, account8, held, came):
    for tail, at in held:
        for i in range(FOUR):
            row = jnp.broadcast_to(tail[i : i + 1, :], (8, LANES))
            found = jnp.take_along_axis(row, account8, axis=1)
            came = jnp.where(home8 == at * FOUR + i, found, came)
    return came


def held_parts(dxs, side, own_half):
    half_of = PLACE[0] if own_half else 1 - PLACE[0]
    return [
        (side, 2 * d + dz, half_of * CHUNKS + chunk_of(dz, dx))
        for d, dx in enumerate(dxs)
        for dz in range(NL)
    ]


def gather_kernel(home, account, *refs):
    n = len(BACK)
    sides, (table, counts, sems) = refs[: n + 1], refs[n + 1 :]
    held = []
    for s, side in enumerate(sides):
        held += held_parts(BACK[s % n], side, s < n)
    copies = [
        pltpu.make_async_copy(side.at[k], table.at[at], sems.at[i])
        for i, (side, k, at) in enumerate(held)
    ]
    for copy in copies:
        copy.start()
    tails = [(side[k, TAIL:, :], at) for side, k, at in held]
    for t in range(home.shape[0] // 8):
        rows = slice(8 * t, 8 * t + 8)
        counts[rows, :] = lookup(
            home[rows, :], account[rows, :], tails, jnp.zeros((8, LANES), F32)
        )
    for copy in copies:
        copy.wait()


def finish_kernel(
    user_rows, run, count, is_open, home, account, counts, table_in, got1, got2,
    table, out, picked, u0, u1, u2, u3, sems, out_sems, list_sems,
):
    users = (u0, u1, u2, u3)

    def listed(g, q):
        return pltpu.make_async_copy(
            user_rows.at[pl.ds(pl.multiple_of(g * 8, 8), 4), :], users[q], list_sems.at[q]
        )

    for q in range(4):
        listed(q, q).start()
    held = []
    for s, side in ((1, got1), (2, got2)):
        held += held_parts(BACK[s], side, False)
    copies = [
        pltpu.make_async_copy(side.at[k], table.at[at], sems.at[i])
        for i, (side, k, at) in enumerate(held)
    ]
    for copy in copies:
        copy.start()
    lines = home.shape[0]
    flat = table.reshape(NC * CHUNKS * ROWS, LANES)
    tails = [(side[k, TAIL:, :], at) for side, k, at in held]
    scale = []
    for t in range(lines // 8):
        rows = slice(8 * t, 8 * t + 8)
        came = lookup(home[rows, :], account[rows, :], tails, counts[rows, :])
        scale.append(1.0 / (count[rows, :] + is_open[rows, :] * came))
    scale = jnp.concatenate(scale, axis=0)
    if lines < LANES:
        scale = jnp.concatenate([scale, jnp.zeros((LANES - lines, LANES), F32)], axis=0)
    scale = scale.T
    for copy in copies:
        copy.wait()

    group = 4

    def leave(g):
        rows = pl.ds(pl.multiple_of(g * group * LANES, group * LANES), group * LANES)
        return pltpu.make_async_copy(picked.at[rows, :], out.at[rows, :], out_sems.at[g])

    def some(turn, scale):
        for q in range(4):
            g = turn * 4 + q
            listed(g, q).wait()
            for b in range(group):
                for j in range(LANES):
                    at = (g * group + b) * LANES + j
                    picked[pl.ds(at, 1), :] = flat[pl.ds(users[q][b, j], 1), :]
            pl.when(g + 4 < lines // group)(lambda g=g, q=q: listed(g + 4, q).start())
            for b in range(group):
                at = pl.ds(pl.multiple_of((g * group + b) * LANES, LANES), LANES)
                factor = jnp.broadcast_to(scale[:, b : b + 1], (LANES, LANES))
                picked[at, :] = (run[at, :] + picked[at, :]) * factor
            leave(g).start()
            scale = pltpu.roll(scale, LANES - group, 1)
        return scale

    lax.fori_loop(0, lines // (4 * group), some, scale)
    for g in range(lines // group):
        leave(g).wait()


def swapped(n, k):
    return [(i, i ^ k) for i in range(n)]


def body(features, home, account, flags):
    rows = features.shape[0]
    lines = rows // LANES
    home = home.reshape(lines, LANES)
    account = account.reshape(lines, LANES)
    flags = flags.reshape(lines, LANES)
    small = jax.ShapeDtypeStruct((lines, LANES), I32)
    small_f = jax.ShapeDtypeStruct((lines, LANES), F32)
    by_owner = functools.partial(jax.ShapeDtypeStruct, (OWNERS, LANES))
    by_slot = jax.ShapeDtypeStruct((OWNERS * LANES, LANES), F32)
    slot, acc_rows, flag_rows = call(
        rank_kernel,
        [small, by_owner(I32), by_owner(F32)],
        (jnp.concatenate([home, account, flags]),),
        [VMEM],
        cost=2_000_000_000,
    )
    grouped = call(
        spread_kernel,
        by_slot,
        (slot, features),
        [VMEM] * 2,
        scratch=[pltpu.SMEM((lines, LANES), I32), pltpu.SemaphoreType.DMA],
        cost=4_000_000_000,
    )
    swap = swapped(NC, 1)

    def exchange(v, dz, dx):
        if dz == 0 and dx == 0:
            return v
        pairs = [
            (row * NX + x, (row ^ dz) * NX + (x + dx) % NX) for row in range(NL) for x in range(NX)
        ]
        return lax.ppermute(v, ("l", "x"), pairs)

    order = (2, 1, 3, 0)
    mine, got = [None] * NX, [None] * NX
    tables = [[None] * NX for _ in range(NL)]

    def meet(dx):
        chunks = call(core_kernel, [block()] * NL, (mine[dx], got[dx]),
                      [VMEM, VMEM], cost=500_000_000)
        for dz in reversed(range(NL)):
            tables[dz][dx] = exchange(chunks[dz], dz, dx)
        return chunks[0]

    met = [acc_rows]
    for at, dx in enumerate(order):
        other, mine[dx] = call(
            functools.partial(closing_kernel, dx),
            [block(NL)] * 2,
            (acc_rows, flag_rows, grouped, met[at]),
            [VMEM] * 3 + [ANY],
            cost=1_500_000_000,
        )
        got[dx] = lax.ppermute(other, "c", swap)
        met.append(meet(order[at - 1]) if at else mine[dx])
    met.append(meet(order[-1]))
    run_slots, counts, opens = call(
        running_kernel,
        [by_slot, by_owner(F32), by_owner(F32)],
        (acc_rows, flag_rows, grouped, met[-1]),
        [VMEM] * 3 + [ANY],
        cost=8_000_000_000,
    )
    own, near, *pairs = call(
        row_kernel,
        [block()] * NL + [one_block()] * NH,
        (*tables[0], *tables[1], counts),
        [VMEM] * (NL * NX) + [ANY],
        scratch=[pltpu.VMEM((NH, ONE, LANES), F32)],
    )
    rows_got = list(pairs)
    for r in (1, 3, 2):
        rows_got[r] = lax.ppermute(pairs[r], "h", swapped(NH, r))
    plane = call(plane_kernel, one_block(), tuple(rows_got), [VMEM] * NH)
    ny = lax.axis_size("y")
    planes = [
        lax.ppermute(plane, "y", [(i, i + r) for i in range(ny - r)]) for r in range(1, ny)
    ]
    came = call(rows_back_kernel, [one_block()] * NH, (*planes, *rows_got),
                [VMEM] * (3 + NH))
    came = list(came)
    for r in (1, 3, 2):
        came[r] = lax.ppermute(came[r], "h", swapped(NH, r))
    parts = call(
        chips_back_kernel,
        [block()] * (NL * NX),
        (*came, own, near, *tables[0], *tables[1]),
        [VMEM] * (NH + NL + NL * NX),
        scratch=[pltpu.VMEM((NH, ONE, LANES), F32)],
    )
    parts = [list(parts[:NX]), list(parts[NX:])]
    kept = parts[0][0]
    for dx in (2, 0, 1, 3):
        for dz in reversed(range(NL)):
            parts[dz][dx] = exchange(parts[dz][dx], dz, (NX - dx) % NX)
    run, count, is_open, users = call(
        in_time_kernel,
        [jax.ShapeDtypeStruct((rows, LANES), F32), small_f, small_f,
         jax.ShapeDtypeStruct((2 * lines, LANES), I32)],
        (slot, slot, home, account, run_slots, counts, opens, kept),
        [SMEM] + [VMEM] * 6 + [ANY],
        cost=10_000_000_000,
    )
    keep, last = [], []
    for dxs in BACK:
        stay, send = call(
            cores_back_kernel,
            [block(2 * len(dxs))] * 2,
            (keep[-1] if keep else count, *[parts[dz][dx] for dx in dxs for dz in range(NL)],
             *[mine[dx] for dx in dxs], *[got[dx] for dx in dxs]),
            [ANY] + [VMEM] * (4 * len(dxs)),
            cost=500_000_000,
        )
        keep.append(stay)
        last.append(lax.ppermute(send, "c", swap))
    table, came_counts = call(
        gather_kernel,
        [block(NC * CHUNKS), small_f],
        (home, account, *keep, last[0]),
        [VMEM] * 6,
        scratch=[pltpu.SemaphoreType.DMA((12,))],
        cost=2_000_000_000,
    )
    _, result = call(
        finish_kernel,
        [block(NC * CHUNKS), jax.ShapeDtypeStruct((rows, LANES), F32)],
        (users, run, count, is_open, home, account, came_counts, table, *last[1:]),
        [VMEM] * 10,
        out_specs=[VMEM, ANY],
        scratch=[pltpu.VMEM((rows, LANES), F32)] + [pltpu.SMEM((4, LANES), I32)] * 4
        + [pltpu.SemaphoreType.DMA((4,)), pltpu.SemaphoreType.DMA((8,)),
           pltpu.SemaphoreType.DMA((4,))],
        aliases={7: 0},
    )
    return result


def solution(mesh):
    axes = ("y", "h", "l", "x", "c")
    split = Mesh(mesh.devices.reshape(-1, NH, NL, NX, NC), axes)
    return jax.shard_map(
        body,
        mesh=split,
        in_specs=(P(axes, None), P(axes, None), P(axes), P(axes)),
        out_specs=P(axes, None),
        check_vma=False,
    )
```

```python
import functools

import jax
import jax.numpy as jnp
from jax import lax
from jax.experimental import pallas as pl
from jax.experimental.pallas import tpu as pltpu
from jax.sharding import Mesh, PartitionSpec as P


LANES = 128
FOUR = 4
TAIL = FOUR * LANES
ROWS = TAIL + 8
ONE = LANES + 8
NH, NL, NX, NC = 4, 2, 4, 2
OWNERS = NH * NL * NX * NC
HALF = OWNERS // NC
CHUNKS = HALF // FOUR
BF16, F32, I32 = jnp.bfloat16, jnp.float32, jnp.int32
VMEM = pl.BlockSpec(memory_space=pltpu.VMEM)
SMEM = pl.BlockSpec(memory_space=pltpu.SMEM)
HBM = pl.BlockSpec(memory_space=pltpu.HBM)
ANY = pl.BlockSpec(memory_space=pl.ANY)


def dot(a, b):
    return lax.dot_general(a, b, (((1,), (0,)), ((), ())), preferred_element_type=F32)


def dot_nt(a, b):
    return lax.dot_general(a, b, (((1,), (1,)), ((), ())), preferred_element_type=F32)


def iota(shape, dim):
    return lax.broadcasted_iota(I32, shape, dim)


def as_bf16(mask):
    return jnp.where(mask, 1.0, 0.0).astype(BF16)


def two_parts(v):
    high = v.astype(BF16)
    low = (v - high.astype(F32)).astype(BF16)
    return jnp.concatenate([high, low], axis=1)


def masked_sum(mask, parts):
    both = dot(mask, parts)
    return both[:, :LANES] + both[:, LANES:]


def call(kernel, out, args, specs, out_specs=None, scratch=(), cost=1_000_000, limit=24, aliases=None):
    return pl.pallas_call(
        kernel,
        out_shape=out,
        in_specs=specs,
        out_specs=out_specs or jax.tree.map(lambda _: VMEM, out),
        scratch_shapes=list(scratch),
        input_output_aliases=aliases or {},
        cost_estimate=pl.CostEstimate(flops=cost, bytes_accessed=1_000_000, transcendentals=0),
        compiler_params=pltpu.CompilerParams(vmem_limit_bytes=limit << 20),
    )(*args)


class Place:
    def __getitem__(self, n):
        return lax.axis_index(("c", "x", "l", "h", "y")[n])


PLACE = Place()


def block(*lead):
    return jax.ShapeDtypeStruct((*lead, ROWS, LANES), F32)


def one_block(*lead):
    return jax.ShapeDtypeStruct((*lead, ONE, LANES), F32)


def chunk_of(dz, dx):
    return (PLACE[2] ^ dz) * NX + lax.rem(PLACE[1] + dx, NX)


def rank_kernel(events, slot_out, acc_out, flag_out):
    lines = slot_out.shape[0]
    below = as_bf16(iota((LANES, LANES), 0) < iota((LANES, LANES), 1))
    with_total = jnp.concatenate([below, jnp.ones((LANES, LANES), BF16)], axis=1)
    owner_ids = iota((OWNERS, LANES), 0)
    before = jnp.zeros((OWNERS, LANES), F32)
    codes = jnp.zeros((OWNERS, LANES), F32)
    step = 8
    for b in range(0, lines, step):
        homes = [events[b + i : b + i + 1, :] for i in range(step)]
        chosen = [owner_ids == home for home in homes]
        counted = dot(jnp.concatenate([as_bf16(c) for c in chosen], axis=0), with_total)
        coded, rank_of = [], []
        for i in range(step):
            some = counted[i * OWNERS : (i + 1) * OWNERS, :]
            rank = jnp.sum(
                jnp.where(chosen[i], some[:, :LANES] + before, 0.0), axis=0, keepdims=True
            ).astype(I32)
            before = before + some[:, LANES:]
            slot_out[b + i : b + i + 1, :] = homes[i] * LANES + rank
            account = events[lines + b + i : lines + b + i + 1, :]
            flag = events[2 * lines + b + i : 2 * lines + b + i + 1, :]
            code = (account * 2 + flag + 1).astype(F32)
            coded.append(jnp.where(chosen[i], code, 0.0).astype(BF16))
            rank_of.append(as_bf16(iota((LANES, LANES), 0) == rank))
        codes = codes + dot_nt(
            jnp.concatenate(coded, axis=1), jnp.concatenate(rank_of, axis=1)
        )
    code_ids = codes.astype(I32) - 1
    acc_out[...] = jnp.right_shift(code_ids, 1)
    flag_out[...] = jnp.where(code_ids >= 0, jnp.bitwise_and(code_ids, 1), 0).astype(F32)


def spread_kernel(slot_rows, features, grouped, slots, sem):
    copy = pltpu.make_async_copy(slot_rows, slots, sem)
    copy.start()
    zero = jnp.zeros((LANES, LANES), F32)

    def clear(o, _):
        grouped[pl.ds(pl.multiple_of(o * LANES, LANES), LANES), :] = zero
        return 0

    lax.fori_loop(0, OWNERS, clear, 0)
    copy.wait()

    for b in range(slot_rows.shape[0]):
        for j in range(LANES):
            at = b * LANES + j
            grouped[pl.ds(slots[b, j], 1), :] = features[at : at + 1, :]


def after_and_ones():
    after = as_bf16(iota((LANES, LANES), 0) > iota((LANES, LANES), 1))
    return jnp.concatenate([after, jnp.ones((LANES, LANES), BF16)], axis=1)


def cut(v, i):
    return v[i * LANES : (i + 1) * LANES, :]


def counted_rows(counted, flagged):
    count = dot(jnp.concatenate(counted, axis=0), jnp.ones((LANES, LANES), BF16))
    lane = iota((LANES, LANES), 1)
    both = jnp.zeros((LANES, LANES), F32)
    for i in range(8):
        both = jnp.where(lane == i, cut(count, i), both)
        both = jnp.where(lane == 8 + i, cut(flagged, i), both)
    return both.T


def closing_kernel(dx, acc_rows, flag_rows, grouped, ready, other, mine):
    sides = after_and_ones()
    for out, half_of in ((other, 1 - PLACE[0]), (mine, PLACE[0])):
        bases = [half_of * HALF + chunk_of(dz, dx) * FOUR for dz in range(NL)]
        acc8 = jnp.concatenate([acc_rows[pl.ds(b, FOUR), :] for b in bases], axis=0)
        flag8 = jnp.concatenate([flag_rows[pl.ds(b, FOUR), :] for b in bases], axis=0)
        member = [iota((LANES, LANES), 0) == acc8[i : i + 1, :] for i in range(8)]
        member_flags = [
            jnp.where(member[i], flag8[i : i + 1, :], 0.0).astype(BF16) for i in range(8)
        ]
        flagged = dot(jnp.concatenate(member_flags, axis=0), sides)
        counted = [as_bf16(member[i] & (cut(flagged, i)[:, :LANES] < 0.5)) for i in range(8)]
        rows = counted_rows(counted, flagged[:, LANES:])
        marks = jnp.minimum(rows[8:16, :], 1.0)
        for dz in range(NL):
            for i in range(FOUR):
                at = pl.multiple_of((bases[dz] + i) * LANES, LANES)
                values = two_parts(grouped[pl.ds(at, LANES), :])
                out[dz, i * LANES : (i + 1) * LANES, :] = masked_sum(
                    counted[dz * FOUR + i], values
                )
            own = slice(dz * FOUR, dz * FOUR + FOUR)
            out[dz, TAIL:, :] = jnp.concatenate([rows[own, :], marks[own, :]], axis=0)


def running_kernel(acc_rows, flag_rows, grouped, ready, run, counts, opens):
    sides = after_and_ones()
    up_to = iota((LANES, LANES), 1) <= iota((LANES, LANES), 0)

    def some(g, _):
        rows = pl.ds(pl.multiple_of(g * 8, 8), 8)
        acc8 = acc_rows[rows, :].astype(F32)
        flag8 = flag_rows[rows, :]
        acc_cols = acc8.T
        same = []
        for i in range(8):
            acc_col = jnp.broadcast_to(acc_cols[:, i : i + 1], (LANES, LANES))
            same.append((acc_col == acc8[i : i + 1, :]) & (acc_col >= 0.0) & up_to)
        same_flags = [
            jnp.where(same[i], flag8[i : i + 1, :], 0.0).astype(BF16) for i in range(8)
        ]
        flagged = dot(jnp.concatenate(same_flags, axis=0), sides)
        session = [as_bf16(same[i] & (cut(flagged, i)[:, :LANES] < 0.5)) for i in range(8)]
        for i in range(8):
            at = pl.ds(pl.multiple_of((g * 8 + i) * LANES, LANES), LANES)
            run[at, :] = masked_sum(session[i], two_parts(grouped[at, :]))
        found = counted_rows(session, flagged[:, LANES:])
        counts[rows, :] = found[:8, :]
        opens[rows, :] = jnp.where(found[8:16, :] < 0.5, 1.0, 0.0)
        return 0

    lax.fori_loop(0, OWNERS // 8, some, 0)


def in_time_kernel(
    slots, slot_rows, home, account, run, counts, opens, ready,
    run_out, count_out, open_out, user_out,
):
    lines = home.shape[0]

    def scalars(t, _):
        rows = pl.ds(pl.multiple_of(t * 8, 8), 8)
        home8 = home[rows, :]
        rank = slot_rows[rows, :] - home8 * LANES
        count = jnp.zeros((8, LANES), F32)
        is_open = jnp.zeros((8, LANES), F32)
        for o in range(OWNERS):
            here = home8 == o
            for_count = jnp.broadcast_to(counts[o : o + 1, :], (8, LANES))
            for_open = jnp.broadcast_to(opens[o : o + 1, :], (8, LANES))
            count = jnp.where(here, jnp.take_along_axis(for_count, rank, axis=1), count)
            is_open = jnp.where(here, jnp.take_along_axis(for_open, rank, axis=1), is_open)
        count_out[rows, :] = count
        open_out[rows, :] = is_open
        chunk = jnp.right_shift(home8, 2)
        row = (home8 - chunk * FOUR) * LANES + account[rows, :]
        user = chunk * ROWS + jnp.where(is_open > 0.5, row, TAIL + FOUR)
        for half in range(2):
            at = pl.ds(pl.multiple_of(t * 16 + half * 8, 8), 4)
            user_out[at, :] = user[half * 4 : half * 4 + 4, :]
        return 0

    lax.fori_loop(0, lines // 8, scalars, 0)

    def collect(b, _):
        for j in range(LANES):
            run_out[pl.ds(b * LANES + j, 1), :] = run[pl.ds(slots[b, j], 1), :]
        return 0

    lax.fori_loop(0, lines, collect, 0)


def sums_of(chunk, i):
    return chunk[i * LANES : (i + 1) * LANES, :]


def keep_of(tail):
    return (1.0 - tail).T


def joined_sums(keep, i, earlier, later):
    return later + jnp.broadcast_to(keep[:, i : i + 1], (LANES, LANES)) * earlier


def joined_tail(earlier, later):
    marks = jnp.concatenate([later[FOUR:, :], later[:FOUR, :]], axis=0)
    return jnp.where(
        iota((8, LANES), 0) < FOUR, later + (1.0 - marks) * earlier, jnp.maximum(later, earlier)
    )


def joined_one(earlier, later):
    tail, first = later[LANES:, :], earlier[LANES:, :]
    mark = tail[1:2, :]
    sub = iota((8, LANES), 0)
    sums = joined_sums(keep_of(tail), 1, earlier[:LANES, :], later[:LANES, :])
    tail = jnp.where(
        sub == 0, tail + (1.0 - mark) * first, jnp.where(sub == 1, jnp.maximum(tail, first), 0.0)
    )
    return jnp.concatenate([sums, tail], axis=0)


def core_kernel(mine, got, *outs):
    first = PLACE[0] == 0
    for dz in range(NL):
        a, b = mine[dz, TAIL:, :], got[dz, TAIL:, :]
        early, late = jnp.where(first, a, b), jnp.where(first, b, a)
        keep = keep_of(late)
        for i in range(FOUR):
            at = slice(i * LANES, (i + 1) * LANES)
            a, b = mine[dz, at, :], got[dz, at, :]
            outs[dz][at, :] = joined_sums(
                keep, FOUR + i, jnp.where(first, a, b), jnp.where(first, b, a)
            )
        outs[dz][TAIL:, :] = joined_tail(early, late)


def row_kernel(*refs):
    tables = (refs[:NX], refs[NX : 2 * NX])
    totals = refs[2 * NX + 1 : 2 * NX + 3]
    outs, pair = refs[2 * NX + 3 : 2 * NX + 3 + NH], refs[-1]
    for x in range(NX):

        @pl.when(PLACE[1] == x)
        def _(x=x):
            for dz in range(NL):
                order = [tables[dz][(x - j) % NX] for j in range(NX)]
                tails = [t[TAIL:, :] for t in order]
                keep = [keep_of(t) for t in tails]
                for i in range(FOUR):
                    total = sums_of(order[0], i)
                    for j in range(1, NX):
                        total = joined_sums(keep[j], FOUR + i, total, sums_of(order[j], i))
                    totals[dz][i * LANES : (i + 1) * LANES, :] = total
                tail = tails[0]
                for j in range(1, NX):
                    tail = joined_tail(tail, tails[j])
                totals[dz][TAIL:, :] = tail

    own, near = totals
    first = PLACE[2] == 0
    a, b = own[TAIL:, :], near[TAIL:, :]
    early, late = jnp.where(first, a, b), jnp.where(first, b, a)
    keep = keep_of(late)
    tail = joined_tail(early, late)
    sub = iota((8, LANES), 0)
    for i in range(FOUR):
        a, b = sums_of(own, i), sums_of(near, i)
        pair[i, :LANES, :] = joined_sums(
            keep, FOUR + i, jnp.where(first, a, b), jnp.where(first, b, a)
        )
        pair[i, LANES:, :] = jnp.where(
            sub == 0, tail[i : i + 1, :],
            jnp.where(sub == 1, tail[FOUR + i : FOUR + i + 1, :], 0.0),
        )
    for r in range(NH):
        outs[r][...] = pair[PLACE[3] ^ r]


def plane_kernel(r0, r1, r2, r3, out):
    rows = (r0, r1, r2, r3)
    for h in range(NH):

        @pl.when(PLACE[3] == h)
        def _(h=h):
            total = rows[h][...]
            for j in range(1, NH):
                total = joined_one(total, rows[h ^ j][...])
            out[...] = total


def rows_back_kernel(p1, p2, p3, r0, r1, r2, r3, *outs):
    rows = (r0, r1, r2, r3)
    start = jnp.zeros((ONE, LANES), F32)
    for r, plane in ((2, p3), (1, p2), (0, p1)):
        start = jnp.where(PLACE[4] > r, joined_one(start, plane[...]), start)
    for h in range(NH):

        @pl.when(PLACE[3] == h)
        def _(h=h):
            state = start
            for j in range(NH):
                k = h ^ j
                outs[k][...] = state
                if j < NH - 1:
                    state = joined_one(state, rows[k][...])


def chips_back_kernel(e0, e1, e2, e3, own, near, *refs):
    tables, outs = (refs[:NX], refs[NX : 2 * NX]), (refs[2 * NX : 3 * NX], refs[3 * NX : 4 * NX])
    came = refs[-1]
    for r, e in enumerate((e0, e1, e2, e3)):
        came[PLACE[3] ^ r] = e[...]
    first = PLACE[2] == 0
    sub = iota((8, LANES), 0)
    tail0 = jnp.zeros((8, LANES), F32)
    for i in range(FOUR):
        tail0 = jnp.where(sub == i, came[i, LANES : LANES + 1, :], tail0)
    between = jnp.where(first, own[TAIL:, :], near[TAIL:, :])
    keep = keep_of(between)
    tail1 = joined_tail(tail0, between)
    for x in range(NX):

        @pl.when(PLACE[1] == x)
        def _(x=x):
            for dz in range(NL):
                order = [(x - j) % NX for j in range(NX)]
                tails = [tables[dz][k][TAIL:, :] for k in order[:-1]]
                keeps = [keep_of(t) for t in tails]
                late = first if dz else jnp.logical_not(first)
                for i in range(FOUR):
                    at = slice(i * LANES, (i + 1) * LANES)
                    state = came[i, :LANES, :]
                    second = joined_sums(
                        keep, FOUR + i, state, jnp.where(first, own[at, :], near[at, :])
                    )
                    state = jnp.where(late, second, state)
                    for j, k in enumerate(order):
                        outs[dz][k][at, :] = state
                        if j < NX - 1:
                            state = joined_sums(
                                keeps[j], FOUR + i, state, sums_of(tables[dz][k], i)
                            )
                tail = jnp.where(late, tail1, tail0)
                for j, k in enumerate(order):
                    outs[dz][k][TAIL:, :] = tail
                    if j < NX - 1:
                        tail = joined_tail(tail, tails[j])


def cores_back_kernel(ready, *refs):
    n = (len(refs) - 2) // 4
    parts, mine, got = refs[: 2 * n], refs[2 * n : 3 * n], refs[3 * n : 4 * n]
    keep_out, send = refs[4 * n :]
    first = PLACE[0] == 0
    counts_only = iota((8, LANES), 0) < FOUR
    for d in range(n):
        for dz in range(NL):
            part, at = parts[2 * d + dz], 2 * d + dz
            core0 = jnp.where(first, mine[d][dz, TAIL:, :], got[d][dz, TAIL:, :])
            keep = keep_of(core0)
            for i in range(FOUR):
                rows = slice(i * LANES, (i + 1) * LANES)
                state = part[rows, :]
                second = joined_sums(
                    keep, FOUR + i, state,
                    jnp.where(first, mine[d][dz, rows, :], got[d][dz, rows, :]),
                )
                keep_out[at, rows, :] = jnp.where(first, state, second)
                send[at, rows, :] = jnp.where(first, second, state)
            state = part[TAIL:, :]
            second = joined_tail(state, core0)
            keep_out[at, TAIL:, :] = jnp.where(counts_only, jnp.where(first, state, second), 0.0)
            send[at, TAIL:, :] = jnp.where(counts_only, jnp.where(first, second, state), 0.0)


BACK = ((2, 0), (1,), (3,))


def lookup(home8, account8, held, came):
    for tail, at in held:
        for i in range(FOUR):
            row = jnp.broadcast_to(tail[i : i + 1, :], (8, LANES))
            found = jnp.take_along_axis(row, account8, axis=1)
            came = jnp.where(home8 == at * FOUR + i, found, came)
    return came


def held_parts(dxs, side, own_half):
    half_of = PLACE[0] if own_half else 1 - PLACE[0]
    return [
        (side, 2 * d + dz, half_of * CHUNKS + chunk_of(dz, dx))
        for d, dx in enumerate(dxs)
        for dz in range(NL)
    ]


def gather_kernel(home, account, *refs):
    n = len(BACK)
    sides, (table, counts, sems) = refs[: n + 1], refs[n + 1 :]
    held = []
    for s, side in enumerate(sides):
        held += held_parts(BACK[s % n], side, s < n)
    copies = [
        pltpu.make_async_copy(side.at[k], table.at[at], sems.at[i])
        for i, (side, k, at) in enumerate(held)
    ]
    for copy in copies:
        copy.start()
    tails = [(side[k, TAIL:, :], at) for side, k, at in held]
    for t in range(home.shape[0] // 8):
        rows = slice(8 * t, 8 * t + 8)
        counts[rows, :] = lookup(
            home[rows, :], account[rows, :], tails, jnp.zeros((8, LANES), F32)
        )
    for copy in copies:
        copy.wait()


def finish_kernel(
    user_rows, run, count, is_open, home, account, counts, table_in, got1, got2,
    table, out, picked, u0, u1, u2, u3, sems, out_sems, list_sems,
):
    users = (u0, u1, u2, u3)

    def listed(g, q):
        return pltpu.make_async_copy(
            user_rows.at[pl.ds(pl.multiple_of(g * 8, 8), 4), :], users[q], list_sems.at[q]
        )

    for q in range(4):
        listed(q, q).start()
    held = []
    for s, side in ((1, got1), (2, got2)):
        held += held_parts(BACK[s], side, False)
    copies = [
        pltpu.make_async_copy(side.at[k], table.at[at], sems.at[i])
        for i, (side, k, at) in enumerate(held)
    ]
    for copy in copies:
        copy.start()
    lines = home.shape[0]
    flat = table.reshape(NC * CHUNKS * ROWS, LANES)
    tails = [(side[k, TAIL:, :], at) for side, k, at in held]
    scale = []
    for t in range(lines // 8):
        rows = slice(8 * t, 8 * t + 8)
        came = lookup(home[rows, :], account[rows, :], tails, counts[rows, :])
        scale.append(1.0 / (count[rows, :] + is_open[rows, :] * came))
    scale = jnp.concatenate(scale, axis=0)
    if lines < LANES:
        scale = jnp.concatenate([scale, jnp.zeros((LANES - lines, LANES), F32)], axis=0)
    scale = scale.T
    for copy in copies:
        copy.wait()

    group = 4

    def leave(g):
        rows = pl.ds(pl.multiple_of(g * group * LANES, group * LANES), group * LANES)
        return pltpu.make_async_copy(picked.at[rows, :], out.at[rows, :], out_sems.at[g])

    def some(turn, scale):
        for q in range(4):
            g = turn * 4 + q
            listed(g, q).wait()
            for b in range(group):
                for j in range(LANES):
                    at = (g * group + b) * LANES + j
                    picked[pl.ds(at, 1), :] = flat[pl.ds(users[q][b, j], 1), :]
            pl.when(g + 4 < lines // group)(lambda g=g, q=q: listed(g + 4, q).start())
            for b in range(group):
                at = pl.ds(pl.multiple_of((g * group + b) * LANES, LANES), LANES)
                factor = jnp.broadcast_to(scale[:, b : b + 1], (LANES, LANES))
                picked[at, :] = (run[at, :] + picked[at, :]) * factor
            leave(g).start()
            scale = pltpu.roll(scale, LANES - group, 1)
        return scale

    lax.fori_loop(0, lines // (4 * group), some, scale)
    for g in range(lines // group):
        leave(g).wait()


def swapped(n, k):
    return [(i, i ^ k) for i in range(n)]


def body(features, home, account, flags):
    rows = features.shape[0]
    lines = rows // LANES
    home = home.reshape(lines, LANES)
    account = account.reshape(lines, LANES)
    flags = flags.reshape(lines, LANES)
    small = jax.ShapeDtypeStruct((lines, LANES), I32)
    small_f = jax.ShapeDtypeStruct((lines, LANES), F32)
    by_owner = functools.partial(jax.ShapeDtypeStruct, (OWNERS, LANES))
    by_slot = jax.ShapeDtypeStruct((OWNERS * LANES, LANES), F32)
    slot, acc_rows, flag_rows = call(
        rank_kernel,
        [small, by_owner(I32), by_owner(F32)],
        (jnp.concatenate([home, account, flags]),),
        [VMEM],
        cost=2_000_000_000,
    )
    grouped = call(
        spread_kernel,
        by_slot,
        (slot, features),
        [VMEM] * 2,
        scratch=[pltpu.SMEM((lines, LANES), I32), pltpu.SemaphoreType.DMA],
        cost=4_000_000_000,
    )
    swap = swapped(NC, 1)

    def exchange(v, dz, dx):
        if dz == 0 and dx == 0:
            return v
        pairs = [
            (row * NX + x, (row ^ dz) * NX + (x + dx) % NX) for row in range(NL) for x in range(NX)
        ]
        return lax.ppermute(v, ("l", "x"), pairs)

    order = (2, 1, 3, 0)
    mine, got = [None] * NX, [None] * NX
    tables = [[None] * NX for _ in range(NL)]

    def meet(dx):
        chunks = call(core_kernel, [block()] * NL, (mine[dx], got[dx]),
                      [VMEM, VMEM], cost=500_000_000)
        for dz in reversed(range(NL)):
            tables[dz][dx] = exchange(chunks[dz], dz, dx)
        return chunks[0]

    met = [acc_rows]
    for at, dx in enumerate(order):
        other, mine[dx] = call(
            functools.partial(closing_kernel, dx),
            [block(NL)] * 2,
            (acc_rows, flag_rows, grouped, met[at]),
            [VMEM] * 3 + [ANY],
            cost=1_500_000_000,
        )
        got[dx] = lax.ppermute(other, "c", swap)
        met.append(meet(order[at - 1]) if at else mine[dx])
    met.append(meet(order[-1]))
    run_slots, counts, opens = call(
        running_kernel,
        [by_slot, by_owner(F32), by_owner(F32)],
        (acc_rows, flag_rows, grouped, met[-1]),
        [VMEM] * 3 + [ANY],
        cost=8_000_000_000,
    )
    own, near, *pairs = call(
        row_kernel,
        [block()] * NL + [one_block()] * NH,
        (*tables[0], *tables[1], counts),
        [VMEM] * (NL * NX) + [ANY],
        scratch=[pltpu.VMEM((NH, ONE, LANES), F32)],
    )
    rows_got = list(pairs)
    for r in (1, 3, 2):
        rows_got[r] = lax.ppermute(pairs[r], "h", swapped(NH, r))
    plane = call(plane_kernel, one_block(), tuple(rows_got), [VMEM] * NH)
    ny = lax.axis_size("y")
    planes = []
    for r in range(1, ny):
        planes.append(lax.ppermute(plane, "y", [(i, i + r) for i in range(ny - r)]))
    came = call(rows_back_kernel, [one_block()] * NH, (*planes, *rows_got),
                [VMEM] * (3 + NH))
    came = list(came)
    for r in (1, 3, 2):
        came[r] = lax.ppermute(came[r], "h", swapped(NH, r))
    parts = call(
        chips_back_kernel,
        [block()] * (NL * NX),
        (*came, own, near, *tables[0], *tables[1]),
        [VMEM] * (NH + NL + NL * NX),
        scratch=[pltpu.VMEM((NH, ONE, LANES), F32)],
    )
    parts = [list(parts[:NX]), list(parts[NX:])]
    kept = parts[0][0]
    for dx in (2, 0, 1, 3):
        for dz in reversed(range(NL)):
            parts[dz][dx] = exchange(parts[dz][dx], dz, (NX - dx) % NX)
    run, count, is_open, users = call(
        in_time_kernel,
        [jax.ShapeDtypeStruct((rows, LANES), F32), small_f, small_f,
         jax.ShapeDtypeStruct((2 * lines, LANES), I32)],
        (slot, slot, home, account, run_slots, counts, opens, kept),
        [SMEM] + [VMEM] * 6 + [ANY],
        cost=10_000_000_000,
    )
    keep, last = [], []
    for dxs in BACK:
        stay, send = call(
            cores_back_kernel,
            [block(2 * len(dxs))] * 2,
            (keep[-1] if keep else count, *[parts[dz][dx] for dx in dxs for dz in range(NL)],
             *[mine[dx] for dx in dxs], *[got[dx] for dx in dxs]),
            [ANY] + [VMEM] * (4 * len(dxs)),
            cost=500_000_000,
        )
        keep.append(stay)
        last.append(lax.ppermute(send, "c", swap))
    table, came_counts = call(
        gather_kernel,
        [block(NC * CHUNKS), small_f],
        (home, account, *keep, last[0]),
        [VMEM] * 6,
        scratch=[pltpu.SemaphoreType.DMA((12,))],
        cost=2_000_000_000,
    )
    _, result = call(
        finish_kernel,
        [block(NC * CHUNKS), jax.ShapeDtypeStruct((rows, LANES), F32)],
        (users, run, count, is_open, home, account, came_counts, table, *last[1:]),
        [VMEM] * 10,
        out_specs=[VMEM, ANY],
        scratch=[pltpu.VMEM((rows, LANES), F32)] + [pltpu.SMEM((4, LANES), I32)] * 4
        + [pltpu.SemaphoreType.DMA((4,)), pltpu.SemaphoreType.DMA((8,)),
           pltpu.SemaphoreType.DMA((4,))],
        aliases={7: 0},
    )
    return result


def solution(mesh):
    axes = ("y", "h", "l", "x", "c")
    split = Mesh(mesh.devices.reshape(-1, NH, NL, NX, NC), axes)
    return jax.shard_map(
        body,
        mesh=split,
        in_specs=(P(axes, None), P(axes, None), P(axes), P(axes)),
        out_specs=P(axes, None),
        check_vma=False,
    )
```
